128 devices in a mesh: comp: 2 (over x_lo), tile: 64 (over y, z, x_hi, core).
Axes of the slice: x: 4 (x_hi: 2, x_lo: 2; x = x_hi * 2 + x_lo), y: 4, z: 4, core: 2. Of those that a mesh axis runs over, the one named last changes fastest.
Arguments:
- starting_perturbation: float32 [2, 128, 512, 512], P('comp', None, 'tile'), may hold values from -6 to 6
- measured_discrepancy: float32 [2, 128, 512, 512], P('comp', None, 'tile'), may hold values from -6 to 6
- diffusion: float32 [2, 128, 512, 512], P('comp', None, 'tile'), may hold values from 0.02 to 0.24
- vert_mix: float32 [2, 128, 128], P('comp'), may hold values from -0.03125 to 0.03125
- ocean_mask: int32 [512, 512], P('tile'), may hold values 0 or 1
- pair_tile: int32 [2, 64, 8], replicated, may hold values from 0 to 63, as said below
- pair_patch: int32 [2, 64, 64], replicated, may hold values from 0 to 31
- dest_patch: int32 [2, 64, 64], P('comp', 'tile'), may hold values from 0 to 31
- pair_blocks: int32 [2, 64, 8], P('comp', 'tile'), may hold values from 1 to 8, 48 in all within a row
- remap_weight: float32 [2, 4096, 128, 128], P('comp', 'tile'), may hold values from -0.5 to 0.5
Outputs:
- final_perturbation: float32 [2, 128, 512, 512], P('comp', None, 'tile')
- gradient: float32 [2, 128, 512, 512], P('comp', None, 'tile')
The draws below stay inside these ranges and needn't reach their ends.
Inputs may be any that keep to these rules, and one draw needn't show every extreme that they name: `pair_tile`: the 8 source tiles listed for destination tile t are distinct; exactly one of them is (t + 32) mod 64, and each other is (t + o) mod 64 for some o from 1 - 8 to 7. A pair's live blocks are its first pair_blocks ones.
All inputs are finite; a program needn't handle non-finite values. No bound on the sum of `ocean_mask` on one device may be relied on, other than what follows from the above.
Results may differ from the reference program's by a relative error of at most 0.0001.
Values sent between devices are 32-bit elements; how exact they have to be, the bound alone decides.
No kernel may reach another device: no remote copies, remote signals or barrier semaphores. Data moves between devices by JAX's collectives and lax.ppermute only.
A program may use at most 128 MiB of HBM per device.

```python
import math
import jax
import jax.numpy as jnp
import numpy as np
from jax import lax

LEV = 128
LON = 512
STEPS = 4
NPAIR = 8
PB = 8
PATCH = 128
TILES = 64
NROWS = 512
NBLK = 64
NPATCH = 32


def draw_pair_tile(key, part):
    key_list = jax.random.split(jax.random.fold_in(key, 17), 2 * TILES)
    tile_ids = jnp.tile(jnp.arange(TILES, dtype=jnp.int32), 2)

    def draw_row(subkey, tile_now):
        first_key, second_key = jax.random.split(subkey)
        near_offsets = jax.random.permutation(first_key, 2 * NPAIR - 1)[:NPAIR - 1].astype(jnp.int32) - (NPAIR - 1)
        all_offsets = jnp.concatenate([near_offsets, jnp.full((1,), TILES // 2, jnp.int32)])
        ordered = jax.random.permutation(second_key, all_offsets)
        return (tile_now + ordered) % TILES
    return jax.vmap(draw_row)(key_list, tile_ids).reshape(2, TILES, NPAIR).astype(jnp.int32)


def set_ends(values, own_key, smallest, high):
    longest = values.shape.index(max(values.shape))
    spots = []
    for shift in (0, 1):
        where = [jax.random.randint(jax.random.fold_in(own_key, axis), (), 0, length) for axis, length in enumerate(values.shape)]
        where[longest] = (where[longest] + shift) % values.shape[longest]
        spots.append(tuple(where))
    return values.at[spots[0]].set(smallest).at[spots[1]].set(high)


def levels(stream_key, dims, cuts, smallest, top_value):
    level = 1.0
    for axis_at, shards_of in cuts:
        draws = jax.random.uniform(jax.random.fold_in(jax.random.fold_in(stream_key, 6), axis_at), (shards_of,), jnp.float32, smallest / len(cuts), top_value / len(cuts))
        level = level * jnp.repeat(jnp.exp(draws), dims[axis_at] // shards_of).reshape((-1,) + (1,) * (len(dims) - 1 - axis_at))
    return level


def profile(count, total, most, skew):
    weights = [(1 << 20) // math.isqrt(grade ** skew) + 1 for grade in range(2, count + 1)]
    surplus, holding = total - most - (count - 1), [1] * (count - 1)
    while surplus > 0:
        free = [i for i in range(count - 1) if holding[i] < most]
        whole, remaining = sum([weights[i] for i in free]), surplus
        for i in free:
            extra = min(most - holding[i], max(1, remaining * weights[i] // whole), surplus)
            holding[i] = holding[i] + extra
            surplus = surplus - extra
    return np.array([most] + holding)


def ragged(key, count, total, limit, lean):
    if count == 2:
        one = jax.random.randint(key, (), max(1, total - limit), min(limit, total - 1) + 1)
        return jnp.stack([one, total - one])
    lengths = jnp.asarray(profile(count, total, limit, lean), jnp.int32)
    couples = (count - 1) // 2
    giver, sink = lengths[1:1 + 2 * couples:2], lengths[2:2 + 2 * couples:2]
    room = jnp.minimum(giver - 1, limit - sink)
    moved = jax.random.randint(jax.random.fold_in(key, 1), (couples,), 0, 1 << 20) % (room + 1)
    lengths = lengths.at[1:1 + 2 * couples:2].set(giver - moved).at[2:2 + 2 * couples:2].set(sink + moved)
    return lengths[jax.random.permutation(jax.random.fold_in(key, 2), count)]


def gaussian(rng, dims, deviation, limit, cuts=(), kind=jnp.bfloat16):
    level = levels(rng, dims, cuts, -0.22, 0.18) if cuts else 1.0
    drawn = jax.random.normal(rng, dims, jnp.float32) * deviation * level
    return jnp.minimum(jnp.maximum(drawn, -limit), limit).astype(kind)


def setup_inputs(seed: int = 0) -> dict:
    splits = jax.random.split(jax.random.key(seed), 11)
    starting_perturbation = gaussian(splits[0], (2, LEV, NROWS, LON), 1.0, 6.0, ((0, 2), (2, 64)), jnp.float32)
    measured_discrepancy = gaussian(splits[1], (2, LEV, NROWS, LON), 1.0, 6.0, ((0, 2), (2, 64)), jnp.float32)
    diffusion = jnp.clip(jnp.exp(math.log(0.24) - 2.4849066 * jax.random.uniform(splits[2], (2, LEV, NROWS, LON), jnp.float32) ** levels(splits[2], (2, LEV, NROWS, LON), ((0, 2), (2, 64)), -0.2, 0.2)), 0.02, 0.24)
    vert_mix = gaussian(splits[3], (2, LEV, LEV), (256 * LEV) ** -0.5, 0.03125, ((0, 2),), jnp.float32)
    ocean_mask = set_ends((jax.random.randint(splits[4], (NROWS, LON), 0, 10) < 7).astype(jnp.int32), jax.random.fold_in(splits[4], 1), 0, 1)
    pair_tile = draw_pair_tile(jax.random.fold_in(splits[10], 71), 0)
    pair_patch = set_ends(jax.random.randint(splits[6], (2, TILES, NBLK), 0, NPATCH), jax.random.fold_in(splits[6], 1), 0, NPATCH - 1).astype(jnp.int32)
    dest_patch = set_ends(jax.random.randint(splits[7], (2, TILES, NBLK), 0, NPATCH), jax.random.fold_in(splits[7], 1), 0, NPATCH - 1).astype(jnp.int32)
    pair_blocks = jax.vmap(lambda own: ragged(own, NPAIR, NPAIR * PB * 3 // 4, PB, 2))(jax.random.split(splits[8], 2 * TILES)).reshape((2, TILES, NPAIR)).astype(jnp.int32)
    remap_weight = gaussian(splits[9], (2, TILES * NBLK, PATCH, PATCH), PATCH ** -0.5, 0.5, ((0, 2), (1, 64)), jnp.float32)
    return dict(starting_perturbation=starting_perturbation, measured_discrepancy=measured_discrepancy, diffusion=diffusion, vert_mix=vert_mix, ocean_mask=ocean_mask, pair_tile=pair_tile, pair_patch=pair_patch, dest_patch=dest_patch, pair_blocks=pair_blocks, remap_weight=remap_weight)


precise = lax.Precision.HIGHEST

def laplace(system_variables):
    padded = jnp.pad(system_variables, ((0, 0), (0, 0), (1, 1), (0, 0)))
    return padded[:, :, 2:] + padded[:, :, :-2] + jnp.roll(system_variables, -1, axis=3) + jnp.roll(system_variables, 1, axis=3) - 4.0 * system_variables

def column_mix(matrix, system_variables):
    return jnp.einsum('clm,cmrx->clrx', matrix, system_variables, precision=precise)

def reference(starting_perturbation, measured_discrepancy, diffusion, vert_mix, ocean_mask, pair_tile, pair_patch, dest_patch, pair_blocks, remap_weight):
    seawater_indicator = jnp.stack([jnp.ones((NROWS, LON), jnp.float32), ocean_mask.astype(jnp.float32)])[:, None]
    block_ids = jnp.arange(NBLK, dtype=jnp.int32)
    owner_pair = block_ids // PB
    slot_ids = block_ids % PB

    def remap(surface, destination):
        source = surface[1 - destination].reshape(TILES * NPATCH, PATCH)
        source_rows = (pair_tile[destination][:, owner_pair] * NPATCH + pair_patch[destination]).reshape(-1)
        live_mask = (slot_ids[None, :] < pair_blocks[destination][:, owner_pair]).astype(jnp.float32).reshape(-1, 1)
        block_terms = jnp.einsum('bij,bj->bi', remap_weight[destination], source[source_rows], precision=precise) * live_mask
        target = (jnp.arange(TILES, dtype=jnp.int32)[:, None] * NPATCH + dest_patch[destination]).reshape(-1)
        summed_sensitivity = jnp.zeros((TILES * NPATCH, PATCH), jnp.float32).at[target].add(block_terms)
        return summed_sensitivity.reshape(NROWS, LON)

    def couple(system_variables):
        surface = system_variables[:, 0]
        summed_sensitivity = jnp.stack([remap(surface, 0), remap(surface, 1)])
        return system_variables.at[:, 0].add(seawater_indicator[:, 0] * summed_sensitivity)

    def forward_step(system_variables):
        return seawater_indicator * (system_variables + diffusion * laplace(system_variables) + column_mix(vert_mix, system_variables))

    def joint_earth_system(system_variables):
        for step_index in range(STEPS):
            system_variables = forward_step(system_variables)
        system_variables = couple(system_variables)
        for step_index in range(STEPS):
            system_variables = forward_step(system_variables)
        return system_variables
    final_perturbation, reverse_derivative_operator = jax.vjp(joint_earth_system, starting_perturbation)
    measurement_mismatch = final_perturbation - measured_discrepancy
    backpropagated_sensitivity = reverse_derivative_operator(measurement_mismatch)[0]
    return (final_perturbation, starting_perturbation + backpropagated_sensitivity)
```

```python
import jax
import jax.numpy as jnp
from jax import lax
from jax.experimental import pallas as pl
from jax.experimental.pallas import tpu as pltpu
from jax.sharding import PartitionSpec as P

F32 = jnp.float32
BF = jnp.bfloat16
LON, LEV = 512, 128
OFF, PAD = 8, 528
NR = 18
VM = pl.BlockSpec(memory_space=pltpu.VMEM)
SM = pl.BlockSpec(memory_space=pltpu.SMEM)
OFFSETS = tuple(range(-7, 8)) + (32,)


def sds(*shape, dtype=F32):
    return jax.ShapeDtypeStruct(shape, dtype)


def cost(us):
    return pl.CostEstimate(flops=int(us * 5e8), bytes_accessed=1 << 20, transcendentals=0)


def params(**kw):
    return pltpu.CompilerParams(vmem_limit_bytes=60 * 2**20, **kw)


def halves(x):
    hi = x.astype(BF)
    return hi, (x - hi.astype(F32)).astype(BF)


def start_in_kernel(x, top, bot):
    for r in range(8):
        dst = top if r < 4 else bot
        dst[r % 4] = x[pl.ds(r, 128, stride=8), :].T


def start_in(x):
    blk = pl.BlockSpec((4, 128, 128), lambda j: (0, j, 0))
    return pl.pallas_call(
        start_in_kernel,
        grid=(4,),
        out_shape=(sds(4, LON, LEV), sds(4, LON, LEV)),
        in_specs=[pl.BlockSpec((1024, 128), lambda j: (0, j))],
        out_specs=(blk, blk),
        compiler_params=params(),
        cost_estimate=cost(4),
        name="start_in",
    )(x)


def diff_in_kernel(x, sea, full, top, bot):
    for r in range(8):
        y = (x[pl.ds(r, 128, stride=8), :] * sea[r : r + 1, :]).T
        full[r] = y
        if r < 3:
            top[r] = y
        if r > 4:
            bot[r - 5] = y


def diff_in(x, sea):
    blk = pl.BlockSpec((3, 128, 128), lambda j: (0, j, 0))
    return pl.pallas_call(
        diff_in_kernel,
        grid=(4,),
        out_shape=(sds(8, LON, LEV), sds(3, LON, LEV), sds(3, LON, LEV)),
        in_specs=[
            pl.BlockSpec((1024, 128), lambda j: (0, j)),
            pl.BlockSpec((8, 128), lambda j: (0, j)),
        ],
        out_specs=(pl.BlockSpec((8, 128, 128), lambda j: (0, j, 0)), blk, blk),
        compiler_params=params(),
        cost_estimate=cost(4),
        name="diff_in",
    )(x, sea)


def to_rows_kernel(x, o):
    for r in range(8):
        o[r] = x[pl.ds(r, 128, stride=8), :].T


def to_rows(x):
    return pl.pallas_call(
        to_rows_kernel,
        grid=(4,),
        out_shape=sds(8, LON, LEV),
        in_specs=[pl.BlockSpec((1024, 128), lambda j: (0, j))],
        out_specs=pl.BlockSpec((8, 128, 128), lambda j: (0, j, 0)),
        compiler_params=params(),
        cost_estimate=cost(4),
        name="to_rows",
    )(x)


def to_raw_kernel(x, o):
    for r in range(8):
        o[pl.ds(r, 128, stride=8), :] = x[r].T


def to_raw(x):
    return pl.pallas_call(
        to_raw_kernel,
        grid=(4,),
        out_shape=sds(1024, LON),
        in_specs=[pl.BlockSpec((8, 128, 128), lambda j: (0, j, 0))],
        out_specs=pl.BlockSpec((1024, 128), lambda j: (0, j)),
        compiler_params=params(),
        cost_estimate=cost(4),
        name="to_raw",
    )(x)


def grad_out_kernel(x, up, dn, o):
    for r in range(8):
        add = up[r] if r < 4 else dn[r - 4]
        o[pl.ds(r, 128, stride=8), :] = (x[r] + add).T


def grad_out(x, up, dn):
    blk = pl.BlockSpec((4, 128, 128), lambda j: (0, j, 0))
    return pl.pallas_call(
        grad_out_kernel,
        grid=(4,),
        out_shape=sds(1024, LON),
        in_specs=[pl.BlockSpec((8, 128, 128), lambda j: (0, j, 0)), blk, blk],
        out_specs=pl.BlockSpec((1024, 128), lambda j: (0, j)),
        compiler_params=params(),
        cost_estimate=cost(4),
        name="grad_out",
    )(x, up, dn)


def mix_kernel(w, fwd, bwd):
    for dst, x in ((fwd, w[...].T), (bwd, w[...])):
        hi, lo = halves(x)
        dst[0:128, 0:128] = hi
        dst[128:256, 0:128] = hi
        dst[0:128, 128:256] = lo
        dst[128:256, 128:256] = jnp.zeros((128, 128), BF)


def mixes(w):
    return pl.pallas_call(
        mix_kernel,
        out_shape=(sds(256, 256, dtype=BF), sds(256, 256, dtype=BF)),
        in_specs=[VM],
        out_specs=(VM, VM),
        name="mixes",
    )(w)


def put(v, r, j, new):
    v[r, pl.ds(OFF + 128 * j, 128), :] = new
    if j == 0:
        v[r, pl.ds(OFF + LON, 1), :] = new[0:1]
    if j == 3:
        v[r, pl.ds(OFF - 1, 1), :] = new[127:128]


def put_halves(h, r, j, new):
    hi, lo = halves(new)
    h[r, pl.ds(128 * j, 128), 0:128] = hi
    h[r, pl.ds(128 * j, 128), 128:256] = lo


def around(v, r, j):
    at = OFF + 128 * j
    n = v[r - 1, pl.ds(at, 128), :] + v[r + 1, pl.ds(at, 128), :]
    return n + (v[r, pl.ds(at - 1, 128), :] + v[r, pl.ds(at + 1, 128), :])


def mixed(h, w2, r, j):
    y = jnp.dot(h[r, pl.ds(128 * j, 128), :], w2[...], preferred_element_type=F32)
    return y[:, 0:128] + y[:, 128:256]


def rows(lo, hi, body):
    def step(r, carry):
        for j in range(4):
            body(r, j)
        return carry

    lax.fori_loop(lo, hi, step, 0)


def forward_step(va, vb, h, d, w2, lo, hi, first=False, last=False):
    def body(r, j):
        y = mixed(h, w2, r, j)
        c = va[r, pl.ds(OFF + 128 * j, 128), :]
        dd = d[r, pl.ds(128 * j, 128), :]
        n = dd * (around(va, r, j) - 4.0 * c)
        if first:
            c = jnp.where(dd > 0.0, c, 0.0)
        new = (c + n) + y
        put(vb, r, j, new)
        if not last:
            put_halves(h, r, j, new)

    rows(lo, hi, body)


def push_step(ga, gb, u, h, d, w2, s, last=False):
    def body(r, j):
        y = mixed(h, w2, r, j)
        at = pl.ds(128 * j, 128)
        n = around(ga, r, j) - 4.0 * ga[r, pl.ds(OFF + 128 * j, 128), :]
        c = u[r, at, :]
        if last:
            u[r, at, :] = (c + n) + y
        else:
            dd = d[r, at, :]
            new = (c + jnp.where(dd > 0.0, n, 0.0)) + y
            u[r, at, :] = new
            put(gb, r, j, dd * new)
            put_halves(h, r, j, new)

    rows(5 - s, 13 + s, body)


def load_diffusion(d, full, up, dn):
    for src, r0, n in ((up, 2, 3), (full, 5, 8), (dn, 13, 3)):

        def cp(i, carry, src=src, r0=r0):
            d[r0 + i] = src[i]
            return carry

        lax.fori_loop(0, n, cp, 0)


def clear_outside(ga, gb, u, h):
    def clear(i, carry):
        r = jnp.where(i < 5, i, i + 8)
        ga[r] = jnp.zeros((PAD, 128), F32)
        gb[r] = jnp.zeros((PAD, 128), F32)
        u[r] = jnp.zeros((LON, 128), F32)
        h[r] = jnp.zeros((LON, 256), BF)
        return carry

    lax.fori_loop(0, 10, clear, 0)


def lanes():
    return lax.broadcasted_iota(jnp.int32, (128, 128), 1)


def gather_surface(read, count):
    def step(r, acc):
        for j in range(4):
            p = 4 * r + j
            acc = jnp.where(lanes() == p, pltpu.roll(read(r, j), p, 1), acc)
        return acc

    return lax.fori_loop(0, count, step, jnp.zeros((128, 128), F32)).T


def spread_column(cols, p):
    return jnp.where(lanes() == 0, pltpu.roll(cols, (128 - p) % 128, 1), 0.0)


BLOCK_SCRATCH = [
    pltpu.VMEM((NR, PAD, 128), F32),
    pltpu.VMEM((NR, PAD, 128), F32),
    pltpu.VMEM((NR, LON, 256), BF),
    pltpu.VMEM((NR, LON, 128), F32),
]


def first_kernel(top, bot, hu, hd, dt, du, dn, w2, o_top, o_bot, o_surf, va, vb, h, d):
    load_diffusion(d, dt, du, dn)
    for src, r0 in ((hu, 1), (top, 5), (bot, 9), (hd, 13)):

        def cp(i, carry, src=src, r0=r0):
            for j in range(4):
                x = src[i, pl.ds(128 * j, 128), :]
                put(va, r0 + i, j, x)
                keep = d[r0 + i, pl.ds(128 * j, 128), :] > 0.0
                put_halves(h, r0 + i, j, jnp.where(keep, x, 0.0))
            return carry

        lax.fori_loop(0, 4, cp, 0)
    forward_step(va, vb, h, d, w2, 2, 16, first=True)
    forward_step(vb, va, h, d, w2, 3, 15)
    forward_step(va, vb, h, d, w2, 4, 14)
    forward_step(vb, va, h, d, w2, 5, 13, last=True)

    def out(i, carry):
        o_top[i] = va[5 + i, pl.ds(OFF, LON), :]
        o_bot[i] = va[9 + i, pl.ds(OFF, LON), :]
        return carry

    lax.fori_loop(0, 4, out, 0)
    o_surf[...] = gather_surface(lambda r, j: va[r + 5, pl.ds(OFF + 128 * j, 128), :], 8)[0:32]


def first_block(*args):
    return pl.pallas_call(
        first_kernel,
        out_shape=(sds(4, LON, LEV), sds(4, LON, LEV), sds(32, 128)),
        in_specs=[VM] * 8,
        out_specs=(VM,) * 3,
        scratch_shapes=BLOCK_SCRATCH,
        compiler_params=params(),
        cost_estimate=cost(15),
        name="first_block",
    )(*args)


def middle_kernel(
    top, bot, hu, hd, s, su, sd, dt, du, dn, m, w2f, w2b,
    o_final, o_adj, o_up, o_dn, o_s, o_su, o_sd, va, vb, h, d, u, cols,
):
    load_diffusion(d, dt, du, dn)
    cols[0:16] = su[...]
    cols[16:48] = s[...]
    cols[48:64] = sd[...]
    cols[64:128] = jnp.zeros((64, 128), F32)
    cols[...] = cols[...].T
    for src, r0 in ((hu, 1), (top, 5), (bot, 9), (hd, 13)):

        def cp(i, carry, src=src, r0=r0):
            for j in range(4):
                x = src[i, pl.ds(128 * j, 128), :]
                x = x + spread_column(cols[...], 4 * (r0 - 1 + i) + j)
                put(va, r0 + i, j, x)
                put_halves(h, r0 + i, j, x)
            return carry

        lax.fori_loop(0, 4, cp, 0)
    forward_step(va, vb, h, d, w2f, 2, 16)
    forward_step(vb, va, h, d, w2f, 3, 15)
    forward_step(va, vb, h, d, w2f, 4, 14)
    forward_step(vb, va, h, d, w2f, 5, 13, last=True)
    clear_outside(va, vb, u, h)

    def body(r, j):
        at = pl.ds(128 * j, 128)
        x = va[r, pl.ds(OFF + 128 * j, 128), :]
        o_final[r - 5, at, :] = x
        x = x - m[r - 5, at, :]
        dd = d[r, at, :]
        x = jnp.where(dd > 0.0, x, 0.0)
        u[r, at, :] = x
        put(vb, r, j, dd * x)
        put_halves(h, r, j, x)

    rows(5, 13, body)
    push_step(vb, va, u, h, d, w2b, 1)
    push_step(va, vb, u, h, d, w2b, 2)
    push_step(vb, va, u, h, d, w2b, 3)
    push_step(va, vb, u, h, d, w2b, 4, last=True)

    def out(i, carry):
        o_up[i] = u[1 + i]
        o_adj[i] = u[5 + i]
        o_adj[4 + i] = u[9 + i]
        o_dn[i] = u[13 + i]
        return carry

    lax.fori_loop(0, 4, out, 0)
    g = gather_surface(lambda r, j: u[r + 1, pl.ds(128 * j, 128), :], 16)
    o_su[...] = g[0:16]
    o_s[...] = g[16:48]
    o_sd[...] = g[48:64]


def middle_block(*args):
    return pl.pallas_call(
        middle_kernel,
        out_shape=(
            sds(8, LON, LEV), sds(8, LON, LEV), sds(4, LON, LEV), sds(4, LON, LEV),
            sds(32, 128), sds(16, 128), sds(16, 128),
        ),
        in_specs=[VM] * 13,
        out_specs=(VM,) * 7,
        scratch_shapes=BLOCK_SCRATCH
        + [pltpu.VMEM((NR, LON, 128), F32), pltpu.VMEM((128, 128), F32)],
        compiler_params=params(),
        cost_estimate=cost(30),
        name="middle_block",
    )(*args)


def last_kernel(
    adj, ru, rd, s, top, bot, dt, du, dn, w2b, o_base, o_up, o_dn, va, vb, h, d, u, cols
):
    load_diffusion(d, dt, du, dn)
    clear_outside(va, vb, u, h)
    cols[0:32] = s[...]
    cols[32:128] = jnp.zeros((96, 128), F32)
    cols[...] = cols[...].T
    for src, r0 in ((ru, 5), (rd, 9)):

        def cp(i, carry, src=src, r0=r0):
            r = r0 + i
            for j in range(4):
                at = pl.ds(128 * j, 128)
                x = adj[r - 5, at, :] + src[i, at, :]
                x = x + spread_column(cols[...], 4 * (r - 5) + j)
                dd = d[r, at, :]
                x = jnp.where(dd > 0.0, x, 0.0)
                u[r, at, :] = x
                put(vb, r, j, dd * x)
                put_halves(h, r, j, x)
            return carry

        lax.fori_loop(0, 4, cp, 0)
    push_step(vb, va, u, h, d, w2b, 1)
    push_step(va, vb, u, h, d, w2b, 2)
    push_step(vb, va, u, h, d, w2b, 3)
    push_step(va, vb, u, h, d, w2b, 4, last=True)

    def out(i, carry):
        o_up[i] = u[1 + i]
        o_base[i] = u[5 + i] + top[i]
        o_base[4 + i] = u[9 + i] + bot[i]
        o_dn[i] = u[13 + i]
        return carry

    lax.fori_loop(0, 4, out, 0)


def last_block(*args):
    return pl.pallas_call(
        last_kernel,
        out_shape=(sds(8, LON, LEV), sds(4, LON, LEV), sds(4, LON, LEV)),
        in_specs=[VM] * 10,
        out_specs=(VM,) * 3,
        scratch_shapes=BLOCK_SCRATCH
        + [pltpu.VMEM((NR, LON, 128), F32), pltpu.VMEM((128, 128), F32)],
        compiler_params=params(),
        cost_estimate=cost(15),
        name="last_block",
    )(*args)


def offer_kernel(me, send_rows, surf, o):
    o[...] = jnp.zeros((512, 128), F32)
    for off in OFFSETS:
        t = lax.rem(me[0] + (off + 64), 64) * 8
        for q in range(8):
            o[pl.ds(t + q, 1), :] = surf[pl.ds(send_rows[t + q], 1), :]


def offer(me, send_rows, surf):
    return pl.pallas_call(
        offer_kernel,
        out_shape=sds(512, 128),
        in_specs=[SM, SM, VM],
        out_specs=VM,
        name="offer",
    )(me, send_rows, surf)


def remap_kernel(pick, live, dest, arrived, w, sea, o):
    def step(i, acc):
        for k in range(4):
            b = 4 * i + k
            x = arrived[pl.ds(pick[b], 1), :]
            red = jnp.sum(w[b] * x, axis=1, keepdims=True)
            where = jnp.where(live[b] > 0, dest[b], -1)
            acc = acc + jnp.where(lanes() == where, red, 0.0)
        return acc

    acc = lax.fori_loop(0, 16, step, jnp.zeros((128, 128), F32))
    o[...] = acc.T[0:32] * sea[...]


def remap(pick, live, dest, arrived, w, sea):
    return pl.pallas_call(
        remap_kernel,
        out_shape=sds(32, 128),
        in_specs=[SM, SM, SM, VM, VM, VM],
        out_specs=VM,
        compiler_params=params(),
        cost_estimate=cost(3),
        name="remap",
    )(pick, live, dest, arrived, w, sea)


def remap_back_kernel(pick, live, dest, s, ru, rd, w, sea, o, cols, wide):
    cols[0:16] = (s[0:16] + ru[...]) * sea[0:16]
    cols[16:32] = (s[16:32] + rd[...]) * sea[16:32]
    cols[32:128] = jnp.zeros((96, 128), F32)
    cols[...] = cols[...].T
    for p in range(32):
        wide[p] = jnp.broadcast_to(cols[:, p : p + 1], (128, 128))
    o[...] = jnp.zeros((512, 128), F32)

    def step(i, carry):
        for k in range(4):
            b = 4 * i + k
            red = jnp.sum(w[b] * wide[dest[b]], axis=0, keepdims=True)
            o[pl.ds(pick[b], 1), :] = jnp.where(live[b] > 0, red, 0.0)
        return carry

    lax.fori_loop(0, 16, step, 0)


def remap_back(pick, live, dest, s, ru, rd, w, sea):
    return pl.pallas_call(
        remap_back_kernel,
        out_shape=sds(512, 128),
        in_specs=[SM, SM, SM, VM, VM, VM, VM, VM],
        out_specs=VM,
        scratch_shapes=[pltpu.VMEM((128, 128), F32), pltpu.VMEM((32, 128, 128), F32)],
        compiler_params=params(),
        cost_estimate=cost(3),
        name="remap_back",
    )(pick, live, dest, s, ru, rd, w, sea)


def collect_kernel(me, send_rows, got, o):
    o[...] = jnp.zeros((32, 128), F32)
    for off in OFFSETS:
        t = lax.rem(me[0] + (off + 64), 64) * 8
        for q in range(8):
            at = pl.ds(send_rows[t + q], 1)
            o[at, :] = o[at, :] + got[pl.ds(t + q, 1), :]


def collect(me, send_rows, got):
    return pl.pallas_call(
        collect_kernel,
        out_shape=sds(32, 128),
        in_specs=[SM, SM, VM],
        out_specs=VM,
        name="collect",
    )(me, send_rows, got)


def shards(
    starting_perturbation,
    measured_discrepancy,
    diffusion,
    vert_mix,
    ocean_mask,
    pair_tile,
    pair_patch,
    dest_patch,
    pair_blocks,
    remap_weight,
):
    component = lax.axis_index("comp")
    own_tile = lax.axis_index("tile")
    down_pairs = [(i, i + 1) for i in range(63)]
    up_pairs = [(i + 1, i) for i in range(63)]

    def to_next(x):
        return lax.ppermute(x, "tile", down_pairs)

    def to_prev(x):
        return lax.ppermute(x, "tile", up_pairs)

    def swap(x):
        return lax.ppermute(x, "comp", [(0, 1), (1, 0)])

    def exchange(x):
        x = x.reshape(64, 8, 128)
        x = lax.all_to_all(x, "tile", split_axis=0, concat_axis=0, tiled=True)
        return x.reshape(512, 128)

    start = starting_perturbation.reshape(1024, LON)
    s_top, s_bot = start_in(start)
    s_hu, s_hd = to_next(s_bot), to_prev(s_top)
    sea = jnp.where(component == 1, ocean_mask.astype(F32), 1.0)
    sea32 = sea.reshape(32, 128)
    dt, d_top, d_bot = diff_in(diffusion.reshape(1024, LON), sea)
    du, dd = to_next(d_bot), to_prev(d_top)
    w2f, w2b = mixes(vert_mix[0])

    slots = jnp.arange(64, dtype=jnp.int32)
    pick = jnp.repeat(pair_tile[component, own_tile], 8) * 8 + slots % 8
    live = (slots % 8 < jnp.repeat(pair_blocks[0, 0], 8)).astype(jnp.int32)
    dest = dest_patch[0, 0]
    hits = (pair_tile[component] == own_tile).astype(jnp.int32)
    sources = pair_patch[component].reshape(64, 8, 8)
    send_rows = jnp.sum(hits[:, :, None] * sources, axis=1).reshape(512)
    me = own_tile.reshape(1)
    weights = remap_weight[0]
    measured = to_rows(measured_discrepancy.reshape(1024, LON))

    v_top, v_bot, surf = first_block(s_top, s_bot, s_hu, s_hd, dt, du, dd, w2f)
    other = swap(surf)
    v_hu, v_hd = to_next(v_bot), to_prev(v_top)
    arrived = exchange(offer(me, send_rows, other))
    fix = remap(pick, live, dest, arrived, weights, sea32)
    f_hu, f_hd = to_next(fix[16:32]), to_prev(fix[0:16])
    final, adj, a_up, a_dn, a0, a0_up, a0_dn = middle_block(
        v_top, v_bot, v_hu, v_hd, fix, f_hu, f_hd, dt, du, dd, measured, w2f, w2b
    )
    r0u, r0d = to_next(a0_dn), to_prev(a0_up)
    ru, rd = to_next(a_dn), to_prev(a_up)
    final_raw = to_raw(final)
    back = exchange(remap_back(pick, live, dest, a0, r0u, r0d, weights, sea32))
    back = swap(collect(me, send_rows, back))
    base, g_up, g_dn = last_block(adj, ru, rd, back, s_top, s_bot, dt, du, dd, w2b)
    gu, gd = to_next(g_dn), to_prev(g_up)
    gradient = grad_out(base, gu, gd)
    shape = starting_perturbation.shape
    return final_raw.reshape(shape), gradient.reshape(shape)


def solution(mesh):
    field = P("comp", None, "tile", None)
    placed = (
        field,
        field,
        field,
        P("comp", None, None),
        P("tile", None),
        P(),
        P(),
        P("comp", "tile", None),
        P("comp", "tile", None),
        P("comp", "tile", None, None),
    )
    return jax.shard_map(
        shards,
        mesh=mesh,
        in_specs=placed,
        out_specs=(field, field),
        check_vma=False,
    )
```

```python
import jax
import jax.numpy as jnp
from jax import lax
from jax.experimental import pallas as pl
from jax.experimental.pallas import tpu as pltpu
from jax.sharding import PartitionSpec as P

F32 = jnp.float32
BF = jnp.bfloat16
LON, LEV = 512, 128
OFF, PAD = 8, 528
NR = 18
VM = pl.BlockSpec(memory_space=pltpu.VMEM)
SM = pl.BlockSpec(memory_space=pltpu.SMEM)
OFFSETS = tuple(range(-7, 8)) + (32,)


def sds(*shape, dtype=F32):
    return jax.ShapeDtypeStruct(shape, dtype)


def cost(us):
    return pl.CostEstimate(flops=int(us * 5e8), bytes_accessed=1 << 20, transcendentals=0)


def params(**kw):
    return pltpu.CompilerParams(vmem_limit_bytes=44 * 2**20, **kw)


def halves(x):
    hi = x.astype(BF)
    return hi, (x - hi.astype(F32)).astype(BF)


def start_in_kernel(x, top, bot):
    for r in range(8):
        dst = top if r < 4 else bot
        dst[r % 4] = x[pl.ds(r, 128, stride=8), :].T


def start_in(x):
    blk = pl.BlockSpec((4, 128, 128), lambda j: (0, j, 0))
    return pl.pallas_call(
        start_in_kernel,
        grid=(4,),
        out_shape=(sds(4, LON, LEV), sds(4, LON, LEV)),
        in_specs=[pl.BlockSpec((1024, 128), lambda j: (0, j))],
        out_specs=(blk, blk),
        compiler_params=params(),
        cost_estimate=cost(4),
        name="start_in",
    )(x)


def diff_in_kernel(x, sea, full, top, bot):
    for r in range(8):
        y = (x[pl.ds(r, 128, stride=8), :] * sea[r : r + 1, :]).T
        full[r] = y
        if r < 3:
            top[r] = y
        if r > 4:
            bot[r - 5] = y


def diff_in(x, sea):
    blk = pl.BlockSpec((3, 128, 128), lambda j: (0, j, 0))
    return pl.pallas_call(
        diff_in_kernel,
        grid=(4,),
        out_shape=(sds(8, LON, LEV), sds(3, LON, LEV), sds(3, LON, LEV)),
        in_specs=[
            pl.BlockSpec((1024, 128), lambda j: (0, j)),
            pl.BlockSpec((8, 128), lambda j: (0, j)),
        ],
        out_specs=(pl.BlockSpec((8, 128, 128), lambda j: (0, j, 0)), blk, blk),
        compiler_params=params(),
        cost_estimate=cost(4),
        name="diff_in",
    )(x, sea)


def to_rows_kernel(x, o):
    for r in range(8):
        o[r] = x[pl.ds(r, 128, stride=8), :].T


def to_rows(x):
    return pl.pallas_call(
        to_rows_kernel,
        grid=(4,),
        out_shape=sds(8, LON, LEV),
        in_specs=[pl.BlockSpec((1024, 128), lambda j: (0, j))],
        out_specs=pl.BlockSpec((8, 128, 128), lambda j: (0, j, 0)),
        compiler_params=params(),
        cost_estimate=cost(4),
        name="to_rows",
    )(x)


def to_raw_kernel(x, o):
    for r in range(8):
        o[pl.ds(r, 128, stride=8), :] = x[r].T


def to_raw(x):
    return pl.pallas_call(
        to_raw_kernel,
        grid=(4,),
        out_shape=sds(1024, LON),
        in_specs=[pl.BlockSpec((8, 128, 128), lambda j: (0, j, 0))],
        out_specs=pl.BlockSpec((1024, 128), lambda j: (0, j)),
        compiler_params=params(),
        cost_estimate=cost(4),
        name="to_raw",
    )(x)


def grad_out_kernel(me, x, up, dn, o):
    for r in range(8):
        add = up[r] if r < 4 else dn[r - 4]
        o[pl.ds(r, 128, stride=8), :] = (x[r] + add).T
    for edge, r0 in ((0, 0), (63, 4)):

        @pl.when(me[0] == edge)
        def _(r0=r0):
            for r in range(r0, r0 + 4):
                o[pl.ds(r, 128, stride=8), :] = x[r].T


def grad_out(me, x, up, dn):
    blk = pl.BlockSpec((4, 128, 128), lambda j: (0, j, 0))
    return pl.pallas_call(
        grad_out_kernel,
        grid=(4,),
        out_shape=sds(1024, LON),
        in_specs=[SM, pl.BlockSpec((8, 128, 128), lambda j: (0, j, 0)), blk, blk],
        out_specs=pl.BlockSpec((1024, 128), lambda j: (0, j)),
        compiler_params=params(),
        cost_estimate=cost(4),
        name="grad_out",
    )(me, x, up, dn)


def mix_kernel(w, fwd, bwd):
    for dst, x in ((fwd, w[...].T), (bwd, w[...])):
        hi, lo = halves(x)
        dst[0:128, 0:128] = hi
        dst[128:256, 0:128] = hi
        dst[0:128, 128:256] = lo
        dst[128:256, 128:256] = jnp.zeros((128, 128), BF)


def mixes(w):
    return pl.pallas_call(
        mix_kernel,
        out_shape=(sds(256, 256, dtype=BF), sds(256, 256, dtype=BF)),
        in_specs=[VM],
        out_specs=(VM, VM),
        name="mixes",
    )(w)


def put(v, r, j, new):
    v[r, pl.ds(OFF + 128 * j, 128), :] = new
    if j == 0:
        v[r, pl.ds(OFF + LON, 1), :] = new[0:1]
    if j == 3:
        v[r, pl.ds(OFF - 1, 1), :] = new[127:128]


def put_halves(h, r, j, new):
    hi, lo = halves(new)
    h[r, pl.ds(128 * j, 128), 0:128] = hi
    h[r, pl.ds(128 * j, 128), 128:256] = lo


def around(v, r, j):
    at = OFF + 128 * j
    n = v[r - 1, pl.ds(at, 128), :] + v[r + 1, pl.ds(at, 128), :]
    return n + (v[r, pl.ds(at - 1, 128), :] + v[r, pl.ds(at + 1, 128), :])


GROUP = {14: 7, 12: 6, 10: 5, 8: 4}


def mixed_rows(h, w2, lo, n, body):
    k = GROUP[n]

    def step(i, carry):
        r0 = lo + k * i
        y = jnp.dot(h[pl.ds(r0, k)].reshape(LON * k, 256), w2[...], preferred_element_type=F32)
        for q in range(k):
            for j in range(4):
                part = y[LON * q + 128 * j : LON * q + 128 * j + 128]
                body(r0 + q, j, part[:, 0:128] + part[:, 128:256])
        return carry

    lax.fori_loop(0, n // k, step, 0)


def forward_step(va, vb, h, d, w2, s, first=False, last=False):
    def body(r, j, y):
        c = va[r, pl.ds(OFF + 128 * j, 128), :]
        dd = d[r, pl.ds(128 * j, 128), :]
        n = dd * (around(va, r, j) - 4.0 * c)
        if first:
            c = jnp.where(dd > 0.0, c, 0.0)
        new = (c + n) + y
        put(vb, r, j, new)
        if not last:
            put_halves(h, r, j, new)

    mixed_rows(h, w2, 1 + s, 16 - 2 * s, body)


def push_step(ga, gb, u, h, d, w2, s, last=False):
    def finish(r, j, new, dd):
        u[r, pl.ds(128 * j, 128), :] = new
        put(gb, r, j, dd * new)
        put_halves(h, r, j, new)

    def body(r, j, y):
        at = pl.ds(128 * j, 128)
        n = around(ga, r, j) - 4.0 * ga[r, pl.ds(OFF + 128 * j, 128), :]
        c = u[r, at, :]
        if last:
            u[r, at, :] = (c + n) + y
        else:
            dd = d[r, at, :]
            finish(r, j, (c + jnp.where(dd > 0.0, n, 0.0)) + y, dd)

    mixed_rows(h, w2, 6 - s, 6 + 2 * s, body)
    for r, near in ((5 - s, 6 - s), (12 + s, 11 + s)):
        for j in range(4):
            at = pl.ds(128 * j, 128)
            n = ga[near, pl.ds(OFF + 128 * j, 128), :]
            if last:
                u[r, at, :] = n
            else:
                dd = d[r, at, :]
                finish(r, j, jnp.where(dd > 0.0, n, 0.0), dd)


def push_block(ga, gb, u, h, d, w2):
    for s, g in ((1, ga), (2, gb), (3, ga), (4, gb)):
        g[5 - s] = jnp.zeros((PAD, 128), F32)
        g[12 + s] = jnp.zeros((PAD, 128), F32)
    push_step(ga, gb, u, h, d, w2, 1)
    push_step(gb, ga, u, h, d, w2, 2)
    push_step(ga, gb, u, h, d, w2, 3)
    push_step(gb, ga, u, h, d, w2, 4, last=True)


def forward_block(va, vb, h, d, w2, first=False):
    forward_step(va, vb, h, d, w2, 1, first=first)
    forward_step(vb, va, h, d, w2, 2)
    forward_step(va, vb, h, d, w2, 3)
    forward_step(vb, va, h, d, w2, 4, last=True)


def copies(sems, pairs):
    out = [pltpu.make_async_copy(a, b, sems.at[i]) for i, (a, b) in enumerate(pairs)]
    for c in out:
        c.start()
    return out


def wait(*todo):
    for c in todo:
        c.wait()


def tile_rows(v, r0, n):
    return v.at[pl.ds(r0, n), pl.ds(OFF, LON), :]


def clear_ends(me, up, dn):
    for edge, todo in ((0, up), (63, dn)):

        @pl.when(me[0] == edge)
        def _(todo=todo):
            for ref, r0, n in todo:
                ref[pl.ds(r0, n)] = jnp.zeros((n,) + ref.shape[1:], F32)


def lanes():
    return lax.broadcasted_iota(jnp.int32, (128, 128), 1)


def gather_surface(read, count):
    def step(r, acc):
        for j in range(4):
            p = 4 * r + j
            acc = jnp.where(lanes() == p, pltpu.roll(read(r, j), p, 1), acc)
        return acc

    return lax.fori_loop(0, count, step, jnp.zeros((128, 128), F32)).T


def spread_column(cols, p):
    return jnp.where(lanes() == 0, pltpu.roll(cols, (128 - p) % 128, 1), 0.0)


BLOCK_SCRATCH = [
    pltpu.VMEM((NR, PAD, 128), F32),
    pltpu.VMEM((NR, PAD, 128), F32),
    pltpu.VMEM((NR, LON, 256), BF),
    pltpu.VMEM((NR, LON, 128), F32),
]
U_SCRATCH = pltpu.VMEM((NR, LON, 128), F32)
COLS = pltpu.VMEM((128, 128), F32)
ANY = pl.BlockSpec(memory_space=pl.ANY)


def dma_sems(n):
    return pltpu.SemaphoreType.DMA((n,))


def first_kernel(me, top, bot, hu, hd, dt, du, dn, w2, o_top, o_bot, o_surf, va, vb, h, d, sems):
    c = copies(
        sems,
        [
            (dt, d.at[pl.ds(5, 8)]),
            (top, tile_rows(va, 5, 4)),
            (bot, tile_rows(va, 9, 4)),
            (du, d.at[pl.ds(2, 3)]),
            (hu, tile_rows(va, 1, 4)),
            (dn, d.at[pl.ds(13, 3)]),
            (hd, tile_rows(va, 13, 4)),
        ],
    )

    def prepare(r0, n):
        def cp(i, carry):
            r = r0 + i
            for j in range(4):
                x = va[r, pl.ds(OFF + 128 * j, 128), :]
                if j == 0:
                    va[r, pl.ds(OFF + LON, 1), :] = x[0:1]
                if j == 3:
                    va[r, pl.ds(OFF - 1, 1), :] = x[127:128]
                keep = d[r, pl.ds(128 * j, 128), :] > 0.0
                put_halves(h, r, j, jnp.where(keep, x, 0.0))
            return carry

        lax.fori_loop(0, n, cp, 0)

    wait(c[0], c[1])
    prepare(5, 4)
    wait(c[2])
    prepare(9, 4)
    wait(*c[3:])
    clear_ends(me, ((va, 1, 4), (d, 2, 3)), ((va, 13, 4), (d, 13, 3)))
    prepare(2, 3)
    prepare(13, 3)
    forward_block(va, vb, h, d, w2, first=True)
    c = copies(sems, [(tile_rows(va, 5, 4), o_top), (tile_rows(va, 9, 4), o_bot)])
    o_surf[...] = gather_surface(lambda r, j: va[r + 5, pl.ds(OFF + 128 * j, 128), :], 8)[0:32]
    wait(*c)


def first_block(*args):
    return pl.pallas_call(
        first_kernel,
        out_shape=(sds(4, LON, LEV), sds(4, LON, LEV), sds(32, 128)),
        in_specs=[SM] + [ANY] * 7 + [VM],
        out_specs=(ANY, ANY, VM),
        scratch_shapes=BLOCK_SCRATCH + [dma_sems(7)],
        compiler_params=params(),
        cost_estimate=cost(15),
        name="first_block",
    )(*args)


def middle_kernel(
    me, top, bot, hu, hd, s, su, sd, dt, du, dn, m, w2f, w2b,
    o_final, o_adj, o_up, o_dn, o_s, o_su, o_sd, va, vb, h, d, u, mm, cols, sems,
):
    c = copies(
        sems,
        [
            (top, tile_rows(va, 5, 4)),
            (bot, tile_rows(va, 9, 4)),
            (hu, tile_rows(va, 1, 4)),
            (hd, tile_rows(va, 13, 4)),
            (dt, d.at[pl.ds(5, 8)]),
            (du, d.at[pl.ds(2, 3)]),
            (dn, d.at[pl.ds(13, 3)]),
            (m, mm),
        ],
    )
    cols[0:16] = su[...]
    cols[16:48] = s[...]
    cols[48:64] = sd[...]
    cols[64:128] = jnp.zeros((64, 128), F32)
    clear_ends(me, ((cols, 0, 16),), ((cols, 48, 16),))
    cols[...] = cols[...].T

    def prepare(r0):
        def cp(i, carry):
            r = r0 + i
            for j in range(4):
                x = va[r, pl.ds(OFF + 128 * j, 128), :]
                x = x + spread_column(cols[...], 4 * (r - 1) + j)
                put(va, r, j, x)
                put_halves(h, r, j, x)
            return carry

        lax.fori_loop(0, 4, cp, 0)

    for i, r0 in ((0, 5), (1, 9)):
        wait(c[i])
        prepare(r0)
    wait(*c[2:7])
    clear_ends(me, ((va, 1, 4), (d, 2, 3)), ((va, 13, 4), (d, 13, 3)))
    prepare(1)
    prepare(13)
    forward_block(va, vb, h, d, w2f)
    out = copies(sems, [(tile_rows(va, 5, 8), o_final)])
    wait(c[7])

    def body(i, carry):
        r = 5 + i
        for j in range(4):
            at = pl.ds(128 * j, 128)
            x = va[r, pl.ds(OFF + 128 * j, 128), :] - mm[i, at, :]
            dd = d[r, at, :]
            x = jnp.where(dd > 0.0, x, 0.0)
            u[r, at, :] = x
            put(vb, r, j, dd * x)
            put_halves(h, r, j, x)
        return carry

    lax.fori_loop(0, 8, body, 0)
    wait(*out)
    push_block(vb, va, u, h, d, w2b)
    out = copies(
        sems,
        [
            (u.at[pl.ds(1, 4)], o_up),
            (u.at[pl.ds(13, 4)], o_dn),
            (u.at[pl.ds(5, 8)], o_adj),
        ],
    )
    g = gather_surface(lambda r, j: u[r + 1, pl.ds(128 * j, 128), :], 16)
    o_su[...] = g[0:16]
    o_s[...] = g[16:48]
    o_sd[...] = g[48:64]
    wait(*out)


def middle_block(*args):
    return pl.pallas_call(
        middle_kernel,
        out_shape=(
            sds(8, LON, LEV), sds(8, LON, LEV), sds(4, LON, LEV), sds(4, LON, LEV),
            sds(32, 128), sds(16, 128), sds(16, 128),
        ),
        in_specs=[SM] + [ANY] * 4 + [VM] * 3 + [ANY] * 4 + [VM] * 2,
        out_specs=(ANY,) * 4 + (VM,) * 3,
        scratch_shapes=BLOCK_SCRATCH
        + [U_SCRATCH, pltpu.VMEM((8, LON, 128), F32), COLS, dma_sems(8)],
        compiler_params=params(),
        cost_estimate=cost(30),
        name="middle_block",
    )(*args)


def last_kernel(
    me, adj, ru, rd, s, top, bot, dt, du, dn, w2b, o_base, o_up, o_dn,
    va, vb, h, d, u, got, base, cols, sems,
):
    c = copies(
        sems,
        [
            (adj, u.at[pl.ds(5, 8)]),
            (dt, d.at[pl.ds(5, 8)]),
            (ru, got.at[pl.ds(0, 4)]),
            (rd, got.at[pl.ds(4, 4)]),
            (du, d.at[pl.ds(2, 3)]),
            (dn, d.at[pl.ds(13, 3)]),
            (top, base.at[pl.ds(0, 4)]),
            (bot, base.at[pl.ds(4, 4)]),
        ],
    )
    cols[0:32] = s[...]
    cols[32:128] = jnp.zeros((96, 128), F32)
    cols[...] = cols[...].T
    wait(*c[0:4])
    clear_ends(me, ((got, 0, 4),), ((got, 4, 4),))

    def cp(i, carry):
        r = 5 + i
        for j in range(4):
            at = pl.ds(128 * j, 128)
            x = u[r, at, :] + got[i, at, :]
            x = x + spread_column(cols[...], 4 * i + j)
            dd = d[r, at, :]
            x = jnp.where(dd > 0.0, x, 0.0)
            u[r, at, :] = x
            put(vb, r, j, dd * x)
            put_halves(h, r, j, x)
        return carry

    lax.fori_loop(0, 8, cp, 0)
    wait(*c[4:8])
    clear_ends(me, ((d, 2, 3),), ((d, 13, 3),))
    push_block(vb, va, u, h, d, w2b)
    out = copies(sems, [(u.at[pl.ds(1, 4)], o_up), (u.at[pl.ds(13, 4)], o_dn)])

    def add(i, carry):
        base[i] = base[i] + u[5 + i]
        return carry

    lax.fori_loop(0, 8, add, 0)
    end = pltpu.make_async_copy(base, o_base, sems.at[2])
    end.start()
    wait(*out)
    end.wait()


def last_block(*args):
    return pl.pallas_call(
        last_kernel,
        out_shape=(sds(8, LON, LEV), sds(4, LON, LEV), sds(4, LON, LEV)),
        in_specs=[SM] + [ANY] * 3 + [VM] + [ANY] * 5 + [VM],
        out_specs=(ANY,) * 3,
        scratch_shapes=BLOCK_SCRATCH
        + [
            U_SCRATCH,
            pltpu.VMEM((8, LON, 128), F32),
            pltpu.VMEM((8, LON, 128), F32),
            COLS,
            dma_sems(8),
        ],
        compiler_params=params(),
        cost_estimate=cost(15),
        name="last_block",
    )(*args)


def offer_kernel(me, send_rows, surf, o):
    o[...] = jnp.zeros((512, 128), F32)
    for off in OFFSETS:
        t = lax.rem(me[0] + (off + 64), 64) * 8
        for q in range(8):
            o[pl.ds(t + q, 1), :] = surf[pl.ds(send_rows[t + q], 1), :]


def offer(me, send_rows, surf):
    return pl.pallas_call(
        offer_kernel,
        out_shape=sds(512, 128),
        in_specs=[SM, SM, VM],
        out_specs=VM,
        name="offer",
    )(me, send_rows, surf)


def fetch_blocks(ids, w, buf, sems):
    for k in range(LIVE):
        pltpu.make_async_copy(w.at[ids[k]], buf.at[k], sems.at[k // 12]).start()


def fetched(w, buf, sems, part):
    pltpu.make_async_copy(w.at[pl.ds(0, 12)], buf.at[pl.ds(12 * part, 12)], sems.at[part]).wait()


LIVE = 48
WEIGHTS = [pltpu.VMEM((LIVE, 128, 128), F32), pltpu.SemaphoreType.DMA((4,))]


def remap_kernel(ids, pick, dest, arrived, w, sea, o, buf, sems):
    fetch_blocks(ids, w, buf, sems)
    acc = jnp.zeros((128, 128), F32)
    for part in range(4):
        fetched(w, buf, sems, part)

        def step(i, acc, part=part):
            for q in range(4):
                k = 12 * part + 4 * i + q
                x = arrived[pl.ds(pick[k], 1), :]
                red = jnp.sum(buf[k] * x, axis=1, keepdims=True)
                acc = acc + jnp.where(lanes() == dest[k], red, 0.0)
            return acc

        acc = lax.fori_loop(0, 3, step, acc)
    o[...] = acc.T[0:32] * sea[...]


def remap(ids, pick, dest, arrived, w, sea):
    return pl.pallas_call(
        remap_kernel,
        out_shape=sds(32, 128),
        in_specs=[SM, SM, SM, VM, ANY, VM],
        out_specs=VM,
        scratch_shapes=WEIGHTS,
        compiler_params=params(),
        cost_estimate=cost(3),
        name="remap",
    )(ids, pick, dest, arrived, w, sea)


def remap_back_kernel(me, ids, pick, dest, s, ru, rd, w, sea, o, cols, wide, buf, sems):
    fetch_blocks(ids, w, buf, sems)
    cols[0:16] = ru[...]
    cols[16:32] = rd[...]
    clear_ends(me, ((cols, 0, 16),), ((cols, 16, 16),))
    cols[0:32] = (cols[0:32] + s[...]) * sea[...]
    cols[32:128] = jnp.zeros((96, 128), F32)
    cols[...] = cols[...].T
    for p in range(32):
        wide[p] = jnp.broadcast_to(cols[:, p : p + 1], (128, 128))
    o[...] = jnp.zeros((512, 128), F32)
    for part in range(4):
        fetched(w, buf, sems, part)

        def step(i, carry, part=part):
            for q in range(4):
                k = 12 * part + 4 * i + q
                red = jnp.sum(buf[k] * wide[dest[k]], axis=0, keepdims=True)
                o[pl.ds(pick[k], 1), :] = red
            return carry

        lax.fori_loop(0, 3, step, 0)


def remap_back(me, ids, pick, dest, s, ru, rd, w, sea):
    return pl.pallas_call(
        remap_back_kernel,
        out_shape=sds(512, 128),
        in_specs=[SM, SM, SM, SM, VM, VM, VM, ANY, VM],
        out_specs=VM,
        scratch_shapes=[COLS, pltpu.VMEM((32, 128, 128), F32)] + WEIGHTS,
        compiler_params=params(),
        cost_estimate=cost(3),
        name="remap_back",
    )(me, ids, pick, dest, s, ru, rd, w, sea)


def collect_kernel(me, send_rows, got, o):
    o[...] = jnp.zeros((32, 128), F32)
    for off in OFFSETS:
        t = lax.rem(me[0] + (off + 64), 64) * 8
        for q in range(8):
            at = pl.ds(send_rows[t + q], 1)
            o[at, :] = o[at, :] + got[pl.ds(t + q, 1), :]


def collect(me, send_rows, got):
    return pl.pallas_call(
        collect_kernel,
        out_shape=sds(32, 128),
        in_specs=[SM, SM, VM],
        out_specs=VM,
        name="collect",
    )(me, send_rows, got)


def shards(
    starting_perturbation,
    measured_discrepancy,
    diffusion,
    vert_mix,
    ocean_mask,
    pair_tile,
    pair_patch,
    dest_patch,
    pair_blocks,
    remap_weight,
):
    component = lax.axis_index("comp")
    own_tile = lax.axis_index("tile")
    down_pairs = [(i, (i + 1) % 64) for i in range(64)]
    up_pairs = [((i + 1) % 64, i) for i in range(64)]

    def to_next(x):
        return lax.ppermute(x, "tile", down_pairs)

    def to_prev(x):
        return lax.ppermute(x, "tile", up_pairs)

    def swap(x):
        return lax.ppermute(x, "comp", [(0, 1), (1, 0)])

    def exchange(x):
        x = x.reshape(64, 8, 128)
        x = lax.all_to_all(x, "tile", split_axis=0, concat_axis=0, tiled=True)
        return x.reshape(512, 128)

    start = starting_perturbation.reshape(1024, LON)
    s_top, s_bot = start_in(start)
    s_hu, s_hd = to_next(s_bot), to_prev(s_top)
    sea = jnp.where(component == 1, ocean_mask.astype(F32), 1.0)
    sea32 = sea.reshape(32, 128)
    dt, d_top, d_bot = diff_in(diffusion.reshape(1024, LON), sea)
    du, dd = to_next(d_bot), to_prev(d_top)
    w2f, w2b = mixes(vert_mix[0])

    slots = jnp.arange(64, dtype=jnp.int32)
    live = slots % 8 < jnp.repeat(pair_blocks[0, 0], 8)
    place = jnp.sum((slots[None, :] < slots[:, None]) & live[None, :], axis=1)
    chosen = ((place[None, :] == slots[:LIVE, None]) & live[None, :]).astype(jnp.int32)
    ids = jnp.sum(chosen * slots[None, :], axis=1)
    pick = jnp.repeat(pair_tile[component, own_tile], 8) * 8 + slots % 8
    pick = jnp.sum(chosen * pick[None, :], axis=1)
    dest = jnp.sum(chosen * dest_patch[0, 0][None, :], axis=1)
    hits = (pair_tile[component] == own_tile).astype(jnp.int32)
    sources = pair_patch[component].reshape(64, 8, 8)
    send_rows = jnp.sum(hits[:, :, None] * sources, axis=1).reshape(512)
    me = own_tile.reshape(1)
    weights = remap_weight[0]
    measured = to_rows(measured_discrepancy.reshape(1024, LON))
    s_hu, s_hd, du, dd, w2f, w2b, ids, pick, dest, send_rows, measured, sea32 = (
        lax.optimization_barrier(
            (s_hu, s_hd, du, dd, w2f, w2b, ids, pick, dest, send_rows, measured, sea32)
        )
    )

    v_top, v_bot, surf = first_block(me, s_top, s_bot, s_hu, s_hd, dt, du, dd, w2f)
    other = swap(surf)
    v_top, v_bot, other = lax.optimization_barrier((v_top, v_bot, other))
    v_hu, v_hd = to_next(v_bot), to_prev(v_top)
    arrived = exchange(offer(me, send_rows, other))
    fix = remap(ids, pick, dest, arrived, weights, sea32)
    f_hu, f_hd = to_next(fix[16:32]), to_prev(fix[0:16])
    final, adj, a_up, a_dn, a0, a0_up, a0_dn = middle_block(
        me, v_top, v_bot, v_hu, v_hd, fix, f_hu, f_hd, dt, du, dd, measured, w2f, w2b
    )
    r0u, r0d = to_next(a0_dn), to_prev(a0_up)
    a_up, a_dn, r0u, r0d = lax.optimization_barrier((a_up, a_dn, r0u, r0d))
    ru, rd = to_next(a_dn), to_prev(a_up)
    back = exchange(remap_back(me, ids, pick, dest, a0, r0u, r0d, weights, sea32))
    back = swap(collect(me, send_rows, back))
    base, g_up, g_dn = last_block(me, adj, ru, rd, back, s_top, s_bot, dt, du, dd, w2b)
    gu, gd = to_next(g_dn), to_prev(g_up)
    final_raw = to_raw(final)
    gradient = grad_out(me, base, gu, gd)
    shape = starting_perturbation.shape
    return final_raw.reshape(shape), gradient.reshape(shape)


def solution(mesh):
    field = P("comp", None, "tile", None)
    placed = (
        field,
        field,
        field,
        P("comp", None, None),
        P("tile", None),
        P(),
        P(),
        P("comp", "tile", None),
        P("comp", "tile", None),
        P("comp", "tile", None, None),
    )
    return jax.shard_map(
        shards,
        mesh=mesh,
        in_specs=placed,
        out_specs=(field, field),
        check_vma=False,
    )
```

```python
import jax
import jax.numpy as jnp
from jax import lax
from jax.experimental import pallas as pl
from jax.experimental.pallas import tpu as pltpu
from jax.sharding import PartitionSpec as P


F32 = jnp.float32
BF = jnp.bfloat16
LON, LEV = 512, 128
OFF, PAD = 8, 528
NR = 18
VM = pl.BlockSpec(memory_space=pltpu.VMEM)
SM = pl.BlockSpec(memory_space=pltpu.SMEM)
OFFSETS = tuple(range(-7, 8)) + (32,)


def sds(*shape, dtype=F32):
    return jax.ShapeDtypeStruct(shape, dtype)


def cost(us):
    return pl.CostEstimate(flops=int(us * 5e8), bytes_accessed=1 << 20, transcendentals=0)


def params(**kw):
    return pltpu.CompilerParams(vmem_limit_bytes=60 * 2**20, **kw)


def halves(x):
    hi = x.astype(BF)
    return hi, (x - hi.astype(F32)).astype(BF)


ANY = pl.BlockSpec(memory_space=pltpu.MemorySpace.HBM)
RAW = pltpu.VMEM((4, 1024, 128), F32)
ROWS = pltpu.VMEM((8, LON, LEV), F32)


def dma_sems(*n):
    return pltpu.SemaphoreType.DMA(n)


def lon_part(ref, j):
    return ref.at[:, pl.ds(128 * j, 128), :]


def start_raw(x, buf, sems):
    out = [
        pltpu.make_async_copy(x.at[:, pl.ds(128 * j, 128)], buf.at[j], sems.at[j])
        for j in range(4)
    ]
    for c in out:
        c.start()
    return out


def turned(buf, j, r):
    return buf[j, pl.ds(r, 128, stride=8), :].T


def start_in_kernel(x, top, bot, buf, out, sems, osems):
    c = start_raw(x, buf, sems)
    todo = []
    for j in range(4):
        c[j].wait()
        for r in range(8):
            out[r, pl.ds(128 * j, 128), :] = turned(buf, j, r)
        for i, dst in enumerate((top, bot)):
            src = out.at[pl.ds(4 * i, 4), pl.ds(128 * j, 128), :]
            todo.append(pltpu.make_async_copy(src, lon_part(dst, j), osems.at[i, j]))
            todo[-1].start()
    for d in todo:
        d.wait()


def start_in(x):
    return pl.pallas_call(
        start_in_kernel,
        out_shape=(sds(4, LON, LEV), sds(4, LON, LEV)),
        in_specs=[ANY],
        out_specs=(ANY, ANY),
        scratch_shapes=[RAW, ROWS, dma_sems(4), dma_sems(2, 4)],
        compiler_params=params(),
        cost_estimate=cost(4),
        name="start_in",
    )(x)


def diff_in_kernel(x, sea, full, top, bot, buf, out, sems, osems):
    c = start_raw(x, buf, sems)
    todo = []
    for j in range(4):
        c[j].wait()
        at = pl.ds(128 * j, 128)
        for r in range(8):
            out[r, at, :] = (buf[j, pl.ds(r, 128, stride=8), :] * sea[r : r + 1, at]).T
        for i, (r0, n, dst) in enumerate(((0, 3, top), (5, 3, bot), (0, 8, full))):
            src = out.at[pl.ds(r0, n), at, :]
            todo.append(pltpu.make_async_copy(src, lon_part(dst, j), osems.at[i, j]))
            todo[-1].start()
    for d in todo:
        d.wait()


def diff_in(x, sea):
    return pl.pallas_call(
        diff_in_kernel,
        out_shape=(sds(8, LON, LEV), sds(3, LON, LEV), sds(3, LON, LEV)),
        in_specs=[ANY, VM],
        out_specs=(ANY,) * 3,
        scratch_shapes=[RAW, ROWS, dma_sems(4), dma_sems(3, 4)],
        compiler_params=params(),
        cost_estimate=cost(4),
        name="diff_in",
    )(x, sea)


def to_rows_kernel(x, o, buf, out, sems, osems):
    c = start_raw(x, buf, sems)
    todo = []
    for j in range(4):
        c[j].wait()
        for r in range(8):
            out[r, pl.ds(128 * j, 128), :] = turned(buf, j, r)
        todo.append(pltpu.make_async_copy(lon_part(out, j), lon_part(o, j), osems.at[j]))
        todo[-1].start()
    for d in todo:
        d.wait()


def to_rows(x):
    return pl.pallas_call(
        to_rows_kernel,
        out_shape=sds(8, LON, LEV),
        in_specs=[ANY],
        out_specs=ANY,
        scratch_shapes=[RAW, ROWS, dma_sems(4), dma_sems(4)],
        compiler_params=params(),
        cost_estimate=cost(4),
        name="to_rows",
    )(x)


def to_raw_kernel(x, o):
    for r in range(8):
        o[pl.ds(r, 128, stride=8), :] = x[r].T


def to_raw(x):
    return pl.pallas_call(
        to_raw_kernel,
        grid=(4,),
        out_shape=sds(1024, LON),
        in_specs=[pl.BlockSpec((8, 128, 128), lambda j: (0, j, 0))],
        out_specs=pl.BlockSpec((1024, 128), lambda j: (0, j)),
        compiler_params=params(),
        cost_estimate=cost(4),
        name="to_raw",
    )(x)


def grad_out_kernel(me, x, up, dn, o, base, add, buf, sems, osems):
    c = []
    for j in range(4):
        at = pl.ds(128 * j, 128)
        for i, (src, dst) in enumerate(
            (
                (lon_part(up, j), add.at[pl.ds(0, 4), at, :]),
                (lon_part(dn, j), add.at[pl.ds(4, 4), at, :]),
                (lon_part(x, j), lon_part(base, j)),
            )
        ):
            c.append(pltpu.make_async_copy(src, dst, sems.at[i, j]))
            c[-1].start()
    keep_up = jnp.where(me[0] > 0, 1.0, 0.0)
    keep_dn = jnp.where(me[0] < 63, 1.0, 0.0)
    todo = []
    for j in range(4):
        at = pl.ds(128 * j, 128)
        for d in c[3 * j : 3 * j + 3]:
            d.wait()
        for r in range(8):
            keep = keep_up if r < 4 else keep_dn
            buf[j, pl.ds(r, 128, stride=8), :] = (base[r, at, :] + keep * add[r, at, :]).T
        todo.append(pltpu.make_async_copy(buf.at[j], o.at[:, at], osems.at[j]))
        todo[-1].start()
    for d in todo:
        d.wait()


def grad_out(me, x, up, dn):
    return pl.pallas_call(
        grad_out_kernel,
        out_shape=sds(1024, LON),
        in_specs=[SM, ANY, ANY, ANY],
        out_specs=ANY,
        scratch_shapes=[ROWS, ROWS, RAW, dma_sems(3, 4), dma_sems(4)],
        compiler_params=params(),
        cost_estimate=cost(4),
        name="grad_out",
    )(me, x, up, dn)


def mix_kernel(w, fwd, bwd):
    for dst, x in ((fwd, w[...].T), (bwd, w[...])):
        hi, lo = halves(x)
        dst[0:128, 0:128] = hi
        dst[128:256, 0:128] = hi
        dst[0:128, 128:256] = lo
        dst[128:256, 128:256] = jnp.zeros((128, 128), BF)


def mixes(w):
    return pl.pallas_call(
        mix_kernel,
        out_shape=(sds(256, 256, dtype=BF), sds(256, 256, dtype=BF)),
        in_specs=[VM],
        out_specs=(VM, VM),
        name="mixes",
    )(w)


def put(v, r, j, new):
    v[r, pl.ds(OFF + 128 * j, 128), :] = new
    if j == 0:
        v[r, pl.ds(OFF + LON, 1), :] = new[0:1]
    if j == 3:
        v[r, pl.ds(OFF - 1, 1), :] = new[127:128]


def put_halves(h, r, j, new):
    hi, lo = halves(new)
    h[r, pl.ds(128 * j, 128), 0:128] = hi
    h[r, pl.ds(128 * j, 128), 128:256] = lo


def around(v, r, j):
    at = OFF + 128 * j
    n = v[r - 1, pl.ds(at, 128), :] + v[r + 1, pl.ds(at, 128), :]
    return n + (v[r, pl.ds(at - 1, 128), :] + v[r, pl.ds(at + 1, 128), :])


GROUP = {14: 7, 12: 6, 10: 5, 8: 4}


def mixed_rows(h, w2, lo, n, body):
    k = GROUP[n]

    def step(i, carry):
        r0 = lo + k * i
        y = jnp.dot(h[pl.ds(r0, k)].reshape(LON * k, 256), w2[...], preferred_element_type=F32)
        for q in range(k):
            for j in range(4):
                part = y[LON * q + 128 * j : LON * q + 128 * j + 128]
                body(r0 + q, j, part[:, 0:128] + part[:, 128:256])
        return carry

    lax.fori_loop(0, n // k, step, 0)


def forward_step(va, vb, h, d, w2, s, first=False, last=False):
    def body(r, j, y):
        c = va[r, pl.ds(OFF + 128 * j, 128), :]
        dd = d[r, pl.ds(128 * j, 128), :]
        n = dd * (around(va, r, j) - 4.0 * c)
        if first:
            c = jnp.where(dd > 0.0, c, 0.0)
        new = (c + n) + y
        put(vb, r, j, new)
        if not last:
            put_halves(h, r, j, new)

    mixed_rows(h, w2, 1 + s, 16 - 2 * s, body)


def push_step(ga, gb, u, h, d, w2, s, last=False):
    def finish(r, j, new, dd):
        u[r, pl.ds(128 * j, 128), :] = new
        put(gb, r, j, dd * new)
        put_halves(h, r, j, new)

    def body(r, j, y):
        at = pl.ds(128 * j, 128)
        n = around(ga, r, j) - 4.0 * ga[r, pl.ds(OFF + 128 * j, 128), :]
        c = u[r, at, :]
        if last:
            u[r, at, :] = (c + n) + y
        else:
            dd = d[r, at, :]
            finish(r, j, (c + jnp.where(dd > 0.0, n, 0.0)) + y, dd)

    mixed_rows(h, w2, 6 - s, 6 + 2 * s, body)
    for r, near in ((5 - s, 6 - s), (12 + s, 11 + s)):
        for j in range(4):
            at = pl.ds(128 * j, 128)
            n = ga[near, pl.ds(OFF + 128 * j, 128), :]
            if last:
                u[r, at, :] = n
            else:
                dd = d[r, at, :]
                finish(r, j, jnp.where(dd > 0.0, n, 0.0), dd)


def push_block(ga, gb, u, h, d, w2):
    for s, g in ((1, ga), (2, gb), (3, ga), (4, gb)):
        g[5 - s] = jnp.zeros((PAD, 128), F32)
        g[12 + s] = jnp.zeros((PAD, 128), F32)
    push_step(ga, gb, u, h, d, w2, 1)
    push_step(gb, ga, u, h, d, w2, 2)
    push_step(ga, gb, u, h, d, w2, 3)
    push_step(gb, ga, u, h, d, w2, 4, last=True)


def forward_block(va, vb, h, d, w2, first=False):
    forward_step(va, vb, h, d, w2, 1, first=first)
    forward_step(vb, va, h, d, w2, 2)
    forward_step(va, vb, h, d, w2, 3)
    forward_step(vb, va, h, d, w2, 4, last=True)


def copies(sems, pairs):
    out = [pltpu.make_async_copy(a, b, sems.at[i]) for i, (a, b) in enumerate(pairs)]
    for c in out:
        c.start()
    return out


def wait(*todo):
    for c in todo:
        c.wait()


def tile_rows(v, r0, n):
    return v.at[pl.ds(r0, n), pl.ds(OFF, LON), :]


def clear_ends(me, up, dn):
    for edge, todo in ((0, up), (63, dn)):

        @pl.when(me[0] == edge)
        def _(todo=todo):
            for ref, r0, n in todo:
                ref[pl.ds(r0, n)] = jnp.zeros((n,) + ref.shape[1:], F32)


def lanes():
    return lax.broadcasted_iota(jnp.int32, (128, 128), 1)


def gather_surface(read, count):
    def step(r, acc):
        for j in range(4):
            p = 4 * r + j
            acc = jnp.where(lanes() == p, pltpu.roll(read(r, j), p, 1), acc)
        return acc

    return lax.fori_loop(0, count, step, jnp.zeros((128, 128), F32)).T


def spread_column(cols, p):
    return jnp.where(lanes() == 0, pltpu.roll(cols, (128 - p) % 128, 1), 0.0)


BLOCK_SCRATCH = [
    pltpu.VMEM((NR, PAD, 128), F32),
    pltpu.VMEM((NR, PAD, 128), F32),
    pltpu.VMEM((NR, LON, 256), BF),
    pltpu.VMEM((NR, LON, 128), F32),
]
U_SCRATCH = pltpu.VMEM((NR, LON, 128), F32)
COLS = pltpu.VMEM((128, 128), F32)
HALF = sds(2, LON, LEV)


def first_kernel(me, top, bot, hu, hd, dt, du, dn, w2, o_t0, o_t1, o_b0, o_b1, o_surf, va, vb, h, d, sems):
    c = copies(
        sems,
        [
            (dt, d.at[pl.ds(5, 8)]),
            (top, tile_rows(va, 5, 4)),
            (bot, tile_rows(va, 9, 4)),
            (du, d.at[pl.ds(2, 3)]),
            (hu, tile_rows(va, 1, 4)),
            (dn, d.at[pl.ds(13, 3)]),
            (hd, tile_rows(va, 13, 4)),
        ],
    )

    def prepare(r0, n):
        def cp(i, carry):
            r = r0 + i
            for j in range(4):
                x = va[r, pl.ds(OFF + 128 * j, 128), :]
                if j == 0:
                    va[r, pl.ds(OFF + LON, 1), :] = x[0:1]
                if j == 3:
                    va[r, pl.ds(OFF - 1, 1), :] = x[127:128]
                keep = d[r, pl.ds(128 * j, 128), :] > 0.0
                put_halves(h, r, j, jnp.where(keep, x, 0.0))
            return carry

        lax.fori_loop(0, n, cp, 0)

    wait(c[0], c[1])
    prepare(5, 4)
    wait(c[2])
    prepare(9, 4)
    wait(*c[3:])
    clear_ends(me, ((va, 1, 4), (d, 2, 3)), ((va, 13, 4), (d, 13, 3)))
    prepare(2, 3)
    prepare(13, 3)
    forward_block(va, vb, h, d, w2, first=True)
    c = copies(sems, [(tile_rows(va, 5 + 2 * i, 2), o) for i, o in enumerate((o_t0, o_t1, o_b0, o_b1))])
    o_surf[...] = gather_surface(lambda r, j: va[r + 5, pl.ds(OFF + 128 * j, 128), :], 8)[0:32]
    wait(*c)


def first_block(*args):
    return pl.pallas_call(
        first_kernel,
        out_shape=(HALF,) * 4 + (sds(32, 128),),
        in_specs=[SM] + [ANY] * 7 + [VM],
        out_specs=(ANY,) * 4 + (VM,),
        scratch_shapes=BLOCK_SCRATCH + [dma_sems(7)],
        compiler_params=params(),
        cost_estimate=cost(15),
        name="first_block",
    )(*args)


def middle_kernel(
    me, t0, t1, b0, b1, hu0, hu1, hd0, hd1, s, su, sd, dt, du, dn, m, w2f, w2b,
    o_final, o_adj, o_u0, o_u1, o_d0, o_d1, o_s, o_su, o_sd, va, vb, h, d, u, mm, cols, sems,
):
    c = copies(
        sems,
        [
            (t0, tile_rows(va, 5, 2)),
            (t1, tile_rows(va, 7, 2)),
            (b0, tile_rows(va, 9, 2)),
            (b1, tile_rows(va, 11, 2)),
            (hu0, tile_rows(va, 1, 2)),
            (hu1, tile_rows(va, 3, 2)),
            (hd0, tile_rows(va, 13, 2)),
            (hd1, tile_rows(va, 15, 2)),
            (dt, d.at[pl.ds(5, 8)]),
            (du, d.at[pl.ds(2, 3)]),
            (dn, d.at[pl.ds(13, 3)]),
            (m, mm),
        ],
    )
    cols[0:16] = su[...]
    cols[16:48] = s[...]
    cols[48:64] = sd[...]
    cols[64:128] = jnp.zeros((64, 128), F32)
    clear_ends(me, ((cols, 0, 16),), ((cols, 48, 16),))
    cols[...] = cols[...].T

    def prepare(r0):
        def cp(i, carry):
            r = r0 + i
            for j in range(4):
                x = va[r, pl.ds(OFF + 128 * j, 128), :]
                x = x + spread_column(cols[...], 4 * (r - 1) + j)
                put(va, r, j, x)
                put_halves(h, r, j, x)
            return carry

        lax.fori_loop(0, 4, cp, 0)

    for i, r0 in ((0, 5), (2, 9)):
        wait(c[i], c[i + 1])
        prepare(r0)
    wait(*c[4:11])
    clear_ends(me, ((va, 1, 4), (d, 2, 3)), ((va, 13, 4), (d, 13, 3)))
    prepare(1)
    prepare(13)
    forward_block(va, vb, h, d, w2f)
    out = copies(sems, [(tile_rows(va, 5, 8), o_final)])
    wait(c[11])

    def body(i, carry):
        r = 5 + i
        for j in range(4):
            at = pl.ds(128 * j, 128)
            x = va[r, pl.ds(OFF + 128 * j, 128), :] - mm[i, at, :]
            dd = d[r, at, :]
            x = jnp.where(dd > 0.0, x, 0.0)
            u[r, at, :] = x
            put(vb, r, j, dd * x)
            put_halves(h, r, j, x)
        return carry

    lax.fori_loop(0, 8, body, 0)
    wait(*out)
    push_block(vb, va, u, h, d, w2b)
    out = copies(
        sems,
        [
            (u.at[pl.ds(1, 2)], o_u0),
            (u.at[pl.ds(3, 2)], o_u1),
            (u.at[pl.ds(13, 2)], o_d0),
            (u.at[pl.ds(15, 2)], o_d1),
            (u.at[pl.ds(5, 8)], o_adj),
        ],
    )
    g = gather_surface(lambda r, j: u[r + 1, pl.ds(128 * j, 128), :], 16)
    o_su[...] = g[0:16]
    o_s[...] = g[16:48]
    o_sd[...] = g[48:64]
    wait(*out)


def middle_block(*args):
    return pl.pallas_call(
        middle_kernel,
        out_shape=(
            sds(8, LON, LEV), sds(8, LON, LEV), HALF, HALF, HALF, HALF,
            sds(32, 128), sds(16, 128), sds(16, 128),
        ),
        in_specs=[SM] + [ANY] * 8 + [VM] * 3 + [ANY] * 4 + [VM] * 2,
        out_specs=(ANY,) * 6 + (VM,) * 3,
        scratch_shapes=BLOCK_SCRATCH
        + [U_SCRATCH, pltpu.VMEM((8, LON, 128), F32), COLS, dma_sems(12)],
        compiler_params=params(),
        cost_estimate=cost(30),
        name="middle_block",
    )(*args)


def last_kernel(
    me, adj, ru0, ru1, rd0, rd1, s, top, bot, dt, du, dn, w2b, o_base, o_up, o_dn,
    va, vb, h, d, u, got, base, cols, sems,
):
    c = copies(
        sems,
        [
            (adj, u.at[pl.ds(5, 8)]),
            (dt, d.at[pl.ds(5, 8)]),
            (ru0, got.at[pl.ds(0, 2)]),
            (ru1, got.at[pl.ds(2, 2)]),
            (rd0, got.at[pl.ds(4, 2)]),
            (rd1, got.at[pl.ds(6, 2)]),
            (du, d.at[pl.ds(2, 3)]),
            (dn, d.at[pl.ds(13, 3)]),
            (top, base.at[pl.ds(0, 4)]),
            (bot, base.at[pl.ds(4, 4)]),
        ],
    )
    cols[0:32] = s[...]
    cols[32:128] = jnp.zeros((96, 128), F32)
    cols[...] = cols[...].T
    wait(*c[0:6])
    clear_ends(me, ((got, 0, 4),), ((got, 4, 4),))

    def cp(i, carry):
        r = 5 + i
        for j in range(4):
            at = pl.ds(128 * j, 128)
            x = u[r, at, :] + got[i, at, :]
            x = x + spread_column(cols[...], 4 * i + j)
            dd = d[r, at, :]
            x = jnp.where(dd > 0.0, x, 0.0)
            u[r, at, :] = x
            put(vb, r, j, dd * x)
            put_halves(h, r, j, x)
        return carry

    lax.fori_loop(0, 8, cp, 0)
    wait(*c[6:10])
    clear_ends(me, ((d, 2, 3),), ((d, 13, 3),))
    push_block(vb, va, u, h, d, w2b)
    out = copies(sems, [(u.at[pl.ds(1, 4)], o_up), (u.at[pl.ds(13, 4)], o_dn)])

    def add(i, carry):
        base[i] = base[i] + u[5 + i]
        return carry

    lax.fori_loop(0, 8, add, 0)
    end = pltpu.make_async_copy(base, o_base, sems.at[2])
    end.start()
    wait(*out)
    end.wait()


def last_block(*args):
    return pl.pallas_call(
        last_kernel,
        out_shape=(sds(8, LON, LEV), sds(4, LON, LEV), sds(4, LON, LEV)),
        in_specs=[SM] + [ANY] * 5 + [VM] + [ANY] * 5 + [VM],
        out_specs=(ANY,) * 3,
        scratch_shapes=BLOCK_SCRATCH
        + [
            U_SCRATCH,
            pltpu.VMEM((8, LON, 128), F32),
            pltpu.VMEM((8, LON, 128), F32),
            COLS,
            dma_sems(10),
        ],
        compiler_params=params(),
        cost_estimate=cost(15),
        name="last_block",
    )(*args)


def offer_kernel(me, send_rows, surf, o):
    o[...] = jnp.zeros((512, 128), F32)
    for off in OFFSETS:
        t = lax.rem(me[0] + (off + 64), 64) * 8
        for q in range(8):
            o[pl.ds(t + q, 1), :] = surf[pl.ds(send_rows[t + q], 1), :]


def offer(me, send_rows, surf):
    return pl.pallas_call(
        offer_kernel,
        out_shape=sds(512, 128),
        in_specs=[SM, SM, VM],
        out_specs=VM,
        name="offer",
    )(me, send_rows, surf)


def fetch_blocks(ids, w, buf, sems):
    for k in range(LIVE):
        pltpu.make_async_copy(w.at[ids[k]], buf.at[k], sems.at[k // 12]).start()


def fetched(w, buf, sems, part):
    pltpu.make_async_copy(w.at[pl.ds(0, 12)], buf.at[pl.ds(12 * part, 12)], sems.at[part]).wait()


LIVE = 48
WEIGHTS = [pltpu.VMEM((LIVE, 128, 128), F32), pltpu.SemaphoreType.DMA((4,))]


def remap_kernel(ids, pick, dest, arrived, w, sea, o, buf, sems):
    fetch_blocks(ids, w, buf, sems)
    acc = jnp.zeros((128, 128), F32)
    for part in range(4):
        fetched(w, buf, sems, part)

        def step(i, acc, part=part):
            for q in range(4):
                k = 12 * part + 4 * i + q
                x = arrived[pl.ds(pick[k], 1), :]
                red = jnp.sum(buf[k] * x, axis=1, keepdims=True)
                acc = acc + jnp.where(lanes() == dest[k], red, 0.0)
            return acc

        acc = lax.fori_loop(0, 3, step, acc)
    o[...] = acc.T[0:32] * sea[...]


def remap(ids, pick, dest, arrived, w, sea):
    return pl.pallas_call(
        remap_kernel,
        out_shape=sds(32, 128),
        in_specs=[SM, SM, SM, VM, ANY, VM],
        out_specs=VM,
        scratch_shapes=WEIGHTS,
        compiler_params=params(),
        cost_estimate=cost(3),
        name="remap",
    )(ids, pick, dest, arrived, w, sea)


def remap_back_kernel(me, ids, pick, dest, s, ru, rd, w, sea, o, cols, wide, buf, sems):
    fetch_blocks(ids, w, buf, sems)
    cols[0:16] = ru[...]
    cols[16:32] = rd[...]
    clear_ends(me, ((cols, 0, 16),), ((cols, 16, 16),))
    cols[0:32] = (cols[0:32] + s[...]) * sea[...]
    cols[32:128] = jnp.zeros((96, 128), F32)
    cols[...] = cols[...].T
    for p in range(32):
        wide[p] = jnp.broadcast_to(cols[:, p : p + 1], (128, 128))
    o[...] = jnp.zeros((512, 128), F32)
    for part in range(4):
        fetched(w, buf, sems, part)

        def step(i, carry, part=part):
            for q in range(4):
                k = 12 * part + 4 * i + q
                red = jnp.sum(buf[k] * wide[dest[k]], axis=0, keepdims=True)
                o[pl.ds(pick[k], 1), :] = red
            return carry

        lax.fori_loop(0, 3, step, 0)


def remap_back(me, ids, pick, dest, s, ru, rd, w, sea):
    return pl.pallas_call(
        remap_back_kernel,
        out_shape=sds(512, 128),
        in_specs=[SM, SM, SM, SM, VM, VM, VM, ANY, VM],
        out_specs=VM,
        scratch_shapes=[COLS, pltpu.VMEM((32, 128, 128), F32)] + WEIGHTS,
        compiler_params=params(),
        cost_estimate=cost(3),
        name="remap_back",
    )(me, ids, pick, dest, s, ru, rd, w, sea)


def collect_kernel(me, send_rows, got, o):
    o[...] = jnp.zeros((32, 128), F32)
    for off in OFFSETS:
        t = lax.rem(me[0] + (off + 64), 64) * 8
        for q in range(8):
            at = pl.ds(send_rows[t + q], 1)
            o[at, :] = o[at, :] + got[pl.ds(t + q, 1), :]


def collect(me, send_rows, got):
    return pl.pallas_call(
        collect_kernel,
        out_shape=sds(32, 128),
        in_specs=[SM, SM, VM],
        out_specs=VM,
        name="collect",
    )(me, send_rows, got)


def shards(
    starting_perturbation,
    measured_discrepancy,
    diffusion,
    vert_mix,
    ocean_mask,
    pair_tile,
    pair_patch,
    dest_patch,
    pair_blocks,
    remap_weight,
):
    component = lax.axis_index("comp")
    own_tile = lax.axis_index("tile")
    down_pairs = [(i, (i + 1) % 64) for i in range(64)]
    up_pairs = [((i + 1) % 64, i) for i in range(64)]

    def to_next(x):
        return lax.ppermute(x, "tile", down_pairs)

    def to_prev(x):
        return lax.ppermute(x, "tile", up_pairs)

    def both(last, first):
        after = to_next(last)
        before = to_prev(first)
        return after, before

    def swap(x):
        return lax.ppermute(x, "comp", [(0, 1), (1, 0)])

    def exchange(x):
        x = x.reshape(64, 8, 128)
        x = lax.all_to_all(x, "tile", split_axis=0, concat_axis=0, tiled=True)
        return x.reshape(512, 128)

    start = starting_perturbation.reshape(1024, LON)
    s_top, s_bot = start_in(start)
    s_hu, s_hd = to_next(s_bot), to_prev(s_top)
    sea = jnp.where(component == 1, ocean_mask.astype(F32), 1.0)
    sea32 = sea.reshape(32, 128)
    dt, d_top, d_bot = diff_in(diffusion.reshape(1024, LON), sea)
    du, dd = to_next(d_bot), to_prev(d_top)
    w2f, w2b = mixes(vert_mix[0])

    slots = jnp.arange(64, dtype=jnp.int32)
    live = slots % 8 < jnp.repeat(pair_blocks[0, 0], 8)
    place = jnp.sum((slots[None, :] < slots[:, None]) & live[None, :], axis=1)
    chosen = ((place[None, :] == slots[:LIVE, None]) & live[None, :]).astype(jnp.int32)
    ids = jnp.sum(chosen * slots[None, :], axis=1)
    pick = jnp.repeat(pair_tile[component, own_tile], 8) * 8 + slots % 8
    pick = jnp.sum(chosen * pick[None, :], axis=1)
    dest = jnp.sum(chosen * dest_patch[0, 0][None, :], axis=1)
    hits = (pair_tile[component] == own_tile).astype(jnp.int32)
    sources = pair_patch[component].reshape(64, 8, 8)
    send_rows = jnp.sum(hits[:, :, None] * sources, axis=1).reshape(512)
    me = own_tile.reshape(1)
    weights = remap_weight[0]
    measured = to_rows(measured_discrepancy.reshape(1024, LON))
    s_hu, s_hd, du, dd, w2f, w2b, ids, pick, dest, send_rows, measured, sea32 = (
        lax.optimization_barrier(
            (s_hu, s_hd, du, dd, w2f, w2b, ids, pick, dest, send_rows, measured, sea32)
        )
    )

    t0, t1, b0, b1, surf = first_block(me, s_top, s_bot, s_hu, s_hd, dt, du, dd, w2f)
    other = swap(surf)
    hu0, hd0 = both(b0, t0)
    offered = offer(me, send_rows, other)
    arrived = exchange(offered)
    b1s, t1s, arrived = lax.optimization_barrier((b1, t1, arrived))
    hu1, hd1 = to_next(b1s), to_prev(t1s)
    fix = remap(ids, pick, dest, arrived, weights, sea32)
    f_hu, f_hd = to_next(fix[16:32]), to_prev(fix[0:16])
    final, adj, u0, u1, d0, d1, a0, a0_up, a0_dn = middle_block(
        me, t0, t1, b0, b1, hu0, hu1, hd0, hd1, fix, f_hu, f_hd, dt, du, dd, measured, w2f, w2b
    )
    r0u, r0d = to_next(a0_dn), to_prev(a0_up)
    u0, d0, r0u, r0d = lax.optimization_barrier((u0, d0, r0u, r0d))
    ru0, rd0 = both(d0, u0)
    offered = remap_back(me, ids, pick, dest, a0, r0u, r0d, weights, sea32)
    back = exchange(offered)
    u1, d1, back = lax.optimization_barrier((u1, d1, back))
    ru1, rd1 = to_next(d1), to_prev(u1)
    back = swap(collect(me, send_rows, back))
    base, g_up, g_dn = last_block(me, adj, ru0, ru1, rd0, rd1, back, s_top, s_bot, dt, du, dd, w2b)
    gu, gd = to_next(g_dn), to_prev(g_up)
    final_raw = to_raw(final)
    gradient = grad_out(me, base, gu, gd)
    shape = starting_perturbation.shape
    return final_raw.reshape(shape), gradient.reshape(shape)


def solution(mesh):
    field = P("comp", None, "tile", None)
    placed = (
        field,
        field,
        field,
        P("comp", None, None),
        P("tile", None),
        P(),
        P(),
        P("comp", "tile", None),
        P("comp", "tile", None),
        P("comp", "tile", None, None),
    )

    return jax.shard_map(
        shards,
        mesh=mesh,
        in_specs=placed,
        out_specs=(field, field),
        check_vma=False,
    )
```

```python
import jax
import jax.numpy as jnp
from jax import lax
from jax.experimental import pallas as pl
from jax.experimental.pallas import tpu as pltpu
from jax.sharding import PartitionSpec as P


F32 = jnp.float32
BF = jnp.bfloat16
LON, LEV = 512, 128
OFF, PAD = 8, 528
NR = 18
VM = pl.BlockSpec(memory_space=pltpu.VMEM)
SM = pl.BlockSpec(memory_space=pltpu.SMEM)
BLOCK_MIB = 44
OFFSETS = tuple(range(-7, 8)) + (32,)


def sds(*shape, dtype=F32):
    return jax.ShapeDtypeStruct(shape, dtype)


def cost(us):
    return pl.CostEstimate(flops=int(us * 5e8), bytes_accessed=1 << 20, transcendentals=0)


def params(mib=BLOCK_MIB):
    return pltpu.CompilerParams(vmem_limit_bytes=mib * 2**20)


def parity(me):
    return lax.rem(me[0], 2)


def halves(x):
    hi = x.astype(BF)
    return hi, (x - hi.astype(F32)).astype(BF)


ANY = pl.BlockSpec(memory_space=pltpu.MemorySpace.HBM)
RAW = pltpu.VMEM((4, 1024, 128), F32)
ROWS = pltpu.VMEM((8, LON, LEV), F32)


def dma_sems(*n):
    return pltpu.SemaphoreType.DMA(n)


def lon_part(ref, j):
    return ref.at[:, pl.ds(128 * j, 128), :]


def start_raw(x, buf, sems):
    out = [
        pltpu.make_async_copy(x.at[:, pl.ds(128 * j, 128)], buf.at[j], sems.at[j])
        for j in range(4)
    ]
    for c in out:
        c.start()
    return out


def turned(buf, j, r):
    return buf[j, pl.ds(r, 128, stride=8), :].T


def start_in_kernel(me, x, outer, inner, buf, out, sems, osems):
    odd = parity(me)
    c = start_raw(x, buf, sems)
    todo = []
    for j in range(4):
        c[j].wait()
        for r in range(8):
            out[r, pl.ds(128 * j, 128), :] = turned(buf, j, r)
        for i, (r0, dst) in enumerate(((4 * odd, outer), (4 - 4 * odd, inner))):
            src = out.at[pl.ds(r0, 4), pl.ds(128 * j, 128), :]
            todo.append(pltpu.make_async_copy(src, lon_part(dst, j), osems.at[i, j]))
            todo[-1].start()
    for d in todo:
        d.wait()


def start_in(me, x):
    return pl.pallas_call(
        start_in_kernel,
        out_shape=(sds(4, LON, LEV), sds(4, LON, LEV)),
        in_specs=[SM, ANY],
        out_specs=(ANY, ANY),
        scratch_shapes=[RAW, ROWS, dma_sems(4), dma_sems(2, 4)],
        compiler_params=params(),
        cost_estimate=cost(4),
        name="start_in",
    )(me, x)


def diff_in_kernel(me, x, sea, outer, inner, full, buf, out, sems, osems):
    odd = parity(me)
    c = start_raw(x, buf, sems)
    todo = []
    for j in range(4):
        c[j].wait()
        at = pl.ds(128 * j, 128)
        for r in range(8):
            out[r, at, :] = (buf[j, pl.ds(r, 128, stride=8), :] * sea[r : r + 1, at]).T
        for i, (r0, n, dst) in enumerate(((5 * odd, 3, outer), (5 - 5 * odd, 3, inner), (0, 8, full))):
            src = out.at[pl.ds(r0, n), at, :]
            todo.append(pltpu.make_async_copy(src, lon_part(dst, j), osems.at[i, j]))
            todo[-1].start()
    for d in todo:
        d.wait()


def diff_in(me, x, sea):
    return pl.pallas_call(
        diff_in_kernel,
        out_shape=(sds(3, LON, LEV), sds(3, LON, LEV), sds(8, LON, LEV)),
        in_specs=[SM, ANY, VM],
        out_specs=(ANY,) * 3,
        scratch_shapes=[RAW, ROWS, dma_sems(4), dma_sems(3, 4)],
        compiler_params=params(),
        cost_estimate=cost(4),
        name="diff_in",
    )(me, x, sea)


def to_rows_kernel(x, o, buf, out, sems, osems):
    c = start_raw(x, buf, sems)
    todo = []
    for j in range(4):
        c[j].wait()
        for r in range(8):
            out[r, pl.ds(128 * j, 128), :] = turned(buf, j, r)
        todo.append(pltpu.make_async_copy(lon_part(out, j), lon_part(o, j), osems.at[j]))
        todo[-1].start()
    for d in todo:
        d.wait()


def to_rows(x):
    return pl.pallas_call(
        to_rows_kernel,
        out_shape=sds(8, LON, LEV),
        in_specs=[ANY],
        out_specs=ANY,
        scratch_shapes=[RAW, ROWS, dma_sems(4), dma_sems(4)],
        compiler_params=params(),
        cost_estimate=cost(4),
        name="to_rows",
    )(x)


def to_raw_kernel(x, o):
    for r in range(8):
        o[pl.ds(r, 128, stride=8), :] = x[r].T


def to_raw(x):
    return pl.pallas_call(
        to_raw_kernel,
        grid=(4,),
        out_shape=sds(1024, LON),
        in_specs=[pl.BlockSpec((8, 128, 128), lambda j: (0, j, 0))],
        out_specs=pl.BlockSpec((1024, 128), lambda j: (0, j)),
        compiler_params=params(),
        cost_estimate=cost(4),
        name="to_raw",
    )(x)


def grad_out_kernel(me, x, outer, inner, o, base, add, buf, sems, osems):
    odd = parity(me)
    c = []
    for j in range(4):
        at = pl.ds(128 * j, 128)
        for i, (src, dst) in enumerate(
            (
                (lon_part(outer, j), add.at[pl.ds(4 * odd, 4), at, :]),
                (lon_part(inner, j), add.at[pl.ds(4 - 4 * odd, 4), at, :]),
                (lon_part(x, j), lon_part(base, j)),
            )
        ):
            c.append(pltpu.make_async_copy(src, dst, sems.at[i, j]))
            c[-1].start()
    keep_up = jnp.where(me[0] > 0, 1.0, 0.0)
    keep_dn = jnp.where(me[0] < 63, 1.0, 0.0)
    todo = []
    for j in range(4):
        at = pl.ds(128 * j, 128)
        for d in c[3 * j : 3 * j + 3]:
            d.wait()
        for r in range(8):
            keep = keep_up if r < 4 else keep_dn
            buf[j, pl.ds(r, 128, stride=8), :] = (base[r, at, :] + keep * add[r, at, :]).T
        todo.append(pltpu.make_async_copy(buf.at[j], o.at[:, at], osems.at[j]))
        todo[-1].start()
    for d in todo:
        d.wait()


def grad_out(me, x, outer, inner):
    return pl.pallas_call(
        grad_out_kernel,
        out_shape=sds(1024, LON),
        in_specs=[SM, ANY, ANY, ANY],
        out_specs=ANY,
        scratch_shapes=[ROWS, ROWS, RAW, dma_sems(3, 4), dma_sems(4)],
        compiler_params=params(),
        cost_estimate=cost(4),
        name="grad_out",
    )(me, x, outer, inner)


def mix_kernel(w, fwd, bwd):
    for dst, x in ((fwd, w[...].T), (bwd, w[...])):
        hi, lo = halves(x)
        dst[0:128, 0:128] = hi
        dst[128:256, 0:128] = hi
        dst[0:128, 128:256] = lo
        dst[128:256, 128:256] = jnp.zeros((128, 128), BF)


def mixes(w):
    return pl.pallas_call(
        mix_kernel,
        out_shape=(sds(256, 256, dtype=BF), sds(256, 256, dtype=BF)),
        in_specs=[VM],
        out_specs=(VM, VM),
        name="mixes",
    )(w)


def put(v, r, j, new):
    v[r, pl.ds(OFF + 128 * j, 128), :] = new
    if j == 0:
        v[r, pl.ds(OFF + LON, 1), :] = new[0:1]
    if j == 3:
        v[r, pl.ds(OFF - 1, 1), :] = new[127:128]


def put_halves(h, r, j, new):
    hi, lo = halves(new)
    h[r, pl.ds(128 * j, 128), 0:128] = hi
    h[r, pl.ds(128 * j, 128), 128:256] = lo


def around(v, r, j):
    at = OFF + 128 * j
    n = v[r - 1, pl.ds(at, 128), :] + v[r + 1, pl.ds(at, 128), :]
    return n + (v[r, pl.ds(at - 1, 128), :] + v[r, pl.ds(at + 1, 128), :])


GROUP = {14: 7, 12: 6, 10: 5, 8: 4}


def mixed_rows(h, w2, lo, n, body):
    k = GROUP[n]

    def step(i, carry):
        r0 = lo + k * i
        y = jnp.dot(h[pl.ds(r0, k)].reshape(LON * k, 256), w2[...], preferred_element_type=F32)
        for q in range(k):
            for j in range(4):
                part = y[LON * q + 128 * j : LON * q + 128 * j + 128]
                body(r0 + q, j, part[:, 0:128] + part[:, 128:256])
        return carry

    lax.fori_loop(0, n // k, step, 0)


def forward_step(va, vb, h, d, w2, s, first=False, last=False):
    def body(r, j, y):
        c = va[r, pl.ds(OFF + 128 * j, 128), :]
        dd = d[r, pl.ds(128 * j, 128), :]
        n = dd * (around(va, r, j) - 4.0 * c)
        if first:
            c = jnp.where(dd > 0.0, c, 0.0)
        new = (c + n) + y
        put(vb, r, j, new)
        if not last:
            put_halves(h, r, j, new)

    mixed_rows(h, w2, 1 + s, 16 - 2 * s, body)


def push_step(ga, gb, u, h, d, w2, s, last=False):
    def finish(r, j, new, dd):
        u[r, pl.ds(128 * j, 128), :] = new
        put(gb, r, j, dd * new)
        put_halves(h, r, j, new)

    def body(r, j, y):
        at = pl.ds(128 * j, 128)
        n = around(ga, r, j) - 4.0 * ga[r, pl.ds(OFF + 128 * j, 128), :]
        c = u[r, at, :]
        if last:
            u[r, at, :] = (c + n) + y
        else:
            dd = d[r, at, :]
            finish(r, j, (c + jnp.where(dd > 0.0, n, 0.0)) + y, dd)

    mixed_rows(h, w2, 6 - s, 6 + 2 * s, body)
    for r, near in ((5 - s, 6 - s), (12 + s, 11 + s)):
        for j in range(4):
            at = pl.ds(128 * j, 128)
            n = ga[near, pl.ds(OFF + 128 * j, 128), :]
            if last:
                u[r, at, :] = n
            else:
                dd = d[r, at, :]
                finish(r, j, jnp.where(dd > 0.0, n, 0.0), dd)


def push_block(ga, gb, u, h, d, w2):
    for s, g in ((1, ga), (2, gb), (3, ga), (4, gb)):
        g[5 - s] = jnp.zeros((PAD, 128), F32)
        g[12 + s] = jnp.zeros((PAD, 128), F32)
    push_step(ga, gb, u, h, d, w2, 1)
    push_step(gb, ga, u, h, d, w2, 2)
    push_step(ga, gb, u, h, d, w2, 3)
    push_step(gb, ga, u, h, d, w2, 4, last=True)


def forward_block(va, vb, h, d, w2, first=False):
    forward_step(va, vb, h, d, w2, 1, first=first)
    forward_step(vb, va, h, d, w2, 2)
    forward_step(va, vb, h, d, w2, 3)
    forward_step(vb, va, h, d, w2, 4, last=True)


def copies(sems, pairs):
    out = [pltpu.make_async_copy(a, b, sems.at[i]) for i, (a, b) in enumerate(pairs)]
    for c in out:
        c.start()
    return out


def wait(*todo):
    for c in todo:
        c.wait()


def plain_rows(v, r0, n):
    return v.at[pl.ds(r0, n)]


def tile_rows(v, r0, n):
    return v.at[pl.ds(r0, n), pl.ds(OFF, LON), :]


def clear_ends(me, up, dn):
    for edge, todo in ((0, up), (63, dn)):

        @pl.when(me[0] == edge)
        def _(todo=todo):
            for ref, r0, n in todo:
                ref[pl.ds(r0, n)] = jnp.zeros((n,) + ref.shape[1:], F32)


def lanes():
    return lax.broadcasted_iota(jnp.int32, (128, 128), 1)


def gather_surface(read, count):
    def step(r, acc):
        for j in range(4):
            p = 4 * r + j
            acc = jnp.where(lanes() == p, pltpu.roll(read(r, j), p, 1), acc)
        return acc

    return lax.fori_loop(0, count, step, jnp.zeros((128, 128), F32)).T


def spread_column(cols, p):
    return jnp.where(lanes() == 0, pltpu.roll(cols, (128 - p) % 128, 1), 0.0)


BLOCK_SCRATCH = [
    pltpu.VMEM((NR, PAD, 128), F32),
    pltpu.VMEM((NR, PAD, 128), F32),
    pltpu.VMEM((NR, LON, 256), BF),
    pltpu.VMEM((NR, LON, 128), F32),
]
U_SCRATCH = pltpu.VMEM((NR, LON, 128), F32)
COLS = pltpu.VMEM((128, 128), F32)
PARTS = (sds(3, LON, LEV), sds(1, LON, LEV), sds(4, LON, LEV))


def near_far(up, dn, odd):
    return up + (dn - up) * odd, dn + (up - dn) * odd


def edge_refs(v, up, dn, odd, cut):
    outer, inner = near_far(up, dn, odd)
    return cut(v, outer, 3), cut(v, outer + 3, 1), cut(v, inner, 4)


def first_kernel(me, so, si, ho, hi, dt, do, di, w2, o0, o1, o2, o_surf, va, vb, h, d, sems):
    odd = parity(me)
    own_o, own_i = near_far(5, 9, odd)
    far_o, far_i = near_far(1, 13, odd)
    d_o, d_i = near_far(2, 13, odd)
    c = copies(
        sems,
        [
            (dt, d.at[pl.ds(5, 8)]),
            (so, tile_rows(va, own_o, 4)),
            (si, tile_rows(va, own_i, 4)),
            (do, d.at[pl.ds(d_o, 3)]),
            (ho, tile_rows(va, far_o, 4)),
            (di, d.at[pl.ds(d_i, 3)]),
            (hi, tile_rows(va, far_i, 4)),
        ],
    )

    def prepare(r0, n):
        def cp(i, carry):
            r = r0 + i
            for j in range(4):
                x = va[r, pl.ds(OFF + 128 * j, 128), :]
                if j == 0:
                    va[r, pl.ds(OFF + LON, 1), :] = x[0:1]
                if j == 3:
                    va[r, pl.ds(OFF - 1, 1), :] = x[127:128]
                keep = d[r, pl.ds(128 * j, 128), :] > 0.0
                put_halves(h, r, j, jnp.where(keep, x, 0.0))
            return carry

        lax.fori_loop(0, n, cp, 0)

    wait(c[0], c[1])
    prepare(own_o, 4)
    wait(c[2])
    prepare(own_i, 4)
    wait(*c[3:])
    clear_ends(me, ((va, 1, 4), (d, 2, 3)), ((va, 13, 4), (d, 13, 3)))
    prepare(2, 3)
    prepare(13, 3)
    forward_block(va, vb, h, d, w2, first=True)
    c = copies(sems, list(zip(edge_refs(va, 5, 9, odd, tile_rows), (o0, o1, o2))))
    o_surf[...] = gather_surface(lambda r, j: va[r + 5, pl.ds(OFF + 128 * j, 128), :], 8)[0:32]
    wait(*c)


def first_block(*args):
    return pl.pallas_call(
        first_kernel,
        out_shape=PARTS + (sds(32, 128),),
        in_specs=[SM] + [ANY] * 7 + [VM],
        out_specs=(ANY,) * 3 + (VM,),
        scratch_shapes=BLOCK_SCRATCH + [dma_sems(7)],
        compiler_params=params(),
        cost_estimate=cost(15),
        name="first_block",
    )(*args)


def middle_kernel(
    me, v0, v1, v2, h0, h1, h2, s, so, si, dt, do, di, m, w2f, w2b,
    o_final, o_adj, o0, o1, o2, o_s, o_so, o_si, va, vb, h, d, u, mm, cols, sems,
):
    odd = parity(me)
    own = edge_refs(va, 5, 9, odd, tile_rows)
    far = edge_refs(va, 1, 13, odd, tile_rows)
    d_o, d_i = near_far(2, 13, odd)
    c = copies(
        sems,
        [
            (v0, own[0]),
            (v1, own[1]),
            (v2, own[2]),
            (h0, far[0]),
            (h1, far[1]),
            (h2, far[2]),
            (dt, d.at[pl.ds(5, 8)]),
            (do, d.at[pl.ds(d_o, 3)]),
            (di, d.at[pl.ds(d_i, 3)]),
            (m, mm),
        ],
    )
    c_o, c_i = near_far(0, 48, odd)
    cols[pl.ds(pl.multiple_of(c_o, 16), 16)] = so[...]
    cols[pl.ds(pl.multiple_of(c_i, 16), 16)] = si[...]
    cols[16:48] = s[...]
    cols[64:128] = jnp.zeros((64, 128), F32)
    clear_ends(me, ((cols, 0, 16),), ((cols, 48, 16),))
    cols[...] = cols[...].T

    def prepare(r0):
        def cp(i, carry):
            r = r0 + i
            for j in range(4):
                x = va[r, pl.ds(OFF + 128 * j, 128), :]
                x = x + spread_column(cols[...], 4 * (r - 1) + j)
                put(va, r, j, x)
                put_halves(h, r, j, x)
            return carry

        lax.fori_loop(0, 4, cp, 0)

    wait(*c[0:3])
    prepare(5)
    prepare(9)
    wait(*c[3:9])
    clear_ends(me, ((va, 1, 4), (d, 2, 3)), ((va, 13, 4), (d, 13, 3)))
    prepare(1)
    prepare(13)
    forward_block(va, vb, h, d, w2f)
    out = copies(sems, [(tile_rows(va, 5, 8), o_final)])
    wait(c[9])

    def body(i, carry):
        r = 5 + i
        for j in range(4):
            at = pl.ds(128 * j, 128)
            x = va[r, pl.ds(OFF + 128 * j, 128), :] - mm[i, at, :]
            dd = d[r, at, :]
            x = jnp.where(dd > 0.0, x, 0.0)
            u[r, at, :] = x
            put(vb, r, j, dd * x)
            put_halves(h, r, j, x)
        return carry

    lax.fori_loop(0, 8, body, 0)
    wait(*out)
    push_block(vb, va, u, h, d, w2b)
    out = copies(
        sems,
        list(zip(edge_refs(u, 1, 13, odd, plain_rows), (o0, o1, o2)))
        + [(u.at[pl.ds(5, 8)], o_adj)],
    )
    cols[...] = gather_surface(lambda r, j: u[r + 1, pl.ds(128 * j, 128), :], 16)
    o_so[...] = cols[pl.ds(pl.multiple_of(c_o, 16), 16)]
    o_s[...] = cols[16:48]
    o_si[...] = cols[pl.ds(pl.multiple_of(c_i, 16), 16)]
    wait(*out)


def middle_block(*args):
    return pl.pallas_call(
        middle_kernel,
        out_shape=(
            sds(8, LON, LEV), sds(8, LON, LEV), *PARTS,
            sds(32, 128), sds(16, 128), sds(16, 128),
        ),
        in_specs=[SM] + [ANY] * 6 + [VM] * 3 + [ANY] * 4 + [VM] * 2,
        out_specs=(ANY,) * 5 + (VM,) * 3,
        scratch_shapes=BLOCK_SCRATCH
        + [U_SCRATCH, pltpu.VMEM((8, LON, 128), F32), COLS, dma_sems(12)],
        compiler_params=params(),
        cost_estimate=cost(30),
        name="middle_block",
    )(*args)


def last_kernel(
    me, adj, r0, r1, r2, s, so, si, dt, do, di, w2b, o_base, o_outer, o_inner,
    va, vb, h, d, u, got, base, cols, sems,
):
    odd = parity(me)
    e_o, e_i = near_far(0, 4, odd)
    d_o, d_i = near_far(2, 13, odd)
    parts = edge_refs(got, 0, 4, odd, plain_rows)
    c = copies(
        sems,
        [
            (adj, u.at[pl.ds(5, 8)]),
            (dt, d.at[pl.ds(5, 8)]),
            (r0, parts[0]),
            (r1, parts[1]),
            (r2, parts[2]),
            (do, d.at[pl.ds(d_o, 3)]),
            (di, d.at[pl.ds(d_i, 3)]),
            (so, base.at[pl.ds(e_o, 4)]),
            (si, base.at[pl.ds(e_i, 4)]),
        ],
    )
    cols[0:32] = s[...]
    cols[32:128] = jnp.zeros((96, 128), F32)
    cols[...] = cols[...].T
    wait(*c[0:5])
    clear_ends(me, ((got, 0, 4),), ((got, 4, 4),))

    def cp(i, carry):
        r = 5 + i
        for j in range(4):
            at = pl.ds(128 * j, 128)
            x = u[r, at, :] + got[i, at, :]
            x = x + spread_column(cols[...], 4 * i + j)
            dd = d[r, at, :]
            x = jnp.where(dd > 0.0, x, 0.0)
            u[r, at, :] = x
            put(vb, r, j, dd * x)
            put_halves(h, r, j, x)
        return carry

    lax.fori_loop(0, 8, cp, 0)
    wait(*c[5:9])
    clear_ends(me, ((d, 2, 3),), ((d, 13, 3),))
    push_block(vb, va, u, h, d, w2b)
    out_o, out_i = near_far(1, 13, odd)
    out = copies(sems, [(u.at[pl.ds(out_o, 4)], o_outer), (u.at[pl.ds(out_i, 4)], o_inner)])

    def add(i, carry):
        base[i] = base[i] + u[5 + i]
        return carry

    lax.fori_loop(0, 8, add, 0)
    end = pltpu.make_async_copy(base, o_base, sems.at[2])
    end.start()
    wait(*out)
    end.wait()


def last_block(*args):
    return pl.pallas_call(
        last_kernel,
        out_shape=(sds(8, LON, LEV), sds(4, LON, LEV), sds(4, LON, LEV)),
        in_specs=[SM] + [ANY] * 4 + [VM] + [ANY] * 5 + [VM],
        out_specs=(ANY,) * 3,
        scratch_shapes=BLOCK_SCRATCH
        + [
            U_SCRATCH,
            pltpu.VMEM((8, LON, 128), F32),
            pltpu.VMEM((8, LON, 128), F32),
            COLS,
            dma_sems(10),
        ],
        compiler_params=params(),
        cost_estimate=cost(15),
        name="last_block",
    )(*args)


def offer_kernel(me, send_rows, surf, o):
    o[...] = jnp.zeros((512, 128), F32)
    for off in OFFSETS:
        t = lax.rem(me[0] + (off + 64), 64) * 8
        for q in range(8):
            o[pl.ds(t + q, 1), :] = surf[pl.ds(send_rows[t + q], 1), :]


def offer(me, send_rows, surf):
    return pl.pallas_call(
        offer_kernel,
        out_shape=sds(512, 128),
        in_specs=[SM, SM, VM],
        out_specs=VM,
        name="offer",
    )(me, send_rows, surf)


LIVE = 48


def remap_kernel(me, ids, pick, dest, arrived, w, sea, o, o_outer, o_inner):
    def step(i, acc):
        for q in range(4):
            k = 4 * i + q
            x = arrived[pl.ds(pick[k], 1), :]
            red = jnp.sum(w[ids[k]] * x, axis=1, keepdims=True)
            acc = acc + jnp.where(lanes() == dest[k], red, 0.0)
        return acc

    acc = lax.fori_loop(0, LIVE // 4, step, jnp.zeros((128, 128), F32))
    o[...] = acc.T[0:32] * sea[...]
    e_o, e_i = near_far(0, 16, parity(me))
    o_outer[...] = o[pl.ds(pl.multiple_of(e_o, 16), 16)]
    o_inner[...] = o[pl.ds(pl.multiple_of(e_i, 16), 16)]


def remap(me, ids, pick, dest, arrived, w, sea):
    return pl.pallas_call(
        remap_kernel,
        out_shape=(sds(32, 128), sds(16, 128), sds(16, 128)),
        in_specs=[SM, SM, SM, SM, VM, VM, VM],
        out_specs=(VM,) * 3,
        compiler_params=params(16),
        cost_estimate=cost(3),
        name="remap",
    )(me, ids, pick, dest, arrived, w, sea)


def remap_back_kernel(me, ids, pick, dest, s, so, si, w, sea, o, cols, wide):
    e_o, e_i = near_far(0, 16, parity(me))
    cols[pl.ds(pl.multiple_of(e_o, 16), 16)] = so[...]
    cols[pl.ds(pl.multiple_of(e_i, 16), 16)] = si[...]
    clear_ends(me, ((cols, 0, 16),), ((cols, 16, 16),))
    cols[0:32] = (cols[0:32] + s[...]) * sea[...]
    cols[32:128] = jnp.zeros((96, 128), F32)
    cols[...] = cols[...].T
    for p in range(32):
        wide[p] = jnp.broadcast_to(cols[:, p : p + 1], (128, 128))
    o[...] = jnp.zeros((512, 128), F32)

    def step(i, carry):
        for q in range(4):
            k = 4 * i + q
            red = jnp.sum(w[ids[k]] * wide[dest[k]], axis=0, keepdims=True)
            o[pl.ds(pick[k], 1), :] = red
        return carry

    lax.fori_loop(0, LIVE // 4, step, 0)


def remap_back(me, ids, pick, dest, s, so, si, w, sea):
    return pl.pallas_call(
        remap_back_kernel,
        out_shape=sds(512, 128),
        in_specs=[SM, SM, SM, SM, VM, VM, VM, VM, VM],
        out_specs=VM,
        scratch_shapes=[COLS, pltpu.VMEM((32, 128, 128), F32)],
        compiler_params=params(16),
        cost_estimate=cost(3),
        name="remap_back",
    )(me, ids, pick, dest, s, so, si, w, sea)


def collect_kernel(me, send_rows, got, o):
    o[...] = jnp.zeros((32, 128), F32)
    for off in OFFSETS:
        t = lax.rem(me[0] + (off + 64), 64) * 8
        for q in range(8):
            at = pl.ds(send_rows[t + q], 1)
            o[at, :] = o[at, :] + got[pl.ds(t + q, 1), :]


def collect(me, send_rows, got):
    return pl.pallas_call(
        collect_kernel,
        out_shape=sds(32, 128),
        in_specs=[SM, SM, VM],
        out_specs=VM,
        name="collect",
    )(me, send_rows, got)


def shards(
    starting_perturbation,
    measured_discrepancy,
    diffusion,
    vert_mix,
    ocean_mask,
    pair_tile,
    pair_patch,
    dest_patch,
    pair_blocks,
    remap_weight,
):
    component = lax.axis_index("comp")
    own_tile = lax.axis_index("tile")
    across = [(i, (i + 1 if i % 2 else i - 1) % 64) for i in range(64)]
    on_chip = [(i, i ^ 1) for i in range(64)]

    def far(x):
        return lax.ppermute(x, "tile", across)

    def near(x):
        return lax.ppermute(x, "tile", on_chip)

    def swap(x):
        return lax.ppermute(x, "comp", [(0, 1), (1, 0)])

    def exchange(x):
        x = x.reshape(64, 8, 128)
        x = lax.all_to_all(x, "tile", split_axis=0, concat_axis=0, tiled=True)
        return x.reshape(512, 128)

    me = own_tile.reshape(1)
    so, si = start_in(me, starting_perturbation.reshape(1024, LON))
    ho, hi = far(so), near(si)
    sea = jnp.where(component == 1, ocean_mask.astype(F32), 1.0)
    sea32 = sea.reshape(32, 128)
    d_o, d_i, dt = diff_in(me, diffusion.reshape(1024, LON), sea)
    do, di = far(d_o), near(d_i)
    w2f, w2b = mixes(vert_mix[0])

    slots = jnp.arange(64, dtype=jnp.int32)
    live = slots % 8 < jnp.repeat(pair_blocks[0, 0], 8)
    place = jnp.sum((slots[None, :] < slots[:, None]) & live[None, :], axis=1)
    chosen = ((place[None, :] == slots[:LIVE, None]) & live[None, :]).astype(jnp.int32)
    ids = jnp.sum(chosen * slots[None, :], axis=1)
    pick = jnp.repeat(pair_tile[component, own_tile], 8) * 8 + slots % 8
    pick = jnp.sum(chosen * pick[None, :], axis=1)
    dest = jnp.sum(chosen * dest_patch[0, 0][None, :], axis=1)
    hits = (pair_tile[component] == own_tile).astype(jnp.int32)
    sources = pair_patch[component].reshape(64, 8, 8)
    send_rows = jnp.sum(hits[:, :, None] * sources, axis=1).reshape(512)
    weights = remap_weight[0]
    measured = to_rows(measured_discrepancy.reshape(1024, LON))
    ho, hi, do, di, w2f, w2b, ids, pick, dest, send_rows, measured, sea32 = (
        lax.optimization_barrier(
            (ho, hi, do, di, w2f, w2b, ids, pick, dest, send_rows, measured, sea32)
        )
    )

    v0, v1, v2, surf = first_block(me, so, si, ho, hi, dt, do, di, w2f)
    other = swap(surf)
    h0, h2 = far(v0), near(v2)
    offered = offer(me, send_rows, other)
    arrived = exchange(offered)
    v1s, arrived = lax.optimization_barrier((v1, arrived))
    h1 = far(v1s)
    fix, fix_o, fix_i = remap(me, ids, pick, dest, arrived, weights, sea32)
    fo, fi = far(fix_o), near(fix_i)
    final, adj, a0, a1, a2, s0, s0_o, s0_i = middle_block(
        me, v0, v1, v2, h0, h1, h2, fix, fo, fi, dt, do, di, measured, w2f, w2b
    )
    ro, ri = far(s0_o), near(s0_i)
    a0, a2, ro, ri = lax.optimization_barrier((a0, a2, ro, ri))
    r0, r2 = far(a0), near(a2)
    offered = remap_back(me, ids, pick, dest, s0, ro, ri, weights, sea32)
    back = exchange(offered)
    a1, back = lax.optimization_barrier((a1, back))
    r1 = far(a1)
    back = swap(collect(me, send_rows, back))
    base, g_o, g_i = last_block(me, adj, r0, r1, r2, back, so, si, dt, do, di, w2b)
    go, gi = far(g_o), near(g_i)
    final_raw = to_raw(final)
    gradient = grad_out(me, base, go, gi)
    shape = starting_perturbation.shape
    return final_raw.reshape(shape), gradient.reshape(shape)


def solution(mesh):
    field = P("comp", None, "tile", None)
    placed = (
        field,
        field,
        field,
        P("comp", None, None),
        P("tile", None),
        P(),
        P(),
        P("comp", "tile", None),
        P("comp", "tile", None),
        P("comp", "tile", None, None),
    )

    return jax.shard_map(
        shards,
        mesh=mesh,
        in_specs=placed,
        out_specs=(field, field),
        check_vma=False,
    )
```

```python
import jax
import jax.numpy as jnp
from jax import lax
from jax.experimental import pallas as pl
from jax.experimental.pallas import tpu as pltpu
from jax.sharding import PartitionSpec as P


F32 = jnp.float32
BF = jnp.bfloat16
LON, LEV = 512, 128
OFF, PAD = 8, 528
NR = 18
VM = pl.BlockSpec(memory_space=pltpu.VMEM)
SM = pl.BlockSpec(memory_space=pltpu.SMEM)
BLOCK_MIB = 44
OFFSETS = tuple(range(-7, 8)) + (32,)


def sds(*shape, dtype=F32):
    return jax.ShapeDtypeStruct(shape, dtype)


def cost(us):
    return pl.CostEstimate(flops=int(us * 5e8), bytes_accessed=1 << 20, transcendentals=0)


def params(mib=BLOCK_MIB):
    return pltpu.CompilerParams(vmem_limit_bytes=mib * 2**20)


def parity(me):
    return lax.rem(me[0], 2)


def halves(x):
    hi = x.astype(BF)
    return hi, (x - hi.astype(F32)).astype(BF)


ANY = pl.BlockSpec(memory_space=pltpu.MemorySpace.HBM)
RAW = pltpu.VMEM((4, 1024, 128), F32)
ROWS = pltpu.VMEM((8, LON, LEV), F32)


def dma_sems(*n):
    return pltpu.SemaphoreType.DMA(n)


def lon_part(ref, j):
    return ref.at[:, pl.ds(128 * j, 128), :]


def start_raw(x, buf, sems):
    out = [
        pltpu.make_async_copy(x.at[:, pl.ds(128 * j, 128)], buf.at[j], sems.at[j])
        for j in range(4)
    ]
    for c in out:
        c.start()
    return out


def turned(buf, j, r):
    return buf[j, pl.ds(r, 128, stride=8), :].T


def start_in_kernel(me, x, outer, inner, full, buf, out, sems, osems):
    odd = parity(me)
    c = start_raw(x, buf, sems)
    todo = []
    for j in range(4):
        c[j].wait()
        for r in range(8):
            out[r, pl.ds(128 * j, 128), :] = turned(buf, j, r)
        for i, (r0, n, dst) in enumerate(((7 * odd, 1, outer), (7 - 7 * odd, 1, inner), (0, 8, full))):
            src = out.at[pl.ds(r0, n), pl.ds(128 * j, 128), :]
            todo.append(pltpu.make_async_copy(src, lon_part(dst, j), osems.at[i, j]))
            todo[-1].start()
    for d in todo:
        d.wait()


def start_in(me, x):
    return pl.pallas_call(
        start_in_kernel,
        out_shape=(sds(1, LON, LEV), sds(1, LON, LEV), sds(8, LON, LEV)),
        in_specs=[SM, ANY],
        out_specs=(ANY,) * 3,
        scratch_shapes=[RAW, ROWS, dma_sems(4), dma_sems(3, 4)],
        compiler_params=params(60),
        cost_estimate=cost(4),
        name="start_in",
    )(me, x)


def diff_in_kernel(me, x, sea, outer, third, inner, full, buf, out, sems, osems):
    odd = parity(me)
    c = start_raw(x, buf, sems)
    todo = []
    for j in range(4):
        c[j].wait()
        at = pl.ds(128 * j, 128)
        for r in range(8):
            out[r, at, :] = (buf[j, pl.ds(r, 128, stride=8), :] * sea[r : r + 1, at]).T
        for i, (r0, n, dst) in enumerate(((6 * odd, 2, outer), (2 + 3 * odd, 1, third), (5 - 5 * odd, 3, inner), (0, 8, full))):
            src = out.at[pl.ds(r0, n), at, :]
            todo.append(pltpu.make_async_copy(src, lon_part(dst, j), osems.at[i, j]))
            todo[-1].start()
    for d in todo:
        d.wait()


def diff_in(me, x, sea):
    return pl.pallas_call(
        diff_in_kernel,
        out_shape=(sds(2, LON, LEV), sds(1, LON, LEV), sds(3, LON, LEV), sds(8, LON, LEV)),
        in_specs=[SM, ANY, VM],
        out_specs=(ANY,) * 4,
        scratch_shapes=[RAW, ROWS, dma_sems(4), dma_sems(4, 4)],
        compiler_params=params(60),
        cost_estimate=cost(4),
        name="diff_in",
    )(me, x, sea)


def to_rows_kernel(x, o, buf, out, sems, osems):
    c = start_raw(x, buf, sems)
    todo = []
    for j in range(4):
        c[j].wait()
        for r in range(8):
            out[r, pl.ds(128 * j, 128), :] = turned(buf, j, r)
        todo.append(pltpu.make_async_copy(lon_part(out, j), lon_part(o, j), osems.at[j]))
        todo[-1].start()
    for d in todo:
        d.wait()


def to_rows(x):
    return pl.pallas_call(
        to_rows_kernel,
        out_shape=sds(8, LON, LEV),
        in_specs=[ANY],
        out_specs=ANY,
        scratch_shapes=[RAW, ROWS, dma_sems(4), dma_sems(4)],
        compiler_params=params(),
        cost_estimate=cost(4),
        name="to_rows",
    )(x)


def to_raw_kernel(x, o):
    for r in range(8):
        o[pl.ds(r, 128, stride=8), :] = x[r].T


def to_raw(x):
    return pl.pallas_call(
        to_raw_kernel,
        grid=(4,),
        out_shape=sds(1024, LON),
        in_specs=[pl.BlockSpec((8, 128, 128), lambda j: (0, j, 0))],
        out_specs=pl.BlockSpec((1024, 128), lambda j: (0, j)),
        compiler_params=params(),
        cost_estimate=cost(4),
        name="to_raw",
    )(x)


def grad_out_kernel(me, x, outer, inner, o, base, add, buf, sems, osems):
    odd = parity(me)
    c = []
    for j in range(4):
        at = pl.ds(128 * j, 128)
        for i, (src, dst) in enumerate(
            (
                (lon_part(outer, j), add.at[pl.ds(4 * odd, 4), at, :]),
                (lon_part(inner, j), add.at[pl.ds(4 - 4 * odd, 4), at, :]),
                (lon_part(x, j), lon_part(base, j)),
            )
        ):
            c.append(pltpu.make_async_copy(src, dst, sems.at[i, j]))
            c[-1].start()
    keep_up = jnp.where(me[0] > 0, 1.0, 0.0)
    keep_dn = jnp.where(me[0] < 63, 1.0, 0.0)
    todo = []
    for j in range(4):
        at = pl.ds(128 * j, 128)
        for d in c[3 * j : 3 * j + 3]:
            d.wait()
        for r in range(8):
            keep = keep_up if r < 4 else keep_dn
            buf[j, pl.ds(r, 128, stride=8), :] = (base[r, at, :] + keep * add[r, at, :]).T
        todo.append(pltpu.make_async_copy(buf.at[j], o.at[:, at], osems.at[j]))
        todo[-1].start()
    for d in todo:
        d.wait()


def grad_out(me, x, outer, inner):
    return pl.pallas_call(
        grad_out_kernel,
        out_shape=sds(1024, LON),
        in_specs=[SM, ANY, ANY, ANY],
        out_specs=ANY,
        scratch_shapes=[ROWS, ROWS, RAW, dma_sems(3, 4), dma_sems(4)],
        compiler_params=params(),
        cost_estimate=cost(4),
        name="grad_out",
    )(me, x, outer, inner)


def mix_kernel(w, fwd, bwd):
    for dst, x in ((fwd, w[...].T), (bwd, w[...])):
        hi, lo = halves(x)
        dst[0:128, 0:128] = hi
        dst[128:256, 0:128] = hi
        dst[0:128, 128:256] = lo
        dst[128:256, 128:256] = jnp.zeros((128, 128), BF)


def mixes(w):
    return pl.pallas_call(
        mix_kernel,
        out_shape=(sds(256, 256, dtype=BF), sds(256, 256, dtype=BF)),
        in_specs=[VM],
        out_specs=(VM, VM),
        name="mixes",
    )(w)


def put(v, r, j, new):
    v[r, pl.ds(OFF + 128 * j, 128), :] = new
    if j == 0:
        v[r, pl.ds(OFF + LON, 1), :] = new[0:1]
    if j == 3:
        v[r, pl.ds(OFF - 1, 1), :] = new[127:128]


def put_halves(h, r, j, new):
    hi, lo = halves(new)
    h[r, pl.ds(128 * j, 128), 0:128] = hi
    h[r, pl.ds(128 * j, 128), 128:256] = lo


def around(v, r, j):
    at = OFF + 128 * j
    n = v[r - 1, pl.ds(at, 128), :] + v[r + 1, pl.ds(at, 128), :]
    return n + (v[r, pl.ds(at - 1, 128), :] + v[r, pl.ds(at + 1, 128), :])


GROUP = {14: 7, 12: 6, 10: 5, 8: 4}


def mixed_rows(h, w2, lo, n, body):
    k = GROUP[n]

    def step(i, carry):
        r0 = lo + k * i
        y = jnp.dot(h[pl.ds(r0, k)].reshape(LON * k, 256), w2[...], preferred_element_type=F32)
        for q in range(k):
            for j in range(4):
                part = y[LON * q + 128 * j : LON * q + 128 * j + 128]
                body(r0 + q, j, part[:, 0:128] + part[:, 128:256])
        return carry

    lax.fori_loop(0, n // k, step, 0)


def forward_step(va, vb, h, d, w2, s, first=False, last=False):
    def body(r, j, y):
        c = va[r, pl.ds(OFF + 128 * j, 128), :]
        dd = d[r, pl.ds(128 * j, 128), :]
        n = dd * (around(va, r, j) - 4.0 * c)
        if first:
            c = jnp.where(dd > 0.0, c, 0.0)
        new = (c + n) + y
        put(vb, r, j, new)
        if not last:
            put_halves(h, r, j, new)

    mixed_rows(h, w2, 1 + s, 16 - 2 * s, body)


def push_step(ga, gb, u, h, d, w2, s, last=False):
    def finish(r, j, new, dd):
        u[r, pl.ds(128 * j, 128), :] = new
        put(gb, r, j, dd * new)
        put_halves(h, r, j, new)

    def body(r, j, y):
        at = pl.ds(128 * j, 128)
        n = around(ga, r, j) - 4.0 * ga[r, pl.ds(OFF + 128 * j, 128), :]
        c = u[r, at, :]
        if last:
            u[r, at, :] = (c + n) + y
        else:
            dd = d[r, at, :]
            finish(r, j, (c + jnp.where(dd > 0.0, n, 0.0)) + y, dd)

    mixed_rows(h, w2, 6 - s, 6 + 2 * s, body)
    for r, near in ((5 - s, 6 - s), (12 + s, 11 + s)):
        for j in range(4):
            at = pl.ds(128 * j, 128)
            n = ga[near, pl.ds(OFF + 128 * j, 128), :]
            if last:
                u[r, at, :] = n
            else:
                dd = d[r, at, :]
                finish(r, j, jnp.where(dd > 0.0, n, 0.0), dd)


def push_block(ga, gb, u, h, d, w2):
    for s, g in ((1, ga), (2, gb), (3, ga), (4, gb)):
        g[5 - s] = jnp.zeros((PAD, 128), F32)
        g[12 + s] = jnp.zeros((PAD, 128), F32)
    push_step(ga, gb, u, h, d, w2, 1)
    push_step(gb, ga, u, h, d, w2, 2)
    push_step(ga, gb, u, h, d, w2, 3)
    push_step(gb, ga, u, h, d, w2, 4, last=True)


def forward_block(va, vb, h, d, w2, first=False):
    forward_step(va, vb, h, d, w2, 1, first=first)
    forward_step(vb, va, h, d, w2, 2)
    forward_step(va, vb, h, d, w2, 3)
    forward_step(vb, va, h, d, w2, 4, last=True)


def copies(sems, pairs):
    out = [pltpu.make_async_copy(a, b, sems.at[i]) for i, (a, b) in enumerate(pairs)]
    for c in out:
        c.start()
    return out


def wait(*todo):
    for c in todo:
        c.wait()


def plain_rows(v, r0, n):
    return v.at[pl.ds(r0, n)]


def tile_rows(v, r0, n):
    return v.at[pl.ds(r0, n), pl.ds(OFF, LON), :]


def clear_ends(me, up, dn):
    for edge, todo in ((0, up), (63, dn)):

        @pl.when(me[0] == edge)
        def _(todo=todo):
            for ref, r0, n in todo:
                ref[pl.ds(r0, n)] = jnp.zeros((n,) + ref.shape[1:], F32)


def lanes():
    return lax.broadcasted_iota(jnp.int32, (128, 128), 1)


def gather_surface(read, count):
    def step(r, acc):
        for j in range(4):
            p = 4 * r + j
            acc = jnp.where(lanes() == p, pltpu.roll(read(r, j), p, 1), acc)
        return acc

    return lax.fori_loop(0, count, step, jnp.zeros((128, 128), F32)).T


def spread_column(cols, p):
    return jnp.where(lanes() == 0, pltpu.roll(cols, (128 - p) % 128, 1), 0.0)


BLOCK_SCRATCH = [
    pltpu.VMEM((NR, PAD, 128), F32),
    pltpu.VMEM((NR, PAD, 128), F32),
    pltpu.VMEM((NR, LON, 256), BF),
    pltpu.VMEM((NR, LON, 128), F32),
]
U_SCRATCH = pltpu.VMEM((NR, LON, 128), F32)
COLS = pltpu.VMEM((128, 128), F32)
PARTS = (sds(3, LON, LEV), sds(1, LON, LEV), sds(4, LON, LEV))


def near_far(up, dn, odd):
    return up + (dn - up) * odd, dn + (up - dn) * odd


def edge_refs(v, up, dn, odd, cut):
    outer, inner = near_far(up, dn, odd)
    return cut(v, outer, 3), cut(v, outer + 3, 1), cut(v, inner, 4)


def diffusion_copies(d, odd, dt, do, dx, di):
    return [
        (dt, d.at[pl.ds(5, 8)]),
        (do, d.at[pl.ds(3 + 10 * odd, 2)]),
        (di, d.at[pl.ds(13 - 11 * odd, 3)]),
    ] + ([] if dx is None else [(dx, d.at[pl.ds(2 + 13 * odd, 1)])])


def prepare_rows(va, h, r0, n, d=None):
    def cp(i, carry):
        r = r0 + i
        for j in range(4):
            x = va[r, pl.ds(OFF + 128 * j, 128), :]
            if j == 0:
                va[r, pl.ds(OFF + LON, 1), :] = x[0:1]
            if j == 3:
                va[r, pl.ds(OFF - 1, 1), :] = x[127:128]
            if d is not None:
                x = jnp.where(d[r, pl.ds(128 * j, 128), :] > 0.0, x, 0.0)
            put_halves(h, r, j, x)
        return carry

    lax.fori_loop(0, n, cp, 0)


def first_step_kernel(me, own, eo, ei, dt, w2, o_outer, o_inner, o_own, va, vb, h, d, sems):
    odd = parity(me)
    c = copies(
        sems,
        [
            (dt, d.at[pl.ds(5, 8)]),
            (own, tile_rows(va, 5, 8)),
            (eo, tile_rows(va, 4 + 9 * odd, 1)),
            (ei, tile_rows(va, 13 - 9 * odd, 1)),
        ],
    )
    wait(*c[0:2])
    prepare_rows(va, h, 5, 8, d)
    wait(*c[2:4])
    clear_ends(me, ((va, 4, 1),), ((va, 13, 1),))
    forward_step(va, vb, h, d, w2, 4, first=True, last=True)
    c = copies(
        sems,
        [
            (tile_rows(vb, 5 + 5 * odd, 3), o_outer),
            (tile_rows(vb, 10 - 5 * odd, 3), o_inner),
            (tile_rows(vb, 5, 8), o_own),
        ],
    )
    wait(*c)


def first_step(*args):
    return pl.pallas_call(
        first_step_kernel,
        out_shape=(sds(3, LON, LEV), sds(3, LON, LEV), sds(8, LON, LEV)),
        in_specs=[SM] + [ANY] * 4 + [VM],
        out_specs=(ANY,) * 3,
        scratch_shapes=BLOCK_SCRATCH + [dma_sems(4)],
        compiler_params=params(60),
        cost_estimate=cost(4),
        name="first_step",
    )(*args)


def first_kernel(me, own, ho, hi, dt, do, di, w2, o0, o1, o2, o_surf, va, vb, h, d, sems):
    odd = parity(me)
    c = copies(
        sems,
        [
            (own, tile_rows(va, 5, 8)),
            (ho, tile_rows(va, 2 + 11 * odd, 3)),
            (hi, tile_rows(va, 13 - 11 * odd, 3)),
        ]
        + diffusion_copies(d, odd, dt, do, None, di),
    )
    wait(c[0])
    prepare_rows(va, h, 5, 8)
    wait(*c[1:])
    clear_ends(me, ((va, 2, 3), (d, 2, 3)), ((va, 13, 3), (d, 13, 3)))
    prepare_rows(va, h, 3, 2)
    prepare_rows(va, h, 13, 2)
    forward_step(va, vb, h, d, w2, 2)
    forward_step(vb, va, h, d, w2, 3)
    forward_step(va, vb, h, d, w2, 4, last=True)
    c = copies(sems, list(zip(edge_refs(vb, 5, 9, odd, tile_rows), (o0, o1, o2))))
    o_surf[...] = gather_surface(lambda r, j: vb[r + 5, pl.ds(OFF + 128 * j, 128), :], 8)[0:32]
    wait(*c)


def first_block(*args):
    return pl.pallas_call(
        first_kernel,
        out_shape=PARTS + (sds(32, 128),),
        in_specs=[SM] + [ANY] * 6 + [VM],
        out_specs=(ANY,) * 3 + (VM,),
        scratch_shapes=BLOCK_SCRATCH + [dma_sems(6)],
        compiler_params=params(),
        cost_estimate=cost(10),
        name="first_block",
    )(*args)


def middle_kernel(
    me, v0, v1, v2, h0, h1, h2, s, so, si, dt, do, dx, di, m, w2f, w2b,
    o_final, o_adj, o0, o1, o2, o_s, o_so, o_si, va, vb, h, d, u, mm, cols, sems,
):
    odd = parity(me)
    own = edge_refs(va, 5, 9, odd, tile_rows)
    far = edge_refs(va, 1, 13, odd, tile_rows)
    c = copies(
        sems,
        [
            (v0, own[0]),
            (v1, own[1]),
            (v2, own[2]),
            (h0, far[0]),
            (h1, far[1]),
            (h2, far[2]),
        ]
        + diffusion_copies(d, odd, dt, do, dx, di)
        + [(m, mm)],
    )
    c_o, c_i = near_far(0, 48, odd)
    cols[pl.ds(pl.multiple_of(c_o, 16), 16)] = so[...]
    cols[pl.ds(pl.multiple_of(c_i, 16), 16)] = si[...]
    cols[16:48] = s[...]
    cols[64:128] = jnp.zeros((64, 128), F32)
    clear_ends(me, ((cols, 0, 16),), ((cols, 48, 16),))
    cols[...] = cols[...].T

    def prepare(r0):
        def cp(i, carry):
            r = r0 + i
            for j in range(4):
                x = va[r, pl.ds(OFF + 128 * j, 128), :]
                x = x + spread_column(cols[...], 4 * (r - 1) + j)
                put(va, r, j, x)
                put_halves(h, r, j, x)
            return carry

        lax.fori_loop(0, 4, cp, 0)

    wait(*c[0:3])
    prepare(5)
    prepare(9)
    wait(*c[3:10])
    clear_ends(me, ((va, 1, 4), (d, 2, 3)), ((va, 13, 4), (d, 13, 3)))
    prepare(1)
    prepare(13)
    forward_block(va, vb, h, d, w2f)
    out = copies(sems, [(tile_rows(va, 5, 8), o_final)])
    wait(c[10])

    def body(i, carry):
        r = 5 + i
        for j in range(4):
            at = pl.ds(128 * j, 128)
            x = va[r, pl.ds(OFF + 128 * j, 128), :] - mm[i, at, :]
            dd = d[r, at, :]
            x = jnp.where(dd > 0.0, x, 0.0)
            u[r, at, :] = x
            put(vb, r, j, dd * x)
            put_halves(h, r, j, x)
        return carry

    lax.fori_loop(0, 8, body, 0)
    wait(*out)
    push_block(vb, va, u, h, d, w2b)
    out = copies(
        sems,
        list(zip(edge_refs(u, 1, 13, odd, plain_rows), (o0, o1, o2)))
        + [(u.at[pl.ds(5, 8)], o_adj)],
    )
    cols[...] = gather_surface(lambda r, j: u[r + 1, pl.ds(128 * j, 128), :], 16)
    o_so[...] = cols[pl.ds(pl.multiple_of(c_o, 16), 16)]
    o_s[...] = cols[16:48]
    o_si[...] = cols[pl.ds(pl.multiple_of(c_i, 16), 16)]
    wait(*out)


def middle_block(*args):
    return pl.pallas_call(
        middle_kernel,
        out_shape=(
            sds(8, LON, LEV), sds(8, LON, LEV), *PARTS,
            sds(32, 128), sds(16, 128), sds(16, 128),
        ),
        in_specs=[SM] + [ANY] * 6 + [VM] * 3 + [ANY] * 5 + [VM] * 2,
        out_specs=(ANY,) * 5 + (VM,) * 3,
        scratch_shapes=BLOCK_SCRATCH
        + [U_SCRATCH, pltpu.VMEM((8, LON, 128), F32), COLS, dma_sems(12)],
        compiler_params=params(),
        cost_estimate=cost(30),
        name="middle_block",
    )(*args)


def last_kernel(
    me, adj, r0, r1, r2, s, own, dt, do, dx, di, w2b, o_base, o_outer, o_inner,
    va, vb, h, d, u, got, base, cols, sems,
):
    odd = parity(me)
    parts = edge_refs(got, 0, 4, odd, plain_rows)
    c = copies(
        sems,
        [
            (adj, u.at[pl.ds(5, 8)]),
            (r0, parts[0]),
            (r1, parts[1]),
            (r2, parts[2]),
        ]
        + diffusion_copies(d, odd, dt, do, dx, di)
        + [(own, base)],
    )
    cols[0:32] = s[...]
    cols[32:128] = jnp.zeros((96, 128), F32)
    cols[...] = cols[...].T
    wait(*c[0:5])
    clear_ends(me, ((got, 0, 4),), ((got, 4, 4),))

    def cp(i, carry):
        r = 5 + i
        for j in range(4):
            at = pl.ds(128 * j, 128)
            x = u[r, at, :] + got[i, at, :]
            x = x + spread_column(cols[...], 4 * i + j)
            dd = d[r, at, :]
            x = jnp.where(dd > 0.0, x, 0.0)
            u[r, at, :] = x
            put(vb, r, j, dd * x)
            put_halves(h, r, j, x)
        return carry

    lax.fori_loop(0, 8, cp, 0)
    wait(*c[5:9])
    clear_ends(me, ((d, 2, 3),), ((d, 13, 3),))
    push_block(vb, va, u, h, d, w2b)
    out_o, out_i = near_far(1, 13, odd)
    out = copies(sems, [(u.at[pl.ds(out_o, 4)], o_outer), (u.at[pl.ds(out_i, 4)], o_inner)])

    def add(i, carry):
        base[i] = base[i] + u[5 + i]
        return carry

    lax.fori_loop(0, 8, add, 0)
    end = pltpu.make_async_copy(base, o_base, sems.at[2])
    end.start()
    wait(*out)
    end.wait()


def last_block(*args):
    return pl.pallas_call(
        last_kernel,
        out_shape=(sds(8, LON, LEV), sds(4, LON, LEV), sds(4, LON, LEV)),
        in_specs=[SM] + [ANY] * 4 + [VM] + [ANY] * 5 + [VM],
        out_specs=(ANY,) * 3,
        scratch_shapes=BLOCK_SCRATCH
        + [
            U_SCRATCH,
            pltpu.VMEM((8, LON, 128), F32),
            pltpu.VMEM((8, LON, 128), F32),
            COLS,
            dma_sems(10),
        ],
        compiler_params=params(),
        cost_estimate=cost(15),
        name="last_block",
    )(*args)


def offer_kernel(me, send_rows, surf, o):
    o[...] = jnp.zeros((512, 128), F32)
    for off in OFFSETS:
        t = lax.rem(me[0] + (off + 64), 64) * 8
        for q in range(8):
            o[pl.ds(t + q, 1), :] = surf[pl.ds(send_rows[t + q], 1), :]


def offer(me, send_rows, surf):
    return pl.pallas_call(
        offer_kernel,
        out_shape=sds(512, 128),
        in_specs=[SM, SM, VM],
        out_specs=VM,
        name="offer",
    )(me, send_rows, surf)


LIVE = 48


def remap_kernel(me, ids, pick, dest, arrived, w, sea, o, o_outer, o_inner):
    def step(i, acc):
        for q in range(4):
            k = 4 * i + q
            x = arrived[pl.ds(pick[k], 1), :]
            red = jnp.sum(w[ids[k]] * x, axis=1, keepdims=True)
            acc = acc + jnp.where(lanes() == dest[k], red, 0.0)
        return acc

    acc = lax.fori_loop(0, LIVE // 4, step, jnp.zeros((128, 128), F32))
    o[...] = acc.T[0:32] * sea[...]
    e_o, e_i = near_far(0, 16, parity(me))
    o_outer[...] = o[pl.ds(pl.multiple_of(e_o, 16), 16)]
    o_inner[...] = o[pl.ds(pl.multiple_of(e_i, 16), 16)]


def remap(me, ids, pick, dest, arrived, w, sea):
    return pl.pallas_call(
        remap_kernel,
        out_shape=(sds(32, 128), sds(16, 128), sds(16, 128)),
        in_specs=[SM, SM, SM, SM, VM, VM, VM],
        out_specs=(VM,) * 3,
        compiler_params=params(16),
        cost_estimate=cost(3),
        name="remap",
    )(me, ids, pick, dest, arrived, w, sea)


def remap_back_kernel(me, ids, pick, dest, s, so, si, w, sea, o, cols, wide):
    e_o, e_i = near_far(0, 16, parity(me))
    cols[pl.ds(pl.multiple_of(e_o, 16), 16)] = so[...]
    cols[pl.ds(pl.multiple_of(e_i, 16), 16)] = si[...]
    clear_ends(me, ((cols, 0, 16),), ((cols, 16, 16),))
    cols[0:32] = (cols[0:32] + s[...]) * sea[...]
    cols[32:128] = jnp.zeros((96, 128), F32)
    cols[...] = cols[...].T
    for p in range(32):
        wide[p] = jnp.broadcast_to(cols[:, p : p + 1], (128, 128))
    o[...] = jnp.zeros((512, 128), F32)

    def step(i, carry):
        for q in range(4):
            k = 4 * i + q
            red = jnp.sum(w[ids[k]] * wide[dest[k]], axis=0, keepdims=True)
            o[pl.ds(pick[k], 1), :] = red
        return carry

    lax.fori_loop(0, LIVE // 4, step, 0)


def remap_back(me, ids, pick, dest, s, so, si, w, sea):
    return pl.pallas_call(
        remap_back_kernel,
        out_shape=sds(512, 128),
        in_specs=[SM, SM, SM, SM, VM, VM, VM, VM, VM],
        out_specs=VM,
        scratch_shapes=[COLS, pltpu.VMEM((32, 128, 128), F32)],
        compiler_params=params(16),
        cost_estimate=cost(3),
        name="remap_back",
    )(me, ids, pick, dest, s, so, si, w, sea)


def collect_kernel(me, send_rows, got, o):
    o[...] = jnp.zeros((32, 128), F32)
    for off in OFFSETS:
        t = lax.rem(me[0] + (off + 64), 64) * 8
        for q in range(8):
            at = pl.ds(send_rows[t + q], 1)
            o[at, :] = o[at, :] + got[pl.ds(t + q, 1), :]


def collect(me, send_rows, got):
    return pl.pallas_call(
        collect_kernel,
        out_shape=sds(32, 128),
        in_specs=[SM, SM, VM],
        out_specs=VM,
        name="collect",
    )(me, send_rows, got)


def shards(
    starting_perturbation,
    measured_discrepancy,
    diffusion,
    vert_mix,
    ocean_mask,
    pair_tile,
    pair_patch,
    dest_patch,
    pair_blocks,
    remap_weight,
):
    component = lax.axis_index("comp")
    own_tile = lax.axis_index("tile")
    across = [(i, min(max(i + 1 if i % 2 else i - 1, 0), 63)) for i in range(64)]
    on_chip = [(i, i ^ 1) for i in range(64)]

    def far(x):
        return lax.ppermute(x, "tile", across)

    def near(x):
        return lax.ppermute(x, "tile", on_chip)

    def swap(x):
        return lax.ppermute(x, "comp", [(0, 1), (1, 0)])

    def exchange(x):
        x = x.reshape(64, 8, 128)
        x = lax.all_to_all(x, "tile", split_axis=0, concat_axis=0, tiled=True)
        return x.reshape(512, 128)

    me = own_tile.reshape(1)
    e_o, e_i, start = start_in(me, starting_perturbation.reshape(1024, LON))
    eo, ei = far(e_o), near(e_i)
    sea = jnp.where(component == 1, ocean_mask.astype(F32), 1.0)
    sea32 = sea.reshape(32, 128)
    d_o, d_x, d_i, dt = diff_in(me, diffusion.reshape(1024, LON), sea)
    do, di = far(d_o), near(d_i)
    w2f, w2b = mixes(vert_mix[0])
    s_o, s_i, one = first_step(me, start, eo, ei, dt, w2f)
    ho, hi = far(s_o), near(s_i)
    dx = far(d_x)

    slots = jnp.arange(64, dtype=jnp.int32)
    live = slots % 8 < jnp.repeat(pair_blocks[0, 0], 8)
    place = jnp.sum((slots[None, :] < slots[:, None]) & live[None, :], axis=1)
    chosen = ((place[None, :] == slots[:LIVE, None]) & live[None, :]).astype(jnp.int32)
    ids = jnp.sum(chosen * slots[None, :], axis=1)
    pick = jnp.repeat(pair_tile[component, own_tile], 8) * 8 + slots % 8
    pick = jnp.sum(chosen * pick[None, :], axis=1)
    dest = jnp.sum(chosen * dest_patch[0, 0][None, :], axis=1)
    hits = (pair_tile[component] == own_tile).astype(jnp.int32)
    sources = pair_patch[component].reshape(64, 8, 8)
    send_rows = jnp.sum(hits[:, :, None] * sources, axis=1).reshape(512)
    weights = remap_weight[0]
    measured = to_rows(measured_discrepancy.reshape(1024, LON))
    ho, hi, do, di, w2b, ids, pick, dest, send_rows, measured, sea32 = (
        lax.optimization_barrier(
            (ho, hi, do, di, w2b, ids, pick, dest, send_rows, measured, sea32)
        )
    )

    v0, v1, v2, surf = first_block(me, one, ho, hi, dt, do, di, w2f)
    other = swap(surf)
    h0, h2 = far(v0), near(v2)
    offered = offer(me, send_rows, other)
    arrived = exchange(offered)
    v1s, arrived = lax.optimization_barrier((v1, arrived))
    h1 = far(v1s)
    fix, fix_o, fix_i = remap(me, ids, pick, dest, arrived, weights, sea32)
    fo, fi = far(fix_o), near(fix_i)
    final, adj, a0, a1, a2, s0, s0_o, s0_i = middle_block(
        me, v0, v1, v2, h0, h1, h2, fix, fo, fi, dt, do, dx, di, measured, w2f, w2b
    )
    ro, ri = far(s0_o), near(s0_i)
    a0, a2, ro, ri = lax.optimization_barrier((a0, a2, ro, ri))
    r0, r2 = far(a0), near(a2)
    offered = remap_back(me, ids, pick, dest, s0, ro, ri, weights, sea32)
    back = exchange(offered)
    a1, back = lax.optimization_barrier((a1, back))
    r1 = far(a1)
    back = swap(collect(me, send_rows, back))
    base, g_o, g_i = last_block(me, adj, r0, r1, r2, back, start, dt, do, dx, di, w2b)
    go, gi = far(g_o), near(g_i)
    final_raw = to_raw(final)
    gradient = grad_out(me, base, go, gi)
    shape = starting_perturbation.shape
    return final_raw.reshape(shape), gradient.reshape(shape)


def solution(mesh):
    field = P("comp", None, "tile", None)
    placed = (
        field,
        field,
        field,
        P("comp", None, None),
        P("tile", None),
        P(),
        P(),
        P("comp", "tile", None),
        P("comp", "tile", None),
        P("comp", "tile", None, None),
    )

    return jax.shard_map(
        shards,
        mesh=mesh,
        in_specs=placed,
        out_specs=(field, field),
        check_vma=False,
    )
```

```python
import jax
import jax.numpy as jnp
from jax import lax
from jax.experimental import pallas as pl
from jax.experimental.pallas import tpu as pltpu
from jax.sharding import PartitionSpec as P


F32 = jnp.float32
BF = jnp.bfloat16
LON, LEV = 512, 128
OFF, PAD = 8, 528
NR = 18
VM = pl.BlockSpec(memory_space=pltpu.VMEM)
SM = pl.BlockSpec(memory_space=pltpu.SMEM)
BLOCK_MIB = 44
OFFSETS = tuple(range(-7, 8)) + (32,)


def sds(*shape, dtype=F32):
    return jax.ShapeDtypeStruct(shape, dtype)


def cost(us):
    return pl.CostEstimate(flops=int(us * 5e8), bytes_accessed=1 << 20, transcendentals=0)


def params(mib=BLOCK_MIB):
    return pltpu.CompilerParams(vmem_limit_bytes=mib * 2**20)


def parity(me):
    return lax.rem(me[0], 2)


def halves(x):
    hi = x.astype(BF)
    return hi, (x - hi.astype(F32)).astype(BF)


ANY = pl.BlockSpec(memory_space=pltpu.MemorySpace.HBM)
RAW = pltpu.VMEM((4, 1024, 128), F32)
ROWS = pltpu.VMEM((8, LON, LEV), F32)


def dma_sems(*n):
    return pltpu.SemaphoreType.DMA(n)


def lon_part(ref, j):
    return ref.at[:, pl.ds(128 * j, 128), :]


def start_raw(x, buf, sems):
    out = [
        pltpu.make_async_copy(x.at[:, pl.ds(128 * j, 128)], buf.at[j], sems.at[j])
        for j in range(4)
    ]
    for c in out:
        c.start()
    return out


def turned(buf, j, r):
    return buf[j, pl.ds(r, 128, stride=8), :].T


def start_in_kernel(me, x, outer, inner, full, buf, out, sems, osems):
    odd = parity(me)
    c = start_raw(x, buf, sems)
    todo = []
    for j in range(4):
        c[j].wait()
        for r in range(8):
            out[r, pl.ds(128 * j, 128), :] = turned(buf, j, r)
        for i, (r0, n, dst) in enumerate(((7 * odd, 1, outer), (7 - 7 * odd, 1, inner), (0, 8, full))):
            src = out.at[pl.ds(r0, n), pl.ds(128 * j, 128), :]
            todo.append(pltpu.make_async_copy(src, lon_part(dst, j), osems.at[i, j]))
            todo[-1].start()
    for d in todo:
        d.wait()


def start_in(me, x):
    return pl.pallas_call(
        start_in_kernel,
        out_shape=(sds(1, LON, LEV), sds(1, LON, LEV), sds(8, LON, LEV)),
        in_specs=[SM, ANY],
        out_specs=(ANY,) * 3,
        scratch_shapes=[RAW, ROWS, dma_sems(4), dma_sems(3, 4)],
        compiler_params=params(60),
        cost_estimate=cost(4),
        name="start_in",
    )(me, x)


def diff_in_kernel(me, x, mask, outer, third, inner, full, buf, out, sems, osems):
    odd = parity(me)
    c = start_raw(x, buf, sems)
    todo = []
    for j in range(4):
        c[j].wait()
        at = pl.ds(128 * j, 128)
        for r in range(8):
            sea = jnp.where(me[1] == 1, mask[r : r + 1, at].astype(F32), 1.0)
            out[r, at, :] = (buf[j, pl.ds(r, 128, stride=8), :] * sea).T
        for i, (r0, n, dst) in enumerate(((6 * odd, 2, outer), (2 + 3 * odd, 1, third), (5 - 5 * odd, 3, inner), (0, 8, full))):
            src = out.at[pl.ds(r0, n), at, :]
            todo.append(pltpu.make_async_copy(src, lon_part(dst, j), osems.at[i, j]))
            todo[-1].start()
    for d in todo:
        d.wait()


def diff_in(me, x, mask):
    return pl.pallas_call(
        diff_in_kernel,
        out_shape=(sds(2, LON, LEV), sds(1, LON, LEV), sds(3, LON, LEV), sds(8, LON, LEV)),
        in_specs=[SM, ANY, VM],
        out_specs=(ANY,) * 4,
        scratch_shapes=[RAW, ROWS, dma_sems(4), dma_sems(4, 4)],
        compiler_params=params(60),
        cost_estimate=cost(4),
        name="diff_in",
    )(me, x, mask)


def to_rows_kernel(x, o, buf, out, sems, osems):
    c = start_raw(x, buf, sems)
    todo = []
    for j in range(4):
        c[j].wait()
        for r in range(8):
            out[r, pl.ds(128 * j, 128), :] = turned(buf, j, r)
        todo.append(pltpu.make_async_copy(lon_part(out, j), lon_part(o, j), osems.at[j]))
        todo[-1].start()
    for d in todo:
        d.wait()


def to_rows(x):
    return pl.pallas_call(
        to_rows_kernel,
        out_shape=sds(8, LON, LEV),
        in_specs=[ANY],
        out_specs=ANY,
        scratch_shapes=[RAW, ROWS, dma_sems(4), dma_sems(4)],
        compiler_params=params(),
        cost_estimate=cost(4),
        name="to_rows",
    )(x)


def to_raw_kernel(x, o):
    for r in range(8):
        o[pl.ds(r, 128, stride=8), :] = x[r].T


def to_raw(x):
    return pl.pallas_call(
        to_raw_kernel,
        grid=(4,),
        out_shape=sds(1024, LON),
        in_specs=[pl.BlockSpec((8, 128, 128), lambda j: (0, j, 0))],
        out_specs=pl.BlockSpec((1024, 128), lambda j: (0, j)),
        compiler_params=params(),
        cost_estimate=cost(4),
        name="to_raw",
    )(x)


def grad_out_kernel(me, x, outer, inner, o, base, add, buf, sems, osems):
    odd = parity(me)
    c = []
    for j in range(4):
        at = pl.ds(128 * j, 128)
        for i, (src, dst) in enumerate(
            (
                (lon_part(outer, j), add.at[pl.ds(4 * odd, 4), at, :]),
                (lon_part(inner, j), add.at[pl.ds(4 - 4 * odd, 4), at, :]),
                (lon_part(x, j), lon_part(base, j)),
            )
        ):
            c.append(pltpu.make_async_copy(src, dst, sems.at[i, j]))
            c[-1].start()
    keep_up = jnp.where(me[0] > 0, 1.0, 0.0)
    keep_dn = jnp.where(me[0] < 63, 1.0, 0.0)
    todo = []
    for j in range(4):
        at = pl.ds(128 * j, 128)
        for d in c[3 * j : 3 * j + 3]:
            d.wait()
        for r in range(8):
            keep = keep_up if r < 4 else keep_dn
            buf[j, pl.ds(r, 128, stride=8), :] = (base[r, at, :] + keep * add[r, at, :]).T
        todo.append(pltpu.make_async_copy(buf.at[j], o.at[:, at], osems.at[j]))
        todo[-1].start()
    for d in todo:
        d.wait()


def grad_out(me, x, outer, inner):
    return pl.pallas_call(
        grad_out_kernel,
        out_shape=sds(1024, LON),
        in_specs=[SM, ANY, ANY, ANY],
        out_specs=ANY,
        scratch_shapes=[ROWS, ROWS, RAW, dma_sems(3, 4), dma_sems(4)],
        compiler_params=params(),
        cost_estimate=cost(4),
        name="grad_out",
    )(me, x, outer, inner)


def mix_kernel(w, fwd, bwd):
    for dst, x in ((fwd, w[...].T), (bwd, w[...])):
        hi, lo = halves(x)
        dst[0:128, 0:128] = hi
        dst[128:256, 0:128] = hi
        dst[0:128, 128:256] = lo
        dst[128:256, 128:256] = jnp.zeros((128, 128), BF)


def put(v, r, j, new):
    v[r, pl.ds(OFF + 128 * j, 128), :] = new
    if j == 0:
        v[r, pl.ds(OFF + LON, 1), :] = new[0:1]
    if j == 3:
        v[r, pl.ds(OFF - 1, 1), :] = new[127:128]


def put_halves(h, r, j, new):
    hi, lo = halves(new)
    h[r, pl.ds(128 * j, 128), 0:128] = hi
    h[r, pl.ds(128 * j, 128), 128:256] = lo


def around(v, r, j):
    at = OFF + 128 * j
    n = v[r - 1, pl.ds(at, 128), :] + v[r + 1, pl.ds(at, 128), :]
    return n + (v[r, pl.ds(at - 1, 128), :] + v[r, pl.ds(at + 1, 128), :])


GROUP = {14: 7, 12: 6, 10: 5, 8: 4}


def mixed_rows(h, w2, lo, n, body):
    k = GROUP[n]

    def step(i, carry):
        r0 = lo + k * i
        y = jnp.dot(h[pl.ds(r0, k)].reshape(LON * k, 256), w2[...], preferred_element_type=F32)
        for q in range(k):
            for j in range(4):
                part = y[LON * q + 128 * j : LON * q + 128 * j + 128]
                body(r0 + q, j, part[:, 0:128] + part[:, 128:256])
        return carry

    lax.fori_loop(0, n // k, step, 0)


def forward_step(va, vb, h, d, w2, s, first=False, last=False):
    def body(r, j, y):
        c = va[r, pl.ds(OFF + 128 * j, 128), :]
        dd = d[r, pl.ds(128 * j, 128), :]
        n = dd * (around(va, r, j) - 4.0 * c)
        if first:
            c = jnp.where(dd > 0.0, c, 0.0)
        new = (c + n) + y
        put(vb, r, j, new)
        if not last:
            put_halves(h, r, j, new)

    mixed_rows(h, w2, 1 + s, 16 - 2 * s, body)


def push_step(ga, gb, u, h, d, w2, s, last=False):
    def finish(r, j, new, dd):
        u[r, pl.ds(128 * j, 128), :] = new
        put(gb, r, j, dd * new)
        put_halves(h, r, j, new)

    def body(r, j, y):
        at = pl.ds(128 * j, 128)
        n = around(ga, r, j) - 4.0 * ga[r, pl.ds(OFF + 128 * j, 128), :]
        c = u[r, at, :]
        if last:
            u[r, at, :] = (c + n) + y
        else:
            dd = d[r, at, :]
            finish(r, j, (c + jnp.where(dd > 0.0, n, 0.0)) + y, dd)

    mixed_rows(h, w2, 6 - s, 6 + 2 * s, body)
    for r, near in ((5 - s, 6 - s), (12 + s, 11 + s)):
        for j in range(4):
            at = pl.ds(128 * j, 128)
            n = ga[near, pl.ds(OFF + 128 * j, 128), :]
            if last:
                u[r, at, :] = n
            else:
                dd = d[r, at, :]
                finish(r, j, jnp.where(dd > 0.0, n, 0.0), dd)


def push_block(ga, gb, u, h, d, w2):
    for s, g in ((1, ga), (2, gb), (3, ga), (4, gb)):
        g[5 - s] = jnp.zeros((PAD, 128), F32)
        g[12 + s] = jnp.zeros((PAD, 128), F32)
    push_step(ga, gb, u, h, d, w2, 1)
    push_step(gb, ga, u, h, d, w2, 2)
    push_step(ga, gb, u, h, d, w2, 3)
    push_step(gb, ga, u, h, d, w2, 4, last=True)


def forward_block(va, vb, h, d, w2, first=False):
    forward_step(va, vb, h, d, w2, 1, first=first)
    forward_step(vb, va, h, d, w2, 2)
    forward_step(va, vb, h, d, w2, 3)
    forward_step(vb, va, h, d, w2, 4, last=True)


def copies(sems, pairs):
    out = [pltpu.make_async_copy(a, b, sems.at[i]) for i, (a, b) in enumerate(pairs)]
    for c in out:
        c.start()
    return out


def wait(*todo):
    for c in todo:
        c.wait()


def plain_rows(v, r0, n):
    return v.at[pl.ds(r0, n)]


def tile_rows(v, r0, n):
    return v.at[pl.ds(r0, n), pl.ds(OFF, LON), :]


def clear_ends(me, up, dn):
    for edge, todo in ((0, up), (63, dn)):

        @pl.when(me[0] == edge)
        def _(todo=todo):
            for ref, r0, n in todo:
                ref[pl.ds(r0, n)] = jnp.zeros((n,) + ref.shape[1:], F32)


def lanes():
    return lax.broadcasted_iota(jnp.int32, (128, 128), 1)


def gather_surface(read, count):
    def step(r, acc):
        for j in range(4):
            p = 4 * r + j
            acc = jnp.where(lanes() == p, pltpu.roll(read(r, j), p, 1), acc)
        return acc

    return lax.fori_loop(0, count, step, jnp.zeros((128, 128), F32)).T


def spread_column(cols, p):
    return jnp.where(lanes() == 0, pltpu.roll(cols, (128 - p) % 128, 1), 0.0)


BLOCK_SCRATCH = [
    pltpu.VMEM((NR, PAD, 128), F32),
    pltpu.VMEM((NR, PAD, 128), F32),
    pltpu.VMEM((NR, LON, 256), BF),
    pltpu.VMEM((NR, LON, 128), F32),
]
U_SCRATCH = pltpu.VMEM((NR, LON, 128), F32)
COLS = pltpu.VMEM((128, 128), F32)
PARTS = (sds(3, LON, LEV), sds(1, LON, LEV), sds(4, LON, LEV))


def near_far(up, dn, odd):
    return up + (dn - up) * odd, dn + (up - dn) * odd


def edge_refs(v, up, dn, odd, cut):
    outer, inner = near_far(up, dn, odd)
    return cut(v, outer, 3), cut(v, outer + 3, 1), cut(v, inner, 4)


def diffusion_copies(d, odd, dt, do, dx, di):
    return [
        (dt, d.at[pl.ds(5, 8)]),
        (do, d.at[pl.ds(3 + 10 * odd, 2)]),
        (di, d.at[pl.ds(13 - 11 * odd, 3)]),
    ] + ([] if dx is None else [(dx, d.at[pl.ds(2 + 13 * odd, 1)])])


def prepare_rows(va, h, r0, n, d=None):
    def cp(i, carry):
        r = r0 + i
        for j in range(4):
            x = va[r, pl.ds(OFF + 128 * j, 128), :]
            if j == 0:
                va[r, pl.ds(OFF + LON, 1), :] = x[0:1]
            if j == 3:
                va[r, pl.ds(OFF - 1, 1), :] = x[127:128]
            if d is not None:
                x = jnp.where(d[r, pl.ds(128 * j, 128), :] > 0.0, x, 0.0)
            put_halves(h, r, j, x)
        return carry

    lax.fori_loop(0, n, cp, 0)


def first_step_kernel(
    me, own, eo, ei, dt, w, o_outer, o_inner, o_mid, w2, w2b, va, vb, h, d, sems
):
    odd = parity(me)
    c = copies(
        sems,
        [
            (dt, d.at[pl.ds(5, 8)]),
            (own, tile_rows(va, 5, 8)),
            (eo, tile_rows(va, 4 + 9 * odd, 1)),
            (ei, tile_rows(va, 13 - 9 * odd, 1)),
        ],
    )
    mix_kernel(w, w2, w2b)
    wait(*c[0:2])
    prepare_rows(va, h, 5, 8, d)
    wait(*c[2:4])
    clear_ends(me, ((va, 4, 1),), ((va, 13, 1),))
    forward_step(va, vb, h, d, w2, 4, first=True, last=True)
    c = copies(
        sems,
        [
            (tile_rows(vb, 5 + 5 * odd, 3), o_outer),
            (tile_rows(vb, 10 - 5 * odd, 3), o_inner),
            (tile_rows(vb, 8, 2), o_mid),
        ],
    )
    wait(*c)


def first_step(*args):
    return pl.pallas_call(
        first_step_kernel,
        out_shape=(
            sds(3, LON, LEV), sds(3, LON, LEV), sds(2, LON, LEV),
            sds(256, 256, dtype=BF), sds(256, 256, dtype=BF),
        ),
        in_specs=[SM] + [ANY] * 4 + [VM],
        out_specs=(ANY,) * 3 + (VM,) * 2,
        scratch_shapes=BLOCK_SCRATCH + [dma_sems(4)],
        compiler_params=params(60),
        cost_estimate=cost(4),
        name="first_step",
    )(*args)


def first_kernel(me, so, si, mid, ho, hi, dt, do, di, w2, o0, o1, o2, o_surf, va, vb, h, d, sems):
    odd = parity(me)
    c = copies(
        sems,
        [
            (so, tile_rows(va, 5 + 5 * odd, 3)),
            (si, tile_rows(va, 10 - 5 * odd, 3)),
            (mid, tile_rows(va, 8, 2)),
            (ho, tile_rows(va, 2 + 11 * odd, 3)),
            (hi, tile_rows(va, 13 - 11 * odd, 3)),
        ]
        + diffusion_copies(d, odd, dt, do, None, di),
    )
    wait(*c[0:3])
    prepare_rows(va, h, 5, 8)
    wait(*c[3:])
    clear_ends(me, ((va, 2, 3), (d, 2, 3)), ((va, 13, 3), (d, 13, 3)))
    prepare_rows(va, h, 3, 2)
    prepare_rows(va, h, 13, 2)
    forward_step(va, vb, h, d, w2, 2)
    forward_step(vb, va, h, d, w2, 3)
    forward_step(va, vb, h, d, w2, 4, last=True)
    c = copies(sems, list(zip(edge_refs(vb, 5, 9, odd, tile_rows), (o0, o1, o2))))
    o_surf[...] = gather_surface(lambda r, j: vb[r + 5, pl.ds(OFF + 128 * j, 128), :], 8)[0:32]
    wait(*c)


def first_block(*args):
    return pl.pallas_call(
        first_kernel,
        out_shape=PARTS + (sds(32, 128),),
        in_specs=[SM] + [ANY] * 8 + [VM],
        out_specs=(ANY,) * 3 + (VM,),
        scratch_shapes=BLOCK_SCRATCH + [dma_sems(8)],
        compiler_params=params(),
        cost_estimate=cost(10),
        name="first_block",
    )(*args)


def middle_kernel(
    me, v0, v1, v2, h0, h1, h2, s, so, si, dt, do, dx, di, m, w2f, w2b,
    o_final, o_adj, o0, o1, o2, o_s, o_so, o_si, va, vb, h, d, u, mm, cols, sems,
):
    odd = parity(me)
    own = edge_refs(va, 5, 9, odd, tile_rows)
    far = edge_refs(va, 1, 13, odd, tile_rows)
    c = copies(
        sems,
        [
            (v0, own[0]),
            (v1, own[1]),
            (v2, own[2]),
            (h0, far[0]),
            (h1, far[1]),
            (h2, far[2]),
        ]
        + diffusion_copies(d, odd, dt, do, dx, di)
        + [(m, mm)],
    )
    c_o, c_i = near_far(0, 48, odd)
    cols[pl.ds(pl.multiple_of(c_o, 16), 16)] = so[...]
    cols[pl.ds(pl.multiple_of(c_i, 16), 16)] = si[...]
    cols[16:48] = s[...]
    cols[64:128] = jnp.zeros((64, 128), F32)
    clear_ends(me, ((cols, 0, 16),), ((cols, 48, 16),))
    cols[...] = cols[...].T

    def prepare(r0):
        def cp(i, carry):
            r = r0 + i
            for j in range(4):
                x = va[r, pl.ds(OFF + 128 * j, 128), :]
                x = x + spread_column(cols[...], 4 * (r - 1) + j)
                put(va, r, j, x)
                put_halves(h, r, j, x)
            return carry

        lax.fori_loop(0, 4, cp, 0)

    wait(*c[0:3])
    prepare(5)
    prepare(9)
    wait(*c[3:10])
    clear_ends(me, ((va, 1, 4), (d, 2, 3)), ((va, 13, 4), (d, 13, 3)))
    prepare(1)
    prepare(13)
    forward_block(va, vb, h, d, w2f)
    out = copies(sems, [(tile_rows(va, 5, 8), o_final)])
    wait(c[10])

    def body(i, carry):
        r = 5 + i
        for j in range(4):
            at = pl.ds(128 * j, 128)
            x = va[r, pl.ds(OFF + 128 * j, 128), :] - mm[i, at, :]
            dd = d[r, at, :]
            x = jnp.where(dd > 0.0, x, 0.0)
            u[r, at, :] = x
            put(vb, r, j, dd * x)
            put_halves(h, r, j, x)
        return carry

    lax.fori_loop(0, 8, body, 0)
    wait(*out)
    push_block(vb, va, u, h, d, w2b)
    out = copies(
        sems,
        list(zip(edge_refs(u, 1, 13, odd, plain_rows), (o0, o1, o2)))
        + [(u.at[pl.ds(5, 8)], o_adj)],
    )
    cols[...] = gather_surface(lambda r, j: u[r + 1, pl.ds(128 * j, 128), :], 16)
    o_so[...] = cols[pl.ds(pl.multiple_of(c_o, 16), 16)]
    o_s[...] = cols[16:48]
    o_si[...] = cols[pl.ds(pl.multiple_of(c_i, 16), 16)]
    wait(*out)


def middle_block(*args):
    return pl.pallas_call(
        middle_kernel,
        out_shape=(
            sds(8, LON, LEV), sds(8, LON, LEV), *PARTS,
            sds(32, 128), sds(16, 128), sds(16, 128),
        ),
        in_specs=[SM] + [ANY] * 6 + [VM] * 3 + [ANY] * 5 + [VM] * 2,
        out_specs=(ANY,) * 5 + (VM,) * 3,
        scratch_shapes=BLOCK_SCRATCH
        + [U_SCRATCH, pltpu.VMEM((8, LON, 128), F32), COLS, dma_sems(12)],
        compiler_params=params(),
        cost_estimate=cost(30),
        name="middle_block",
    )(*args)


def last_kernel(
    me, adj, r0, r1, r2, s, own, dt, do, dx, di, w2b, o_base, o_outer, o_inner,
    va, vb, h, d, u, got, base, cols, sems,
):
    odd = parity(me)
    parts = edge_refs(got, 0, 4, odd, plain_rows)
    c = copies(
        sems,
        [
            (adj, u.at[pl.ds(5, 8)]),
            (r0, parts[0]),
            (r1, parts[1]),
            (r2, parts[2]),
        ]
        + diffusion_copies(d, odd, dt, do, dx, di)
        + [(own, base)],
    )
    cols[0:32] = s[...]
    cols[32:128] = jnp.zeros((96, 128), F32)
    cols[...] = cols[...].T
    wait(*c[0:5])
    clear_ends(me, ((got, 0, 4),), ((got, 4, 4),))

    def cp(i, carry):
        r = 5 + i
        for j in range(4):
            at = pl.ds(128 * j, 128)
            x = u[r, at, :] + got[i, at, :]
            x = x + spread_column(cols[...], 4 * i + j)
            dd = d[r, at, :]
            x = jnp.where(dd > 0.0, x, 0.0)
            u[r, at, :] = x
            put(vb, r, j, dd * x)
            put_halves(h, r, j, x)
        return carry

    lax.fori_loop(0, 8, cp, 0)
    wait(*c[5:9])
    clear_ends(me, ((d, 2, 3),), ((d, 13, 3),))
    push_block(vb, va, u, h, d, w2b)
    out_o, out_i = near_far(1, 13, odd)
    out = copies(sems, [(u.at[pl.ds(out_o, 4)], o_outer), (u.at[pl.ds(out_i, 4)], o_inner)])

    def add(i, carry):
        base[i] = base[i] + u[5 + i]
        return carry

    lax.fori_loop(0, 8, add, 0)
    end = pltpu.make_async_copy(base, o_base, sems.at[2])
    end.start()
    wait(*out)
    end.wait()


def last_block(*args):
    return pl.pallas_call(
        last_kernel,
        out_shape=(sds(8, LON, LEV), sds(4, LON, LEV), sds(4, LON, LEV)),
        in_specs=[SM] + [ANY] * 4 + [VM] + [ANY] * 5 + [VM],
        out_specs=(ANY,) * 3,
        scratch_shapes=BLOCK_SCRATCH
        + [
            U_SCRATCH,
            pltpu.VMEM((8, LON, 128), F32),
            pltpu.VMEM((8, LON, 128), F32),
            COLS,
            dma_sems(10),
        ],
        compiler_params=params(),
        cost_estimate=cost(15),
        name="last_block",
    )(*args)


def offer_kernel(me, send_rows, surf, o):
    o[...] = jnp.zeros((512, 128), F32)
    for off in OFFSETS:
        t = lax.rem(me[0] + (off + 64), 64) * 8
        for q in range(8):
            o[pl.ds(t + q, 1), :] = surf[pl.ds(send_rows[t + q], 1), :]


def offer(me, send_rows, surf):
    return pl.pallas_call(
        offer_kernel,
        out_shape=sds(512, 128),
        in_specs=[SM, SM, VM],
        out_specs=VM,
        name="offer",
    )(me, send_rows, surf)


LIVE = 48


def remap_kernel(me, ids, pick, dest, arrived, w, sea, o, o_outer, o_inner):
    def step(i, acc):
        for q in range(4):
            k = 4 * i + q
            x = arrived[pl.ds(pick[k], 1), :]
            red = jnp.sum(w[ids[k]] * x, axis=1, keepdims=True)
            acc = acc + jnp.where(lanes() == dest[k], red, 0.0)
        return acc

    acc = lax.fori_loop(0, LIVE // 4, step, jnp.zeros((128, 128), F32))
    o[...] = acc.T[0:32] * sea[...]
    e_o, e_i = near_far(0, 16, parity(me))
    o_outer[...] = o[pl.ds(pl.multiple_of(e_o, 16), 16)]
    o_inner[...] = o[pl.ds(pl.multiple_of(e_i, 16), 16)]


def remap(me, ids, pick, dest, arrived, w, sea):
    return pl.pallas_call(
        remap_kernel,
        out_shape=(sds(32, 128), sds(16, 128), sds(16, 128)),
        in_specs=[SM, SM, SM, SM, VM, VM, VM],
        out_specs=(VM,) * 3,
        compiler_params=params(16),
        cost_estimate=cost(3),
        name="remap",
    )(me, ids, pick, dest, arrived, w, sea)


def remap_back_kernel(me, ids, pick, dest, s, so, si, w, sea, o, cols, wide):
    e_o, e_i = near_far(0, 16, parity(me))
    cols[pl.ds(pl.multiple_of(e_o, 16), 16)] = so[...]
    cols[pl.ds(pl.multiple_of(e_i, 16), 16)] = si[...]
    clear_ends(me, ((cols, 0, 16),), ((cols, 16, 16),))
    cols[0:32] = (cols[0:32] + s[...]) * sea[...]
    cols[32:128] = jnp.zeros((96, 128), F32)
    cols[...] = cols[...].T
    for p in range(32):
        wide[p] = jnp.broadcast_to(cols[:, p : p + 1], (128, 128))
    o[...] = jnp.zeros((512, 128), F32)

    def step(i, carry):
        for q in range(4):
            k = 4 * i + q
            red = jnp.sum(w[ids[k]] * wide[dest[k]], axis=0, keepdims=True)
            o[pl.ds(pick[k], 1), :] = red
        return carry

    lax.fori_loop(0, LIVE // 4, step, 0)


def remap_back(me, ids, pick, dest, s, so, si, w, sea):
    return pl.pallas_call(
        remap_back_kernel,
        out_shape=sds(512, 128),
        in_specs=[SM, SM, SM, SM, VM, VM, VM, VM, VM],
        out_specs=VM,
        scratch_shapes=[COLS, pltpu.VMEM((32, 128, 128), F32)],
        compiler_params=params(16),
        cost_estimate=cost(3),
        name="remap_back",
    )(me, ids, pick, dest, s, so, si, w, sea)


def collect_kernel(me, send_rows, got, o):
    o[...] = jnp.zeros((32, 128), F32)
    for off in OFFSETS:
        t = lax.rem(me[0] + (off + 64), 64) * 8
        for q in range(8):
            at = pl.ds(send_rows[t + q], 1)
            o[at, :] = o[at, :] + got[pl.ds(t + q, 1), :]


def collect(me, send_rows, got):
    return pl.pallas_call(
        collect_kernel,
        out_shape=sds(32, 128),
        in_specs=[SM, SM, VM],
        out_specs=VM,
        name="collect",
    )(me, send_rows, got)


def shards(
    starting_perturbation,
    measured_discrepancy,
    diffusion,
    vert_mix,
    ocean_mask,
    pair_tile,
    pair_patch,
    dest_patch,
    pair_blocks,
    remap_weight,
):
    component = lax.axis_index("comp")
    own_tile = lax.axis_index("tile")
    across = [(i, (i + 1 if i % 2 else i - 1) % 64) for i in range(64)]
    on_chip = [(i, i ^ 1) for i in range(64)]

    def far(x):
        return lax.ppermute(x, "tile", across)

    def near(x):
        return lax.ppermute(x, "tile", on_chip)

    def swap(x):
        return lax.ppermute(x, "comp", [(0, 1), (1, 0)])

    def exchange(x):
        x = x.reshape(64, 8, 128)
        x = lax.all_to_all(x, "tile", split_axis=0, concat_axis=0, tiled=True)
        return x.reshape(512, 128)

    me = jnp.stack([own_tile, component]).astype(jnp.int32)
    e_o, e_i, start = start_in(me, starting_perturbation.reshape(1024, LON))
    eo, ei = far(e_o), near(e_i)
    d_o, d_x, d_i, dt = diff_in(me, diffusion.reshape(1024, LON), ocean_mask)
    do, di = far(d_o), near(d_i)
    s_o, s_i, mid, w2f, w2b = first_step(me, start, eo, ei, dt, vert_mix[0])
    ho, hi = far(s_o), near(s_i)
    dx = far(d_x)
    pair_tile, pair_patch, dest_patch, pair_blocks, ocean_mask, do = lax.optimization_barrier(
        (pair_tile, pair_patch, dest_patch, pair_blocks, ocean_mask, do)
    )

    sea = jnp.where(component == 1, ocean_mask.astype(F32), 1.0)
    sea32 = sea.reshape(32, 128)
    slots = jnp.arange(64, dtype=jnp.int32)
    live = slots % 8 < jnp.repeat(pair_blocks[0, 0], 8)
    place = jnp.sum((slots[None, :] < slots[:, None]) & live[None, :], axis=1)
    chosen = ((place[None, :] == slots[:LIVE, None]) & live[None, :]).astype(jnp.int32)
    ids = jnp.sum(chosen * slots[None, :], axis=1)
    pick = jnp.repeat(pair_tile[component, own_tile], 8) * 8 + slots % 8
    pick = jnp.sum(chosen * pick[None, :], axis=1)
    dest = jnp.sum(chosen * dest_patch[0, 0][None, :], axis=1)
    hits = (pair_tile[component] == own_tile).astype(jnp.int32)
    sources = pair_patch[component].reshape(64, 8, 8)
    send_rows = jnp.sum(hits[:, :, None] * sources, axis=1).reshape(512)
    weights = remap_weight[0]
    measured = to_rows(measured_discrepancy.reshape(1024, LON))
    ho, hi, do, di, w2b, ids, pick, dest, send_rows, measured, sea32 = (
        lax.optimization_barrier(
            (ho, hi, do, di, w2b, ids, pick, dest, send_rows, measured, sea32)
        )
    )

    v0, v1, v2, surf = first_block(me, s_o, s_i, mid, ho, hi, dt, do, di, w2f)
    other = swap(surf)
    h0, h2 = far(v0), near(v2)
    offered = offer(me, send_rows, other)
    arrived = exchange(offered)
    v1s, arrived = lax.optimization_barrier((v1, arrived))
    h1 = far(v1s)
    fix, fix_o, fix_i = remap(me, ids, pick, dest, arrived, weights, sea32)
    fo, fi = far(fix_o), near(fix_i)
    final, adj, a0, a1, a2, s0, s0_o, s0_i = middle_block(
        me, v0, v1, v2, h0, h1, h2, fix, fo, fi, dt, do, dx, di, measured, w2f, w2b
    )
    ro, ri = far(s0_o), near(s0_i)
    a0, a2, ro, ri = lax.optimization_barrier((a0, a2, ro, ri))
    r0, r2 = far(a0), near(a2)
    offered = remap_back(me, ids, pick, dest, s0, ro, ri, weights, sea32)
    back = exchange(offered)
    a1, back = lax.optimization_barrier((a1, back))
    r1 = far(a1)
    back = swap(collect(me, send_rows, back))
    base, g_o, g_i = last_block(me, adj, r0, r1, r2, back, start, dt, do, dx, di, w2b)
    go, gi = far(g_o), near(g_i)
    final_raw = to_raw(final)
    gradient = grad_out(me, base, go, gi)
    shape = starting_perturbation.shape
    return final_raw.reshape(shape), gradient.reshape(shape)


def solution(mesh):
    field = P("comp", None, "tile", None)
    placed = (
        field,
        field,
        field,
        P("comp", None, None),
        P("tile", None),
        P(),
        P(),
        P("comp", "tile", None),
        P("comp", "tile", None),
        P("comp", "tile", None, None),
    )

    return jax.shard_map(
        shards,
        mesh=mesh,
        in_specs=placed,
        out_specs=(field, field),
        check_vma=False,
    )
```

```python
import jax
import jax.numpy as jnp
from jax import lax
from jax.experimental import pallas as pl
from jax.experimental.pallas import tpu as pltpu
from jax.sharding import PartitionSpec as P


F32 = jnp.float32
BF = jnp.bfloat16
LON, LEV = 512, 128
OFF, PAD = 8, 528
NR = 18
VM = pl.BlockSpec(memory_space=pltpu.VMEM)
SM = pl.BlockSpec(memory_space=pltpu.SMEM)
BLOCK_MIB = 44
OFFSETS = tuple(range(-7, 8)) + (32,)


def sds(*shape, dtype=F32):
    return jax.ShapeDtypeStruct(shape, dtype)


def cost(us):
    return pl.CostEstimate(flops=int(us * 5e8), bytes_accessed=1 << 20, transcendentals=0)


def params(mib=BLOCK_MIB):
    return pltpu.CompilerParams(vmem_limit_bytes=mib * 2**20)


def parity(me):
    return lax.rem(me[0], 2)


def halves(x):
    hi = x.astype(BF)
    return hi, (x - hi.astype(F32)).astype(BF)


ANY = pl.BlockSpec(memory_space=pltpu.MemorySpace.HBM)
RAW = pltpu.VMEM((4, 1024, 128), F32)
ROWS = pltpu.VMEM((8, LON, LEV), F32)


def dma_sems(*n):
    return pltpu.SemaphoreType.DMA(n)


def lon_part(ref, j):
    return ref.at[:, pl.ds(128 * j, 128), :]


def start_raw(x, buf, sems):
    out = [
        pltpu.make_async_copy(x.at[:, pl.ds(128 * j, 128)], buf.at[j], sems.at[j])
        for j in range(4)
    ]
    for c in out:
        c.start()
    return out


def turned(buf, j, r):
    return buf[j, pl.ds(r, 128, stride=8), :].T


def start_in_kernel(x, outer, inner, full, buf, out, sems, osems):
    odd = lax.rem(lax.axis_index("tile"), 2)
    c = start_raw(x, buf, sems)
    todo = []
    for j in range(4):
        c[j].wait()
        for r in range(8):
            out[r, pl.ds(128 * j, 128), :] = turned(buf, j, r)
        for i, (r0, n, dst) in enumerate(((7 * odd, 1, outer), (7 - 7 * odd, 1, inner), (0, 8, full))):
            src = out.at[pl.ds(r0, n), pl.ds(128 * j, 128), :]
            todo.append(pltpu.make_async_copy(src, lon_part(dst, j), osems.at[i, j]))
            todo[-1].start()
    for d in todo:
        d.wait()


def start_in(x):
    return pl.pallas_call(
        start_in_kernel,
        out_shape=(sds(1, LON, LEV), sds(1, LON, LEV), sds(8, LON, LEV)),
        in_specs=[ANY],
        out_specs=(ANY,) * 3,
        scratch_shapes=[RAW, ROWS, dma_sems(4), dma_sems(3, 4)],
        compiler_params=params(60),
        cost_estimate=cost(4),
        name="start_in",
    )(x)


def diff_in_kernel(me, x, mask, outer, third, inner, full, buf, out, sems, osems):
    odd = parity(me)
    c = start_raw(x, buf, sems)
    todo = []
    for j in range(4):
        c[j].wait()
        at = pl.ds(128 * j, 128)
        for r in range(8):
            sea = jnp.where(me[1] == 1, mask[r : r + 1, at].astype(F32), 1.0)
            out[r, at, :] = (buf[j, pl.ds(r, 128, stride=8), :] * sea).T
        for i, (r0, n, dst) in enumerate(((6 * odd, 2, outer), (2 + 3 * odd, 1, third), (5 - 5 * odd, 3, inner), (0, 8, full))):
            src = out.at[pl.ds(r0, n), at, :]
            todo.append(pltpu.make_async_copy(src, lon_part(dst, j), osems.at[i, j]))
            todo[-1].start()
    for d in todo:
        d.wait()


def diff_in(me, x, mask):
    return pl.pallas_call(
        diff_in_kernel,
        out_shape=(sds(2, LON, LEV), sds(1, LON, LEV), sds(3, LON, LEV), sds(8, LON, LEV)),
        in_specs=[SM, ANY, VM],
        out_specs=(ANY,) * 4,
        scratch_shapes=[RAW, ROWS, dma_sems(4), dma_sems(4, 4)],
        compiler_params=params(60),
        cost_estimate=cost(4),
        name="diff_in",
    )(me, x, mask)


def to_rows_kernel(x, o, buf, out, sems, osems):
    c = start_raw(x, buf, sems)
    todo = []
    for j in range(4):
        c[j].wait()
        for r in range(8):
            out[r, pl.ds(128 * j, 128), :] = turned(buf, j, r)
        todo.append(pltpu.make_async_copy(lon_part(out, j), lon_part(o, j), osems.at[j]))
        todo[-1].start()
    for d in todo:
        d.wait()


def to_rows(x):
    return pl.pallas_call(
        to_rows_kernel,
        out_shape=sds(8, LON, LEV),
        in_specs=[ANY],
        out_specs=ANY,
        scratch_shapes=[RAW, ROWS, dma_sems(4), dma_sems(4)],
        compiler_params=params(),
        cost_estimate=cost(4),
        name="to_rows",
    )(x)


def to_raw_kernel(x, o):
    for r in range(8):
        o[pl.ds(r, 128, stride=8), :] = x[r].T


def to_raw(x):
    return pl.pallas_call(
        to_raw_kernel,
        grid=(4,),
        out_shape=sds(1024, LON),
        in_specs=[pl.BlockSpec((8, 128, 128), lambda j: (0, j, 0))],
        out_specs=pl.BlockSpec((1024, 128), lambda j: (0, j)),
        compiler_params=params(),
        cost_estimate=cost(4),
        name="to_raw",
    )(x)


def grad_out_kernel(me, x, outer, inner, o, base, add, buf, sems, osems):
    odd = parity(me)
    c = []
    for j in range(4):
        at = pl.ds(128 * j, 128)
        for i, (src, dst) in enumerate(
            (
                (lon_part(outer, j), add.at[pl.ds(4 * odd, 4), at, :]),
                (lon_part(inner, j), add.at[pl.ds(4 - 4 * odd, 4), at, :]),
                (lon_part(x, j), lon_part(base, j)),
            )
        ):
            c.append(pltpu.make_async_copy(src, dst, sems.at[i, j]))
            c[-1].start()
    keep_up = jnp.where(me[0] > 0, 1.0, 0.0)
    keep_dn = jnp.where(me[0] < 63, 1.0, 0.0)
    todo = []
    for j in range(4):
        at = pl.ds(128 * j, 128)
        for d in c[3 * j : 3 * j + 3]:
            d.wait()
        for r in range(8):
            keep = keep_up if r < 4 else keep_dn
            buf[j, pl.ds(r, 128, stride=8), :] = (base[r, at, :] + keep * add[r, at, :]).T
        todo.append(pltpu.make_async_copy(buf.at[j], o.at[:, at], osems.at[j]))
        todo[-1].start()
    for d in todo:
        d.wait()


def grad_out(me, x, outer, inner):
    return pl.pallas_call(
        grad_out_kernel,
        out_shape=sds(1024, LON),
        in_specs=[SM, ANY, ANY, ANY],
        out_specs=ANY,
        scratch_shapes=[ROWS, ROWS, RAW, dma_sems(3, 4), dma_sems(4)],
        compiler_params=params(),
        cost_estimate=cost(4),
        name="grad_out",
    )(me, x, outer, inner)


def mix_kernel(w, fwd, bwd):
    for dst, x in ((fwd, w[...].T), (bwd, w[...])):
        hi, lo = halves(x)
        dst[0:128, 0:128] = hi
        dst[128:256, 0:128] = hi
        dst[0:128, 128:256] = lo
        dst[128:256, 128:256] = jnp.zeros((128, 128), BF)


def put(v, r, j, new):
    v[r, pl.ds(OFF + 128 * j, 128), :] = new
    if j == 0:
        v[r, pl.ds(OFF + LON, 1), :] = new[0:1]
    if j == 3:
        v[r, pl.ds(OFF - 1, 1), :] = new[127:128]


def put_halves(h, r, j, new):
    hi, lo = halves(new)
    h[r, pl.ds(128 * j, 128), 0:128] = hi
    h[r, pl.ds(128 * j, 128), 128:256] = lo


def around(v, r, j):
    at = OFF + 128 * j
    n = v[r - 1, pl.ds(at, 128), :] + v[r + 1, pl.ds(at, 128), :]
    return n + (v[r, pl.ds(at - 1, 128), :] + v[r, pl.ds(at + 1, 128), :])


GROUP = {14: 7, 12: 6, 10: 5, 8: 4}


def mixed_rows(h, w2, lo, n, body):
    k = GROUP[n]

    def step(i, carry):
        r0 = lo + k * i
        y = jnp.dot(h[pl.ds(r0, k)].reshape(LON * k, 256), w2[...], preferred_element_type=F32)
        for q in range(k):
            for j in range(4):
                part = y[LON * q + 128 * j : LON * q + 128 * j + 128]
                body(r0 + q, j, part[:, 0:128] + part[:, 128:256])
        return carry

    lax.fori_loop(0, n // k, step, 0)


def forward_step(va, vb, h, d, w2, s, first=False, last=False):
    def body(r, j, y):
        c = va[r, pl.ds(OFF + 128 * j, 128), :]
        dd = d[r, pl.ds(128 * j, 128), :]
        n = dd * (around(va, r, j) - 4.0 * c)
        if first:
            c = jnp.where(dd > 0.0, c, 0.0)
        new = (c + n) + y
        put(vb, r, j, new)
        if not last:
            put_halves(h, r, j, new)

    mixed_rows(h, w2, 1 + s, 16 - 2 * s, body)


def push_step(ga, gb, u, h, d, w2, s, last=False):
    def finish(r, j, new, dd):
        u[r, pl.ds(128 * j, 128), :] = new
        put(gb, r, j, dd * new)
        put_halves(h, r, j, new)

    def body(r, j, y):
        at = pl.ds(128 * j, 128)
        n = around(ga, r, j) - 4.0 * ga[r, pl.ds(OFF + 128 * j, 128), :]
        c = u[r, at, :]
        if last:
            u[r, at, :] = (c + n) + y
        else:
            dd = d[r, at, :]
            finish(r, j, (c + jnp.where(dd > 0.0, n, 0.0)) + y, dd)

    mixed_rows(h, w2, 6 - s, 6 + 2 * s, body)
    for r, near in ((5 - s, 6 - s), (12 + s, 11 + s)):
        for j in range(4):
            at = pl.ds(128 * j, 128)
            n = ga[near, pl.ds(OFF + 128 * j, 128), :]
            if last:
                u[r, at, :] = n
            else:
                dd = d[r, at, :]
                finish(r, j, jnp.where(dd > 0.0, n, 0.0), dd)


def push_block(ga, gb, u, h, d, w2):
    for s, g in ((1, ga), (2, gb), (3, ga), (4, gb)):
        g[5 - s] = jnp.zeros((PAD, 128), F32)
        g[12 + s] = jnp.zeros((PAD, 128), F32)
    push_step(ga, gb, u, h, d, w2, 1)
    push_step(gb, ga, u, h, d, w2, 2)
    push_step(ga, gb, u, h, d, w2, 3)
    push_step(gb, ga, u, h, d, w2, 4, last=True)


def forward_block(va, vb, h, d, w2, first=False):
    forward_step(va, vb, h, d, w2, 1, first=first)
    forward_step(vb, va, h, d, w2, 2)
    forward_step(va, vb, h, d, w2, 3)
    forward_step(vb, va, h, d, w2, 4, last=True)


def copies(sems, pairs):
    out = [pltpu.make_async_copy(a, b, sems.at[i]) for i, (a, b) in enumerate(pairs)]
    for c in out:
        c.start()
    return out


def wait(*todo):
    for c in todo:
        c.wait()


def plain_rows(v, r0, n):
    return v.at[pl.ds(r0, n)]


def tile_rows(v, r0, n):
    return v.at[pl.ds(r0, n), pl.ds(OFF, LON), :]


def clear_ends(me, up, dn):
    for edge, todo in ((0, up), (63, dn)):

        @pl.when(me[0] == edge)
        def _(todo=todo):
            for ref, r0, n in todo:
                ref[pl.ds(r0, n)] = jnp.zeros((n,) + ref.shape[1:], F32)


def lanes():
    return lax.broadcasted_iota(jnp.int32, (128, 128), 1)


def gather_surface(read, count):
    def step(r, acc):
        for j in range(4):
            p = 4 * r + j
            acc = jnp.where(lanes() == p, pltpu.roll(read(r, j), p, 1), acc)
        return acc

    return lax.fori_loop(0, count, step, jnp.zeros((128, 128), F32)).T


def spread_column(cols, p):
    return jnp.where(lanes() == 0, pltpu.roll(cols, (128 - p) % 128, 1), 0.0)


BLOCK_SCRATCH = [
    pltpu.VMEM((NR, PAD, 128), F32),
    pltpu.VMEM((NR, PAD, 128), F32),
    pltpu.VMEM((NR, LON, 256), BF),
    pltpu.VMEM((NR, LON, 128), F32),
]
U_SCRATCH = pltpu.VMEM((NR, LON, 128), F32)
COLS = pltpu.VMEM((128, 128), F32)


def part_shapes(n):
    return sds(n, LON, LEV), sds(4 - n, LON, LEV), sds(4, LON, LEV)


def near_far(up, dn, odd):
    return up + (dn - up) * odd, dn + (up - dn) * odd


def edge_refs(v, up, dn, odd, cut, n):
    outer, inner = near_far(up, dn, odd)
    return cut(v, outer, n), cut(v, outer + n, 4 - n), cut(v, inner, 4)


def diffusion_copies(d, odd, dt, do, dx, di):
    return [
        (dt, d.at[pl.ds(5, 8)]),
        (do, d.at[pl.ds(3 + 10 * odd, 2)]),
        (di, d.at[pl.ds(13 - 11 * odd, 3)]),
    ] + ([] if dx is None else [(dx, d.at[pl.ds(2 + 13 * odd, 1)])])


def prepare_rows(va, h, r0, n, d=None):
    def cp(i, carry):
        r = r0 + i
        for j in range(4):
            x = va[r, pl.ds(OFF + 128 * j, 128), :]
            if j == 0:
                va[r, pl.ds(OFF + LON, 1), :] = x[0:1]
            if j == 3:
                va[r, pl.ds(OFF - 1, 1), :] = x[127:128]
            if d is not None:
                x = jnp.where(d[r, pl.ds(128 * j, 128), :] > 0.0, x, 0.0)
            put_halves(h, r, j, x)
        return carry

    lax.fori_loop(0, n, cp, 0)


def first_step_kernel(
    me, own, eo, ei, dt, w, o_outer, o_inner, o_mid, w2, w2b, va, vb, h, d, sems
):
    odd = parity(me)
    c = copies(
        sems,
        [
            (dt, d.at[pl.ds(5, 8)]),
            (own, tile_rows(va, 5, 8)),
            (eo, tile_rows(va, 4 + 9 * odd, 1)),
            (ei, tile_rows(va, 13 - 9 * odd, 1)),
        ],
    )
    mix_kernel(w, w2, w2b)
    wait(*c[0:2])
    prepare_rows(va, h, 5, 8, d)
    wait(*c[2:4])
    clear_ends(me, ((va, 4, 1),), ((va, 13, 1),))
    forward_step(va, vb, h, d, w2, 4, first=True, last=True)
    c = copies(
        sems,
        [
            (tile_rows(vb, 5 + 5 * odd, 3), o_outer),
            (tile_rows(vb, 10 - 5 * odd, 3), o_inner),
            (tile_rows(vb, 8, 2), o_mid),
        ],
    )
    wait(*c)


def first_step(*args):
    return pl.pallas_call(
        first_step_kernel,
        out_shape=(
            sds(3, LON, LEV), sds(3, LON, LEV), sds(2, LON, LEV),
            sds(256, 256, dtype=BF), sds(256, 256, dtype=BF),
        ),
        in_specs=[SM] + [ANY] * 4 + [VM],
        out_specs=(ANY,) * 3 + (VM,) * 2,
        scratch_shapes=BLOCK_SCRATCH + [dma_sems(4)],
        compiler_params=params(60),
        cost_estimate=cost(4),
        name="first_step",
    )(*args)


def first_kernel(me, so, si, mid, ho, hi, dt, do, di, w2, o0, o1, o2, o_surf, va, vb, h, d, sems):
    odd = parity(me)
    c = copies(
        sems,
        [
            (so, tile_rows(va, 5 + 5 * odd, 3)),
            (si, tile_rows(va, 10 - 5 * odd, 3)),
            (mid, tile_rows(va, 8, 2)),
            (ho, tile_rows(va, 2 + 11 * odd, 3)),
            (hi, tile_rows(va, 13 - 11 * odd, 3)),
        ]
        + diffusion_copies(d, odd, dt, do, None, di),
    )
    wait(*c[0:3])
    prepare_rows(va, h, 5, 8)
    wait(*c[3:])
    clear_ends(me, ((va, 2, 3), (d, 2, 3)), ((va, 13, 3), (d, 13, 3)))
    prepare_rows(va, h, 3, 2)
    prepare_rows(va, h, 13, 2)
    forward_step(va, vb, h, d, w2, 2)
    forward_step(vb, va, h, d, w2, 3)
    forward_step(va, vb, h, d, w2, 4, last=True)
    c = copies(sems, list(zip(edge_refs(vb, 5, 9, odd, tile_rows, 2), (o0, o1, o2))))
    o_surf[...] = gather_surface(lambda r, j: vb[r + 5, pl.ds(OFF + 128 * j, 128), :], 8)[0:32]
    wait(*c)


def first_block(*args):
    return pl.pallas_call(
        first_kernel,
        out_shape=part_shapes(2) + (sds(32, 128),),
        in_specs=[SM] + [ANY] * 8 + [VM],
        out_specs=(ANY,) * 3 + (VM,),
        scratch_shapes=BLOCK_SCRATCH + [dma_sems(8)],
        compiler_params=params(60),
        cost_estimate=cost(10),
        name="first_block",
    )(*args)


def middle_kernel(
    me, v0, v1, v2, h0, h1, h2, s, so, si, dt, do, dx, di, m, w2f, w2b,
    o_final, o_adj, o0, o1, o2, o_s, o_so, o_si, va, vb, h, d, u, mm, cols, sems,
):
    odd = parity(me)
    own = edge_refs(va, 5, 9, odd, tile_rows, 2)
    far = edge_refs(va, 1, 13, odd, tile_rows, 2)
    c = copies(
        sems,
        [
            (v0, own[0]),
            (v1, own[1]),
            (v2, own[2]),
            (h0, far[0]),
            (h1, far[1]),
            (h2, far[2]),
        ]
        + diffusion_copies(d, odd, dt, do, dx, di)
        + [(m, mm)],
    )
    c_o, c_i = near_far(0, 48, odd)
    cols[pl.ds(pl.multiple_of(c_o, 16), 16)] = so[...]
    cols[pl.ds(pl.multiple_of(c_i, 16), 16)] = si[...]
    cols[16:48] = s[...]
    cols[64:128] = jnp.zeros((64, 128), F32)
    clear_ends(me, ((cols, 0, 16),), ((cols, 48, 16),))
    cols[...] = cols[...].T

    def prepare(r0):
        def cp(i, carry):
            r = r0 + i
            for j in range(4):
                x = va[r, pl.ds(OFF + 128 * j, 128), :]
                x = x + spread_column(cols[...], 4 * (r - 1) + j)
                put(va, r, j, x)
                put_halves(h, r, j, x)
            return carry

        lax.fori_loop(0, 4, cp, 0)

    wait(*c[0:3])
    prepare(5)
    prepare(9)
    wait(*c[3:10])
    clear_ends(me, ((va, 1, 4), (d, 2, 3)), ((va, 13, 4), (d, 13, 3)))
    prepare(1)
    prepare(13)
    forward_block(va, vb, h, d, w2f)
    out = copies(sems, [(tile_rows(va, 5, 8), o_final)])
    wait(c[10])

    def body(i, carry):
        r = 5 + i
        for j in range(4):
            at = pl.ds(128 * j, 128)
            x = va[r, pl.ds(OFF + 128 * j, 128), :] - mm[i, at, :]
            dd = d[r, at, :]
            x = jnp.where(dd > 0.0, x, 0.0)
            u[r, at, :] = x
            put(vb, r, j, dd * x)
            put_halves(h, r, j, x)
        return carry

    lax.fori_loop(0, 8, body, 0)
    wait(*out)
    push_block(vb, va, u, h, d, w2b)
    out = copies(
        sems,
        list(zip(edge_refs(u, 1, 13, odd, plain_rows, 3), (o0, o1, o2)))
        + [(u.at[pl.ds(5, 8)], o_adj)],
    )
    cols[...] = gather_surface(lambda r, j: u[r + 1, pl.ds(128 * j, 128), :], 16)
    o_so[...] = cols[pl.ds(pl.multiple_of(c_o, 16), 16)]
    o_s[...] = cols[16:48]
    o_si[...] = cols[pl.ds(pl.multiple_of(c_i, 16), 16)]
    wait(*out)


def middle_block(*args):
    return pl.pallas_call(
        middle_kernel,
        out_shape=(
            sds(8, LON, LEV), sds(8, LON, LEV), *part_shapes(3),
            sds(32, 128), sds(16, 128), sds(16, 128),
        ),
        in_specs=[SM] + [ANY] * 6 + [VM] * 3 + [ANY] * 5 + [VM] * 2,
        out_specs=(ANY,) * 5 + (VM,) * 3,
        scratch_shapes=BLOCK_SCRATCH
        + [U_SCRATCH, pltpu.VMEM((8, LON, 128), F32), COLS, dma_sems(12)],
        compiler_params=params(),
        cost_estimate=cost(30),
        name="middle_block",
    )(*args)


def last_kernel(
    me, adj, r0, r1, r2, s, own, dt, do, dx, di, w2b, o_base, o_outer, o_inner,
    va, vb, h, d, u, got, base, cols, sems,
):
    odd = parity(me)
    parts = edge_refs(got, 0, 4, odd, plain_rows, 3)
    c = copies(
        sems,
        [
            (adj, u.at[pl.ds(5, 8)]),
            (r0, parts[0]),
            (r1, parts[1]),
            (r2, parts[2]),
        ]
        + diffusion_copies(d, odd, dt, do, dx, di)
        + [(own, base)],
    )
    cols[0:32] = s[...]
    cols[32:128] = jnp.zeros((96, 128), F32)
    cols[...] = cols[...].T
    wait(*c[0:5])
    clear_ends(me, ((got, 0, 4),), ((got, 4, 4),))

    def cp(i, carry):
        r = 5 + i
        for j in range(4):
            at = pl.ds(128 * j, 128)
            x = u[r, at, :] + got[i, at, :]
            x = x + spread_column(cols[...], 4 * i + j)
            dd = d[r, at, :]
            x = jnp.where(dd > 0.0, x, 0.0)
            u[r, at, :] = x
            put(vb, r, j, dd * x)
            put_halves(h, r, j, x)
        return carry

    lax.fori_loop(0, 8, cp, 0)
    wait(*c[5:9])
    clear_ends(me, ((d, 2, 3),), ((d, 13, 3),))
    push_block(vb, va, u, h, d, w2b)
    out_o, out_i = near_far(1, 13, odd)
    out = copies(sems, [(u.at[pl.ds(out_o, 4)], o_outer), (u.at[pl.ds(out_i, 4)], o_inner)])

    def add(i, carry):
        base[i] = base[i] + u[5 + i]
        return carry

    lax.fori_loop(0, 8, add, 0)
    end = pltpu.make_async_copy(base, o_base, sems.at[2])
    end.start()
    wait(*out)
    end.wait()


def last_block(*args):
    return pl.pallas_call(
        last_kernel,
        out_shape=(sds(8, LON, LEV), sds(4, LON, LEV), sds(4, LON, LEV)),
        in_specs=[SM] + [ANY] * 4 + [VM] + [ANY] * 5 + [VM],
        out_specs=(ANY,) * 3,
        scratch_shapes=BLOCK_SCRATCH
        + [
            U_SCRATCH,
            pltpu.VMEM((8, LON, 128), F32),
            pltpu.VMEM((8, LON, 128), F32),
            COLS,
            dma_sems(10),
        ],
        compiler_params=params(),
        cost_estimate=cost(15),
        name="last_block",
    )(*args)


def offer_kernel(me, send_rows, surf, o):
    o[...] = jnp.zeros((512, 128), F32)
    for off in OFFSETS:
        t = lax.rem(me[0] + (off + 64), 64) * 8
        for q in range(8):
            o[pl.ds(t + q, 1), :] = surf[pl.ds(send_rows[t + q], 1), :]


def offer(me, send_rows, surf):
    return pl.pallas_call(
        offer_kernel,
        out_shape=sds(512, 128),
        in_specs=[SM, SM, VM],
        out_specs=VM,
        name="offer",
    )(me, send_rows, surf)


LIVE = 48


def remap_kernel(me, ids, pick, dest, arrived, w, sea, o, o_outer, o_inner):
    def step(i, acc):
        for q in range(4):
            k = 4 * i + q
            x = arrived[pl.ds(pick[k], 1), :]
            red = jnp.sum(w[ids[k]] * x, axis=1, keepdims=True)
            acc = acc + jnp.where(lanes() == dest[k], red, 0.0)
        return acc

    acc = lax.fori_loop(0, LIVE // 4, step, jnp.zeros((128, 128), F32))
    o[...] = acc.T[0:32] * sea[...]
    e_o, e_i = near_far(0, 16, parity(me))
    o_outer[...] = o[pl.ds(pl.multiple_of(e_o, 16), 16)]
    o_inner[...] = o[pl.ds(pl.multiple_of(e_i, 16), 16)]


def remap(me, ids, pick, dest, arrived, w, sea):
    return pl.pallas_call(
        remap_kernel,
        out_shape=(sds(32, 128), sds(16, 128), sds(16, 128)),
        in_specs=[SM, SM, SM, SM, VM, VM, VM],
        out_specs=(VM,) * 3,
        compiler_params=params(16),
        cost_estimate=cost(3),
        name="remap",
    )(me, ids, pick, dest, arrived, w, sea)


def remap_back_kernel(me, ids, pick, dest, s, so, si, w, sea, o, cols, wide):
    e_o, e_i = near_far(0, 16, parity(me))
    cols[pl.ds(pl.multiple_of(e_o, 16), 16)] = so[...]
    cols[pl.ds(pl.multiple_of(e_i, 16), 16)] = si[...]
    clear_ends(me, ((cols, 0, 16),), ((cols, 16, 16),))
    cols[0:32] = (cols[0:32] + s[...]) * sea[...]
    cols[32:128] = jnp.zeros((96, 128), F32)
    cols[...] = cols[...].T
    for p in range(32):
        wide[p] = jnp.broadcast_to(cols[:, p : p + 1], (128, 128))
    o[...] = jnp.zeros((512, 128), F32)

    def step(i, carry):
        for q in range(4):
            k = 4 * i + q
            red = jnp.sum(w[ids[k]] * wide[dest[k]], axis=0, keepdims=True)
            o[pl.ds(pick[k], 1), :] = red
        return carry

    lax.fori_loop(0, LIVE // 4, step, 0)


def remap_back(me, ids, pick, dest, s, so, si, w, sea):
    return pl.pallas_call(
        remap_back_kernel,
        out_shape=sds(512, 128),
        in_specs=[SM, SM, SM, SM, VM, VM, VM, VM, VM],
        out_specs=VM,
        scratch_shapes=[COLS, pltpu.VMEM((32, 128, 128), F32)],
        compiler_params=params(16),
        cost_estimate=cost(3),
        name="remap_back",
    )(me, ids, pick, dest, s, so, si, w, sea)


def collect_kernel(me, send_rows, got, o):
    o[...] = jnp.zeros((32, 128), F32)
    for off in OFFSETS:
        t = lax.rem(me[0] + (off + 64), 64) * 8
        for q in range(8):
            at = pl.ds(send_rows[t + q], 1)
            o[at, :] = o[at, :] + got[pl.ds(t + q, 1), :]


def collect(me, send_rows, got):
    return pl.pallas_call(
        collect_kernel,
        out_shape=sds(32, 128),
        in_specs=[SM, SM, VM],
        out_specs=VM,
        name="collect",
    )(me, send_rows, got)


def shards(
    starting_perturbation,
    measured_discrepancy,
    diffusion,
    vert_mix,
    ocean_mask,
    pair_tile,
    pair_patch,
    dest_patch,
    pair_blocks,
    remap_weight,
):
    component = lax.axis_index("comp")
    own_tile = lax.axis_index("tile")
    across = [(i, (i + 1 if i % 2 else i - 1) % 64) for i in range(64)]
    on_chip = [(i, i ^ 1) for i in range(64)]

    def far(x):
        return lax.ppermute(x, "tile", across)

    def near(x):
        return lax.ppermute(x, "tile", on_chip)

    def swap(x):
        return lax.ppermute(x, "comp", [(0, 1), (1, 0)])

    def exchange(x):
        x = x.reshape(64, 8, 128)
        x = lax.all_to_all(x, "tile", split_axis=0, concat_axis=0, tiled=True)
        return x.reshape(512, 128)

    me = jnp.stack([own_tile, component]).astype(jnp.int32)
    e_o, e_i, start = start_in(starting_perturbation.reshape(1024, LON))
    eo, ei = far(e_o), near(e_i)
    d_o, d_x, d_i, dt = diff_in(me, diffusion.reshape(1024, LON), ocean_mask)
    do, di = far(d_o), near(d_i)
    s_o, s_i, mid, w2f, w2b = first_step(me, start, eo, ei, dt, vert_mix[0])
    ho, hi = far(s_o), near(s_i)
    dx = far(d_x)
    pair_tile, pair_patch, dest_patch, pair_blocks, ocean_mask, do = lax.optimization_barrier(
        (pair_tile, pair_patch, dest_patch, pair_blocks, ocean_mask, do)
    )

    sea = jnp.where(component == 1, ocean_mask.astype(F32), 1.0)
    sea32 = sea.reshape(32, 128)
    slots = jnp.arange(64, dtype=jnp.int32)
    live = slots % 8 < jnp.repeat(pair_blocks[0, 0], 8)
    place = jnp.sum((slots[None, :] < slots[:, None]) & live[None, :], axis=1)
    chosen = ((place[None, :] == slots[:LIVE, None]) & live[None, :]).astype(jnp.int32)
    ids = jnp.sum(chosen * slots[None, :], axis=1)
    pick = jnp.repeat(pair_tile[component, own_tile], 8) * 8 + slots % 8
    pick = jnp.sum(chosen * pick[None, :], axis=1)
    dest = jnp.sum(chosen * dest_patch[0, 0][None, :], axis=1)
    hits = (pair_tile[component] == own_tile).astype(jnp.int32)
    sources = pair_patch[component].reshape(64, 8, 8)
    send_rows = jnp.sum(hits[:, :, None] * sources, axis=1).reshape(512)
    weights = remap_weight[0]
    measured = to_rows(measured_discrepancy.reshape(1024, LON))
    ho, hi, do, di, w2b, ids, pick, dest, send_rows, measured, sea32 = (
        lax.optimization_barrier(
            (ho, hi, do, di, w2b, ids, pick, dest, send_rows, measured, sea32)
        )
    )

    v0, v1, v2, surf = first_block(me, s_o, s_i, mid, ho, hi, dt, do, di, w2f)
    other = swap(surf)
    h0, h2 = far(v0), near(v2)
    offered = offer(me, send_rows, other)
    arrived = exchange(offered)
    v1s, arrived = lax.optimization_barrier((v1, arrived))
    h1 = far(v1s)
    fix, fix_o, fix_i = remap(me, ids, pick, dest, arrived, weights, sea32)
    fo, fi = far(fix_o), near(fix_i)
    final, adj, a0, a1, a2, s0, s0_o, s0_i = middle_block(
        me, v0, v1, v2, h0, h1, h2, fix, fo, fi, dt, do, dx, di, measured, w2f, w2b
    )
    ro, ri = far(s0_o), near(s0_i)
    r0, r2 = far(a0), near(a2)
    offered = remap_back(me, ids, pick, dest, s0, ro, ri, weights, sea32)
    back = exchange(offered)
    a1, back = lax.optimization_barrier((a1, back))
    r1 = far(a1)
    back = swap(collect(me, send_rows, back))
    base, g_o, g_i = last_block(me, adj, r0, r1, r2, back, start, dt, do, dx, di, w2b)
    go, gi = far(g_o), near(g_i)
    final_raw = to_raw(final)
    gradient = grad_out(me, base, go, gi)
    shape = starting_perturbation.shape
    return final_raw.reshape(shape), gradient.reshape(shape)


def solution(mesh):
    field = P("comp", None, "tile", None)
    placed = (
        field,
        field,
        field,
        P("comp", None, None),
        P("tile", None),
        P(),
        P(),
        P("comp", "tile", None),
        P("comp", "tile", None),
        P("comp", "tile", None, None),
    )

    return jax.shard_map(
        shards,
        mesh=mesh,
        in_specs=placed,
        out_specs=(field, field),
        check_vma=False,
    )
```

```python
import jax
import jax.numpy as jnp
from jax import lax
from jax.experimental import pallas as pl
from jax.experimental.pallas import tpu as pltpu
from jax.sharding import PartitionSpec as P


F32 = jnp.float32
BF = jnp.bfloat16
LON, LEV = 512, 128
OFF, PAD = 8, 528
NR = 18
VM = pl.BlockSpec(memory_space=pltpu.VMEM)
SM = pl.BlockSpec(memory_space=pltpu.SMEM)
BLOCK_MIB = 44
OFFSETS = tuple(range(-7, 8)) + (32,)


def sds(*shape, dtype=F32):
    return jax.ShapeDtypeStruct(shape, dtype)


def cost(us):
    return pl.CostEstimate(flops=int(us * 5e8), bytes_accessed=1 << 20, transcendentals=0)


def params(mib=BLOCK_MIB):
    return pltpu.CompilerParams(vmem_limit_bytes=mib * 2**20)


def parity(me):
    return lax.rem(me[0], 2)


def halves(x):
    hi = x.astype(BF)
    return hi, (x - hi.astype(F32)).astype(BF)


ANY = pl.BlockSpec(memory_space=pltpu.MemorySpace.HBM)
RAW = pltpu.VMEM((4, 1024, 128), F32)
ROWS = pltpu.VMEM((8, LON, LEV), F32)


def dma_sems(*n):
    return pltpu.SemaphoreType.DMA(n)


def lon_part(ref, j):
    return ref.at[:, pl.ds(128 * j, 128), :]


def start_raw(x, buf, sems):
    out = [
        pltpu.make_async_copy(x.at[:, pl.ds(128 * j, 128)], buf.at[j], sems.at[j])
        for j in range(4)
    ]
    for c in out:
        c.start()
    return out


def turned(buf, j, r):
    return buf[j, pl.ds(r, 128, stride=8), :].T


def start_in_kernel(x, outer, inner, full, buf, out, sems, osems):
    odd = lax.rem(lax.axis_index("tile"), 2)
    c = start_raw(x, buf, sems)
    todo = []
    for j in range(4):
        c[j].wait()
        for r in range(8):
            out[r, pl.ds(128 * j, 128), :] = turned(buf, j, r)
        for i, (r0, n, dst) in enumerate(((7 * odd, 1, outer), (7 - 7 * odd, 1, inner), (0, 8, full))):
            src = out.at[pl.ds(r0, n), pl.ds(128 * j, 128), :]
            todo.append(pltpu.make_async_copy(src, lon_part(dst, j), osems.at[i, j]))
            todo[-1].start()
    for d in todo:
        d.wait()


def start_in(x):
    return pl.pallas_call(
        start_in_kernel,
        out_shape=(sds(1, LON, LEV), sds(1, LON, LEV), sds(8, LON, LEV)),
        in_specs=[ANY],
        out_specs=(ANY,) * 3,
        scratch_shapes=[RAW, ROWS, dma_sems(4), dma_sems(3, 4)],
        compiler_params=params(60),
        cost_estimate=cost(4),
        name="start_in",
    )(x)


def diff_in_kernel(me, x, mask, outer, third, inner, full, buf, out, sems, osems):
    odd = parity(me)
    c = start_raw(x, buf, sems)
    todo = []
    for j in range(4):
        c[j].wait()
        at = pl.ds(128 * j, 128)
        for r in range(8):
            sea = jnp.where(me[1] == 1, mask[r : r + 1, at].astype(F32), 1.0)
            out[r, at, :] = (buf[j, pl.ds(r, 128, stride=8), :] * sea).T
        for i, (r0, n, dst) in enumerate(((6 * odd, 2, outer), (2 + 3 * odd, 1, third), (5 - 5 * odd, 3, inner), (0, 8, full))):
            src = out.at[pl.ds(r0, n), at, :]
            todo.append(pltpu.make_async_copy(src, lon_part(dst, j), osems.at[i, j]))
            todo[-1].start()
    for d in todo:
        d.wait()


def diff_in(me, x, mask):
    return pl.pallas_call(
        diff_in_kernel,
        out_shape=(sds(2, LON, LEV), sds(1, LON, LEV), sds(3, LON, LEV), sds(8, LON, LEV)),
        in_specs=[SM, ANY, VM],
        out_specs=(ANY,) * 4,
        scratch_shapes=[RAW, ROWS, dma_sems(4), dma_sems(4, 4)],
        compiler_params=params(60),
        cost_estimate=cost(4),
        name="diff_in",
    )(me, x, mask)


def to_rows_kernel(x, o, buf, out, sems, osems):
    c = start_raw(x, buf, sems)
    todo = []
    for j in range(4):
        c[j].wait()
        for r in range(8):
            out[r, pl.ds(128 * j, 128), :] = turned(buf, j, r)
        todo.append(pltpu.make_async_copy(lon_part(out, j), lon_part(o, j), osems.at[j]))
        todo[-1].start()
    for d in todo:
        d.wait()


def to_rows(x):
    return pl.pallas_call(
        to_rows_kernel,
        out_shape=sds(8, LON, LEV),
        in_specs=[ANY],
        out_specs=ANY,
        scratch_shapes=[RAW, ROWS, dma_sems(4), dma_sems(4)],
        compiler_params=params(),
        cost_estimate=cost(4),
        name="to_rows",
    )(x)


def to_raw_kernel(x, o):
    for r in range(8):
        o[pl.ds(r, 128, stride=8), :] = x[r].T


def to_raw(x):
    return pl.pallas_call(
        to_raw_kernel,
        grid=(4,),
        out_shape=sds(1024, LON),
        in_specs=[pl.BlockSpec((8, 128, 128), lambda j: (0, j, 0))],
        out_specs=pl.BlockSpec((1024, 128), lambda j: (0, j)),
        compiler_params=params(),
        cost_estimate=cost(4),
        name="to_raw",
    )(x)


def grad_out_kernel(me, x, outer, inner, o, base, add, buf, sems, osems):
    odd = parity(me)
    c = []
    for j in range(4):
        at = pl.ds(128 * j, 128)
        for i, (src, dst) in enumerate(
            (
                (lon_part(outer, j), add.at[pl.ds(4 * odd, 4), at, :]),
                (lon_part(inner, j), add.at[pl.ds(4 - 4 * odd, 4), at, :]),
                (lon_part(x, j), lon_part(base, j)),
            )
        ):
            c.append(pltpu.make_async_copy(src, dst, sems.at[i, j]))
            c[-1].start()
    keep_up = jnp.where(me[0] > 0, 1.0, 0.0)
    keep_dn = jnp.where(me[0] < 63, 1.0, 0.0)
    todo = []
    for j in range(4):
        at = pl.ds(128 * j, 128)
        for d in c[3 * j : 3 * j + 3]:
            d.wait()
        for r in range(8):
            keep = keep_up if r < 4 else keep_dn
            buf[j, pl.ds(r, 128, stride=8), :] = (base[r, at, :] + keep * add[r, at, :]).T
        todo.append(pltpu.make_async_copy(buf.at[j], o.at[:, at], osems.at[j]))
        todo[-1].start()
    for d in todo:
        d.wait()


def grad_out(me, x, outer, inner):
    return pl.pallas_call(
        grad_out_kernel,
        out_shape=sds(1024, LON),
        in_specs=[SM, ANY, ANY, ANY],
        out_specs=ANY,
        scratch_shapes=[ROWS, ROWS, RAW, dma_sems(3, 4), dma_sems(4)],
        compiler_params=params(),
        cost_estimate=cost(4),
        name="grad_out",
    )(me, x, outer, inner)


def mix_kernel(w, fwd, bwd):
    for dst, x in ((fwd, w[...].T), (bwd, w[...])):
        hi, lo = halves(x)
        dst[0:128, 0:128] = hi
        dst[128:256, 0:128] = hi
        dst[0:128, 128:256] = lo
        dst[128:256, 128:256] = jnp.zeros((128, 128), BF)


def put(v, r, j, new):
    v[r, pl.ds(OFF + 128 * j, 128), :] = new
    if j == 0:
        v[r, pl.ds(OFF + LON, 1), :] = new[0:1]
    if j == 3:
        v[r, pl.ds(OFF - 1, 1), :] = new[127:128]


def put_halves(h, r, j, new):
    hi, lo = halves(new)
    h[r, pl.ds(128 * j, 128), 0:128] = hi
    h[r, pl.ds(128 * j, 128), 128:256] = lo


def around(v, r, j):
    at = OFF + 128 * j
    n = v[r - 1, pl.ds(at, 128), :] + v[r + 1, pl.ds(at, 128), :]
    return n + (v[r, pl.ds(at - 1, 128), :] + v[r, pl.ds(at + 1, 128), :])


GROUP = {14: 7, 12: 6, 10: 5, 8: 4}


def mixed_rows(h, w2, lo, n, body):
    k = GROUP[n]

    def step(i, carry):
        r0 = lo + k * i
        y = jnp.dot(h[pl.ds(r0, k)].reshape(LON * k, 256), w2[...], preferred_element_type=F32)
        for q in range(k):
            for j in range(4):
                part = y[LON * q + 128 * j : LON * q + 128 * j + 128]
                body(r0 + q, j, part[:, 0:128] + part[:, 128:256])
        return carry

    lax.fori_loop(0, n // k, step, 0)


def forward_step(va, vb, h, d, w2, s, first=False, last=False):
    def body(r, j, y):
        c = va[r, pl.ds(OFF + 128 * j, 128), :]
        dd = d[r, pl.ds(128 * j, 128), :]
        n = dd * (around(va, r, j) - 4.0 * c)
        if first:
            c = jnp.where(dd > 0.0, c, 0.0)
        new = (c + n) + y
        put(vb, r, j, new)
        if not last:
            put_halves(h, r, j, new)

    mixed_rows(h, w2, 1 + s, 16 - 2 * s, body)


def push_step(ga, gb, u, h, d, w2, s, last=False):
    def finish(r, j, new, dd):
        u[r, pl.ds(128 * j, 128), :] = new
        put(gb, r, j, dd * new)
        put_halves(h, r, j, new)

    def body(r, j, y):
        at = pl.ds(128 * j, 128)
        n = around(ga, r, j) - 4.0 * ga[r, pl.ds(OFF + 128 * j, 128), :]
        c = u[r, at, :]
        if last:
            u[r, at, :] = (c + n) + y
        else:
            dd = d[r, at, :]
            finish(r, j, (c + jnp.where(dd > 0.0, n, 0.0)) + y, dd)

    mixed_rows(h, w2, 6 - s, 6 + 2 * s, body)
    for r, near in ((5 - s, 6 - s), (12 + s, 11 + s)):
        for j in range(4):
            at = pl.ds(128 * j, 128)
            n = ga[near, pl.ds(OFF + 128 * j, 128), :]
            if last:
                u[r, at, :] = n
            else:
                dd = d[r, at, :]
                finish(r, j, jnp.where(dd > 0.0, n, 0.0), dd)


def push_block(ga, gb, u, h, d, w2):
    for s, g in ((1, ga), (2, gb), (3, ga), (4, gb)):
        g[5 - s] = jnp.zeros((PAD, 128), F32)
        g[12 + s] = jnp.zeros((PAD, 128), F32)
    push_step(ga, gb, u, h, d, w2, 1)
    push_step(gb, ga, u, h, d, w2, 2)
    push_step(ga, gb, u, h, d, w2, 3)
    push_step(gb, ga, u, h, d, w2, 4, last=True)


def forward_block(va, vb, h, d, w2, first=False):
    forward_step(va, vb, h, d, w2, 1, first=first)
    forward_step(vb, va, h, d, w2, 2)
    forward_step(va, vb, h, d, w2, 3)
    forward_step(vb, va, h, d, w2, 4, last=True)


def copies(sems, pairs):
    out = [pltpu.make_async_copy(a, b, sems.at[i]) for i, (a, b) in enumerate(pairs)]
    for c in out:
        c.start()
    return out


def wait(*todo):
    for c in todo:
        c.wait()


def plain_rows(v, r0, n):
    return v.at[pl.ds(r0, n)]


def tile_rows(v, r0, n):
    return v.at[pl.ds(r0, n), pl.ds(OFF, LON), :]


def clear_ends(me, up, dn):
    for edge, todo in ((0, up), (63, dn)):

        @pl.when(me[0] == edge)
        def _(todo=todo):
            for ref, r0, n in todo:
                ref[pl.ds(r0, n)] = jnp.zeros((n,) + ref.shape[1:], F32)


def lanes():
    return lax.broadcasted_iota(jnp.int32, (128, 128), 1)


def gather_surface(read, count):
    def step(r, acc):
        for j in range(4):
            p = 4 * r + j
            acc = jnp.where(lanes() == p, pltpu.roll(read(r, j), p, 1), acc)
        return acc

    return lax.fori_loop(0, count, step, jnp.zeros((128, 128), F32)).T


def spread_column(cols, p):
    return jnp.where(lanes() == 0, pltpu.roll(cols, (128 - p) % 128, 1), 0.0)


BLOCK_SCRATCH = [
    pltpu.VMEM((NR, PAD, 128), F32),
    pltpu.VMEM((NR, PAD, 128), F32),
    pltpu.VMEM((NR, LON, 256), BF),
    pltpu.VMEM((NR, LON, 128), F32),
]
U_SCRATCH = pltpu.VMEM((NR, LON, 128), F32)
COLS = pltpu.VMEM((128, 128), F32)


def part_shapes(n):
    return sds(n, LON, LEV), sds(4 - n, LON, LEV), sds(4, LON, LEV)


def near_far(up, dn, odd):
    return up + (dn - up) * odd, dn + (up - dn) * odd


def edge_refs(v, up, dn, odd, cut, n):
    outer, inner = near_far(up, dn, odd)
    return cut(v, outer, n), cut(v, outer + n, 4 - n), cut(v, inner, 4)


def diffusion_copies(d, odd, dt, do, dx, di):
    return [
        (dt, d.at[pl.ds(5, 8)]),
        (do, d.at[pl.ds(3 + 10 * odd, 2)]),
        (di, d.at[pl.ds(13 - 11 * odd, 3)]),
    ] + ([] if dx is None else [(dx, d.at[pl.ds(2 + 13 * odd, 1)])])


def prepare_rows(va, h, r0, n, d=None):
    def cp(i, carry):
        r = r0 + i
        for j in range(4):
            x = va[r, pl.ds(OFF + 128 * j, 128), :]
            if j == 0:
                va[r, pl.ds(OFF + LON, 1), :] = x[0:1]
            if j == 3:
                va[r, pl.ds(OFF - 1, 1), :] = x[127:128]
            if d is not None:
                x = jnp.where(d[r, pl.ds(128 * j, 128), :] > 0.0, x, 0.0)
            put_halves(h, r, j, x)
        return carry

    lax.fori_loop(0, n, cp, 0)


def first_step_kernel(
    me, own, eo, ei, dt, w, o_outer, o_inner, o_mid, w2, w2b, va, vb, h, d, sems
):
    odd = parity(me)
    c = copies(
        sems,
        [
            (dt, d.at[pl.ds(5, 8)]),
            (own, tile_rows(va, 5, 8)),
            (eo, tile_rows(va, 4 + 9 * odd, 1)),
            (ei, tile_rows(va, 13 - 9 * odd, 1)),
        ],
    )
    mix_kernel(w, w2, w2b)
    wait(*c[0:2])
    prepare_rows(va, h, 5, 8, d)
    wait(*c[2:4])
    clear_ends(me, ((va, 4, 1),), ((va, 13, 1),))
    forward_step(va, vb, h, d, w2, 4, first=True, last=True)
    c = copies(
        sems,
        [
            (tile_rows(vb, 5 + 5 * odd, 3), o_outer),
            (tile_rows(vb, 10 - 5 * odd, 3), o_inner),
            (tile_rows(vb, 8, 2), o_mid),
        ],
    )
    wait(*c)


def first_step(*args):
    return pl.pallas_call(
        first_step_kernel,
        out_shape=(
            sds(3, LON, LEV), sds(3, LON, LEV), sds(2, LON, LEV),
            sds(256, 256, dtype=BF), sds(256, 256, dtype=BF),
        ),
        in_specs=[SM] + [ANY] * 4 + [VM],
        out_specs=(ANY,) * 3 + (VM,) * 2,
        scratch_shapes=BLOCK_SCRATCH + [dma_sems(4)],
        compiler_params=params(60),
        cost_estimate=cost(4),
        name="first_step",
    )(*args)


def first_kernel(me, so, si, mid, ho, hi, dt, do, di, w2, o0, o1, o2, o_surf, va, vb, h, d, sems):
    odd = parity(me)
    c = copies(
        sems,
        [
            (so, tile_rows(va, 5 + 5 * odd, 3)),
            (si, tile_rows(va, 10 - 5 * odd, 3)),
            (mid, tile_rows(va, 8, 2)),
            (ho, tile_rows(va, 2 + 11 * odd, 3)),
            (hi, tile_rows(va, 13 - 11 * odd, 3)),
        ]
        + diffusion_copies(d, odd, dt, do, None, di),
    )
    wait(*c[0:3])
    prepare_rows(va, h, 5, 8)
    wait(*c[3:])
    clear_ends(me, ((va, 2, 3), (d, 2, 3)), ((va, 13, 3), (d, 13, 3)))
    prepare_rows(va, h, 3, 2)
    prepare_rows(va, h, 13, 2)
    forward_step(va, vb, h, d, w2, 2)
    forward_step(vb, va, h, d, w2, 3)
    forward_step(va, vb, h, d, w2, 4, last=True)
    c = copies(sems, list(zip(edge_refs(vb, 5, 9, odd, tile_rows, 3), (o0, o1, o2))))
    o_surf[...] = gather_surface(lambda r, j: vb[r + 5, pl.ds(OFF + 128 * j, 128), :], 8)[0:32]
    wait(*c)


def first_block(*args):
    return pl.pallas_call(
        first_kernel,
        out_shape=part_shapes(3) + (sds(32, 128),),
        in_specs=[SM] + [ANY] * 8 + [VM],
        out_specs=(ANY,) * 3 + (VM,),
        scratch_shapes=BLOCK_SCRATCH + [dma_sems(8)],
        compiler_params=params(60),
        cost_estimate=cost(10),
        name="first_block",
    )(*args)


def middle_kernel(
    me, v0, v1, v2, h0, h1, h2, s, so, si, dt, do, dx, di, m, w2f, w2b,
    o_final, o_adj, o0, o1, o2, o_s, o_so, o_si, va, vb, h, d, u, mm, cols, sems,
):
    odd = parity(me)
    own = edge_refs(va, 5, 9, odd, tile_rows, 3)
    far = edge_refs(va, 1, 13, odd, tile_rows, 3)
    c = copies(
        sems,
        [
            (v0, own[0]),
            (v1, own[1]),
            (v2, own[2]),
            (h0, far[0]),
            (h1, far[1]),
            (h2, far[2]),
        ]
        + diffusion_copies(d, odd, dt, do, dx, di)
        + [(m, mm)],
    )
    c_o, c_i = near_far(0, 48, odd)
    cols[pl.ds(pl.multiple_of(c_o, 16), 16)] = so[...]
    cols[pl.ds(pl.multiple_of(c_i, 16), 16)] = si[...]
    cols[16:48] = s[...]
    cols[64:128] = jnp.zeros((64, 128), F32)
    clear_ends(me, ((cols, 0, 16),), ((cols, 48, 16),))
    cols[...] = cols[...].T

    def prepare(r0):
        def cp(i, carry):
            r = r0 + i
            for j in range(4):
                x = va[r, pl.ds(OFF + 128 * j, 128), :]
                x = x + spread_column(cols[...], 4 * (r - 1) + j)
                put(va, r, j, x)
                put_halves(h, r, j, x)
            return carry

        lax.fori_loop(0, 4, cp, 0)

    wait(*c[0:3])
    prepare(5)
    prepare(9)
    wait(*c[3:10])
    clear_ends(me, ((va, 1, 4), (d, 2, 3)), ((va, 13, 4), (d, 13, 3)))
    prepare(1)
    prepare(13)
    forward_block(va, vb, h, d, w2f)
    out = copies(sems, [(tile_rows(va, 5, 8), o_final)])
    wait(c[10])

    def body(i, carry):
        r = 5 + i
        for j in range(4):
            at = pl.ds(128 * j, 128)
            x = va[r, pl.ds(OFF + 128 * j, 128), :] - mm[i, at, :]
            dd = d[r, at, :]
            x = jnp.where(dd > 0.0, x, 0.0)
            u[r, at, :] = x
            put(vb, r, j, dd * x)
            put_halves(h, r, j, x)
        return carry

    lax.fori_loop(0, 8, body, 0)
    wait(*out)
    push_block(vb, va, u, h, d, w2b)
    out = copies(
        sems,
        list(zip(edge_refs(u, 1, 13, odd, plain_rows, 3), (o0, o1, o2)))
        + [(u.at[pl.ds(5, 8)], o_adj)],
    )
    cols[...] = gather_surface(lambda r, j: u[r + 1, pl.ds(128 * j, 128), :], 16)
    o_so[...] = cols[pl.ds(pl.multiple_of(c_o, 16), 16)]
    o_s[...] = cols[16:48]
    o_si[...] = cols[pl.ds(pl.multiple_of(c_i, 16), 16)]
    wait(*out)


def middle_block(*args):
    return pl.pallas_call(
        middle_kernel,
        out_shape=(
            sds(8, LON, LEV), sds(8, LON, LEV), *part_shapes(3),
            sds(32, 128), sds(16, 128), sds(16, 128),
        ),
        in_specs=[SM] + [ANY] * 6 + [VM] * 3 + [ANY] * 5 + [VM] * 2,
        out_specs=(ANY,) * 5 + (VM,) * 3,
        scratch_shapes=BLOCK_SCRATCH
        + [U_SCRATCH, pltpu.VMEM((8, LON, 128), F32), COLS, dma_sems(12)],
        compiler_params=params(),
        cost_estimate=cost(30),
        name="middle_block",
    )(*args)


def last_kernel(
    me, adj, r0, r1, r2, s, own, dt, do, dx, di, w2b, o_base, o_outer, o_inner,
    va, vb, h, d, u, got, base, cols, sems,
):
    odd = parity(me)
    parts = edge_refs(got, 0, 4, odd, plain_rows, 3)
    c = copies(
        sems,
        [
            (adj, u.at[pl.ds(5, 8)]),
            (r0, parts[0]),
            (r1, parts[1]),
            (r2, parts[2]),
        ]
        + diffusion_copies(d, odd, dt, do, dx, di)
        + [(own, base)],
    )
    cols[0:32] = s[...]
    cols[32:128] = jnp.zeros((96, 128), F32)
    cols[...] = cols[...].T
    wait(*c[0:5])
    clear_ends(me, ((got, 0, 4),), ((got, 4, 4),))

    def cp(i, carry):
        r = 5 + i
        for j in range(4):
            at = pl.ds(128 * j, 128)
            x = u[r, at, :] + got[i, at, :]
            x = x + spread_column(cols[...], 4 * i + j)
            dd = d[r, at, :]
            x = jnp.where(dd > 0.0, x, 0.0)
            u[r, at, :] = x
            put(vb, r, j, dd * x)
            put_halves(h, r, j, x)
        return carry

    lax.fori_loop(0, 8, cp, 0)
    wait(*c[5:9])
    clear_ends(me, ((d, 2, 3),), ((d, 13, 3),))
    push_block(vb, va, u, h, d, w2b)
    out_o, out_i = near_far(1, 13, odd)
    out = copies(sems, [(u.at[pl.ds(out_o, 4)], o_outer), (u.at[pl.ds(out_i, 4)], o_inner)])

    def add(i, carry):
        base[i] = base[i] + u[5 + i]
        return carry

    lax.fori_loop(0, 8, add, 0)
    end = pltpu.make_async_copy(base, o_base, sems.at[2])
    end.start()
    wait(*out)
    end.wait()


def last_block(*args):
    return pl.pallas_call(
        last_kernel,
        out_shape=(sds(8, LON, LEV), sds(4, LON, LEV), sds(4, LON, LEV)),
        in_specs=[SM] + [ANY] * 4 + [VM] + [ANY] * 5 + [VM],
        out_specs=(ANY,) * 3,
        scratch_shapes=BLOCK_SCRATCH
        + [
            U_SCRATCH,
            pltpu.VMEM((8, LON, 128), F32),
            pltpu.VMEM((8, LON, 128), F32),
            COLS,
            dma_sems(10),
        ],
        compiler_params=params(),
        cost_estimate=cost(15),
        name="last_block",
    )(*args)


def offer_kernel(me, send_rows, surf, o):
    o[...] = jnp.zeros((512, 128), F32)
    for off in OFFSETS:
        t = lax.rem(me[0] + (off + 64), 64) * 8
        for q in range(8):
            o[pl.ds(t + q, 1), :] = surf[pl.ds(send_rows[t + q], 1), :]


def offer(me, send_rows, surf):
    return pl.pallas_call(
        offer_kernel,
        out_shape=sds(512, 128),
        in_specs=[SM, SM, VM],
        out_specs=VM,
        name="offer",
    )(me, send_rows, surf)


LIVE = 48


def remap_kernel(me, ids, pick, dest, arrived, w, sea, o, o_outer, o_inner):
    def step(i, acc):
        for q in range(4):
            k = 4 * i + q
            x = arrived[pl.ds(pick[k], 1), :]
            red = jnp.sum(w[ids[k]] * x, axis=1, keepdims=True)
            acc = acc + jnp.where(lanes() == dest[k], red, 0.0)
        return acc

    acc = lax.fori_loop(0, LIVE // 4, step, jnp.zeros((128, 128), F32))
    o[...] = acc.T[0:32] * sea[...]
    e_o, e_i = near_far(0, 16, parity(me))
    o_outer[...] = o[pl.ds(pl.multiple_of(e_o, 16), 16)]
    o_inner[...] = o[pl.ds(pl.multiple_of(e_i, 16), 16)]


def remap(me, ids, pick, dest, arrived, w, sea):
    return pl.pallas_call(
        remap_kernel,
        out_shape=(sds(32, 128), sds(16, 128), sds(16, 128)),
        in_specs=[SM, SM, SM, SM, VM, VM, VM],
        out_specs=(VM,) * 3,
        compiler_params=params(16),
        cost_estimate=cost(3),
        name="remap",
    )(me, ids, pick, dest, arrived, w, sea)


def remap_back_kernel(me, ids, pick, dest, s, so, si, w, sea, o, cols, wide):
    e_o, e_i = near_far(0, 16, parity(me))
    cols[pl.ds(pl.multiple_of(e_o, 16), 16)] = so[...]
    cols[pl.ds(pl.multiple_of(e_i, 16), 16)] = si[...]
    clear_ends(me, ((cols, 0, 16),), ((cols, 16, 16),))
    cols[0:32] = (cols[0:32] + s[...]) * sea[...]
    cols[32:128] = jnp.zeros((96, 128), F32)
    cols[...] = cols[...].T
    for p in range(32):
        wide[p] = jnp.broadcast_to(cols[:, p : p + 1], (128, 128))
    o[...] = jnp.zeros((512, 128), F32)

    def step(i, carry):
        for q in range(4):
            k = 4 * i + q
            red = jnp.sum(w[ids[k]] * wide[dest[k]], axis=0, keepdims=True)
            o[pl.ds(pick[k], 1), :] = red
        return carry

    lax.fori_loop(0, LIVE // 4, step, 0)


def remap_back(me, ids, pick, dest, s, so, si, w, sea):
    return pl.pallas_call(
        remap_back_kernel,
        out_shape=sds(512, 128),
        in_specs=[SM, SM, SM, SM, VM, VM, VM, VM, VM],
        out_specs=VM,
        scratch_shapes=[COLS, pltpu.VMEM((32, 128, 128), F32)],
        compiler_params=params(16),
        cost_estimate=cost(3),
        name="remap_back",
    )(me, ids, pick, dest, s, so, si, w, sea)


def collect_kernel(me, send_rows, got, o, *sums):
    for acc in sums:
        acc[...] = jnp.zeros((32, 128), F32)
    for off in OFFSETS:
        t = lax.rem(me[0] + (off + 64), 64) * 8
        for q in range(8):
            acc = sums[q % 4]
            at = pl.ds(send_rows[t + q], 1)
            acc[at, :] = acc[at, :] + got[pl.ds(t + q, 1), :]
    o[...] = (sums[0][...] + sums[1][...]) + (sums[2][...] + sums[3][...])


def collect(me, send_rows, got):
    return pl.pallas_call(
        collect_kernel,
        out_shape=sds(32, 128),
        in_specs=[SM, SM, VM],
        out_specs=VM,
        scratch_shapes=[pltpu.VMEM((32, 128), F32)] * 4,
        name="collect",
    )(me, send_rows, got)


def shards(
    starting_perturbation,
    measured_discrepancy,
    diffusion,
    vert_mix,
    ocean_mask,
    pair_tile,
    pair_patch,
    dest_patch,
    pair_blocks,
    remap_weight,
):
    component = lax.axis_index("comp")
    own_tile = lax.axis_index("tile")
    across = [(i, (i + 1 if i % 2 else i - 1) % 64) for i in range(64)]
    on_chip = [(i, i ^ 1) for i in range(64)]

    def far(x):
        return lax.ppermute(x, "tile", across)

    def near(x):
        return lax.ppermute(x, "tile", on_chip)

    def swap(x):
        return lax.ppermute(x, "comp", [(0, 1), (1, 0)])

    def exchange(x):
        x = x.reshape(64, 8, 128)
        x = lax.all_to_all(x, "tile", split_axis=0, concat_axis=0, tiled=True)
        return x.reshape(512, 128)

    me = jnp.stack([own_tile, component]).astype(jnp.int32)
    e_o, e_i, start = start_in(starting_perturbation.reshape(1024, LON))
    eo, ei = far(e_o), near(e_i)
    d_o, d_x, d_i, dt = diff_in(me, diffusion.reshape(1024, LON), ocean_mask)
    do, di = far(d_o), near(d_i)
    s_o, s_i, mid, w2f, w2b = first_step(me, start, eo, ei, dt, vert_mix[0])
    ho, hi = far(s_o), near(s_i)
    dx = far(d_x)
    pair_tile, pair_patch, dest_patch, pair_blocks, ocean_mask, do = lax.optimization_barrier(
        (pair_tile, pair_patch, dest_patch, pair_blocks, ocean_mask, do)
    )

    sea = jnp.where(component == 1, ocean_mask.astype(F32), 1.0)
    sea32 = sea.reshape(32, 128)
    slots = jnp.arange(64, dtype=jnp.int32)
    live = slots % 8 < jnp.repeat(pair_blocks[0, 0], 8)
    place = jnp.sum((slots[None, :] < slots[:, None]) & live[None, :], axis=1)
    chosen = ((place[None, :] == slots[:LIVE, None]) & live[None, :]).astype(jnp.int32)
    ids = jnp.sum(chosen * slots[None, :], axis=1)
    pick = jnp.repeat(pair_tile[component, own_tile], 8) * 8 + slots % 8
    pick = jnp.sum(chosen * pick[None, :], axis=1)
    dest = jnp.sum(chosen * dest_patch[0, 0][None, :], axis=1)
    hits = (pair_tile[component] == own_tile).astype(jnp.int32)
    sources = pair_patch[component].reshape(64, 8, 8)
    send_rows = jnp.sum(hits[:, :, None] * sources, axis=1).reshape(512)
    weights = remap_weight[0]
    measured = to_rows(measured_discrepancy.reshape(1024, LON))
    ho, hi, do, di, w2b, ids, pick, dest, send_rows, measured, sea32 = (
        lax.optimization_barrier(
            (ho, hi, do, di, w2b, ids, pick, dest, send_rows, measured, sea32)
        )
    )

    v0, v1, v2, surf = first_block(me, s_o, s_i, mid, ho, hi, dt, do, di, w2f)
    other = swap(surf)
    h0, h2 = far(v0), near(v2)
    offered = offer(me, send_rows, other)
    arrived = exchange(offered)
    v1s, arrived = lax.optimization_barrier((v1, arrived))
    h1 = far(v1s)
    fix, fix_o, fix_i = remap(me, ids, pick, dest, arrived, weights, sea32)
    fo, fi = far(fix_o), near(fix_i)
    final, adj, a0, a1, a2, s0, s0_o, s0_i = middle_block(
        me, v0, v1, v2, h0, h1, h2, fix, fo, fi, dt, do, dx, di, measured, w2f, w2b
    )
    ro, ri = far(s0_o), near(s0_i)
    r0, r2 = far(a0), near(a2)
    offered = remap_back(me, ids, pick, dest, s0, ro, ri, weights, sea32)
    back = exchange(offered)
    a1, back = lax.optimization_barrier((a1, back))
    r1 = far(a1)
    back = swap(collect(me, send_rows, back))
    base, g_o, g_i = last_block(me, adj, r0, r1, r2, back, start, dt, do, dx, di, w2b)
    go, gi = far(g_o), near(g_i)
    final_raw = to_raw(final)
    gradient = grad_out(me, base, go, gi)
    shape = starting_perturbation.shape
    return final_raw.reshape(shape), gradient.reshape(shape)


def solution(mesh):
    field = P("comp", None, "tile", None)
    placed = (
        field,
        field,
        field,
        P("comp", None, None),
        P("tile", None),
        P(),
        P(),
        P("comp", "tile", None),
        P("comp", "tile", None),
        P("comp", "tile", None, None),
    )

    return jax.shard_map(
        shards,
        mesh=mesh,
        in_specs=placed,
        out_specs=(field, field),
        check_vma=False,
    )
```
